8 devices in a mesh: data: 1 (over z), cp: 2 (over y), tp: 4 (over x, core).
Axes of the slice: x: 2, y: 2, z: 1, core: 2. Of those that a mesh axis runs over, the one named last changes fastest.
Arguments:
- x_in: bfloat16 [4096, 2048], P(('data', 'cp', 'tp'))
- w_q: bfloat16 [2048, 16, 128], P(None, 'tp')
- w_k: bfloat16 [2048, 16, 128], P(None, 'tp')
- w_v: bfloat16 [2048, 16, 128], P(None, 'tp')
- w_o: bfloat16 [16, 128, 2048], P('tp')
- expert_idx: int32 [4096, 2], P(('data', 'cp', 'tp'))
- gate_wts: float32 [4096, 2], P(('data', 'cp', 'tp'))
- w_gate: bfloat16 [64, 2048, 1024], P(('cp', 'tp'))
- w_up: bfloat16 [64, 2048, 1024], P(('cp', 'tp'))
- w_down: bfloat16 [64, 1024, 2048], P(('cp', 'tp'))
Outputs:
- output: bfloat16 [4096, 2048], P(('data', 'cp', 'tp'))
All inputs are finite; a program needn't handle non-finite values.
Results may differ from the reference program's by a relative error of at most 0.0146932.
Values are sent between devices in bfloat16 or wider.
A program may use at most 1 GiB of HBM per device.

```python
import math
import jax
import jax.numpy as jnp
import numpy as np
from jax import lax

D = 2048
FF = 1024
HEADS = 16
KV_HEADS = 16
HEAD = 128
EXPERTS = 64
TOK_DEV = 512
CP_SIZE = 2
TP_SIZE = 4

NUM_DEVS = CP_SIZE * TP_SIZE
SEQ_LEN = TOK_DEV * NUM_DEVS
HALF_ROWS = TOK_DEV // 2
SEG_LEN = HALF_ROWS * TP_SIZE
CAPACITY = 4 * TOK_DEV // EXPERTS
Q_PER_KV = HEADS // KV_HEADS


def draw_routing(key):
    key_hot, key_src = jax.random.split(key)
    rest_cnt = 2 * TOK_DEV - 2 * CAPACITY
    base_cnt, extra_cnt = divmod(rest_cnt, EXPERTS - 2)
    counts = [CAPACITY, CAPACITY] + [base_cnt + 1] * extra_cnt + [base_cnt] * (EXPERTS - 2 - extra_cnt)
    rank_table = np.repeat(np.arange(EXPERTS), counts)
    rank_ids = jnp.asarray(rank_table).astype(jnp.int32)
    hot_pair = jnp.asarray(rank_table[:TOK_DEV] < 2).astype(jnp.int32)
    expert_perm = jax.random.permutation(key_hot, EXPERTS)

    def one_source(src_dev):
        key_perm, key_rank, key_swap = jax.random.split(jax.random.fold_in(key_src, src_dev), 3)
        cold_ids = expert_perm[2:][jax.random.permutation(key_perm, EXPERTS - 2)]
        id_table = jnp.concatenate([expert_perm[:2], cold_ids])
        choice_ids = id_table[rank_ids]
        rand_rank = jax.random.permutation(key_rank, TOK_DEV)
        pair_score = (rand_rank + hot_pair * (TOK_DEV // 2)) * TOK_DEV + rand_rank
        pair_order = jnp.argsort(pair_score)
        first_ids = choice_ids[:TOK_DEV][pair_order]
        second = choice_ids[TOK_DEV:][pair_order]
        swap_flag = jax.random.randint(key_swap, (TOK_DEV,), 0, 2) == 1
        return jnp.stack([jnp.where(swap_flag, second, first_ids), jnp.where(swap_flag, first_ids, second)], axis=1)

    return jax.vmap(one_source)(jnp.arange(NUM_DEVS)).reshape(SEQ_LEN, 2).astype(jnp.int32)


def row_positions():
    rows_all = jnp.arange(SEQ_LEN)
    dev_index = rows_all // TOK_DEV
    cp_rank = dev_index // TP_SIZE
    tp_rank = dev_index % TP_SIZE
    within = rows_all % TOK_DEV
    seg_index = jnp.where(within < HALF_ROWS, cp_rank, 2 * CP_SIZE - 1 - cp_rank)
    return seg_index * SEG_LEN + tp_rank * HALF_ROWS + within % HALF_ROWS


def setup_inputs(seed: int = 0, part: int = 0) -> dict:
    key_q, key_k, key_v, key_o, key_g, key_u, key_d = jax.random.split(jax.random.key(seed), 7)
    key_x, key_route, key_gate = jax.random.split(jax.random.fold_in(jax.random.key(seed + 1), part), 3)
    score_gain = math.sqrt(0.8 * math.log(SEQ_LEN))
    x_in = jax.random.normal(key_x, (SEQ_LEN, D), jnp.float32)
    w_q = jax.random.normal(key_q, (D, HEADS, HEAD), jnp.float32) * (score_gain / math.sqrt(D))
    w_k = jax.random.normal(key_k, (D, KV_HEADS, HEAD), jnp.float32) / math.sqrt(D)
    w_v = jax.random.normal(key_v, (D, KV_HEADS, HEAD), jnp.float32) / math.sqrt(D)
    w_o = jax.random.normal(key_o, (HEADS, HEAD, D), jnp.float32) / math.sqrt(HEADS * HEAD)
    w_gate = jax.random.normal(key_g, (EXPERTS, D, FF), jnp.float32) / math.sqrt(D)
    w_up = jax.random.normal(key_u, (EXPERTS, D, FF), jnp.float32) / math.sqrt(D)
    w_down = jax.random.normal(key_d, (EXPERTS, FF, D), jnp.float32) * (1.5 / math.sqrt(FF))
    gate_wts = jax.random.uniform(key_gate, (SEQ_LEN, 2), jnp.float32, 0.3, 0.7)
    return {'x_in': x_in.astype(jnp.bfloat16), 'w_q': w_q.astype(jnp.bfloat16), 'w_k': w_k.astype(jnp.bfloat16), 'w_v': w_v.astype(jnp.bfloat16), 'w_o': w_o.astype(jnp.bfloat16), 'expert_idx': draw_routing(key_route), 'gate_wts': gate_wts, 'w_gate': w_gate.astype(jnp.bfloat16), 'w_up': w_up.astype(jnp.bfloat16), 'w_down': w_down.astype(jnp.bfloat16)}


def reference(x_in, w_q, w_k, w_v, w_o, expert_idx, gate_wts, w_gate, w_up, w_down):
    positions = row_positions()
    queries = jnp.dot(x_in, w_q.reshape(D, HEADS * HEAD), preferred_element_type=jnp.float32).astype(jnp.bfloat16)
    keys_all = jnp.dot(x_in, w_k.reshape(D, KV_HEADS * HEAD), preferred_element_type=jnp.float32).astype(jnp.bfloat16)
    keys_all = keys_all.reshape(SEQ_LEN, KV_HEADS, HEAD).astype(jnp.float32)
    values_all = jnp.dot(x_in, w_v.reshape(D, KV_HEADS * HEAD), preferred_element_type=jnp.float32).astype(jnp.bfloat16)
    values_all = values_all.reshape(SEQ_LEN, KV_HEADS, HEAD).astype(jnp.float32)
    att_scale = 1.0 / math.sqrt(HEAD)

    def attend(q_inputs):
        q_block, q_pos = q_inputs
        scores = jnp.einsum('qngc,knc->ngqk', q_block.astype(jnp.float32), keys_all) * att_scale
        scores = jnp.where(positions[None, None, None, :] <= q_pos[None, None, :, None], scores, -jnp.inf)
        exp_scores = jnp.exp(scores - jnp.max(scores, axis=-1, keepdims=True))
        attn_prob = (exp_scores / jnp.sum(exp_scores, axis=-1, keepdims=True)).astype(jnp.bfloat16)
        head_out = jnp.einsum('ngqk,knc->qngc', attn_prob.astype(jnp.float32), values_all)
        return head_out.astype(jnp.bfloat16).reshape(TOK_DEV, HEADS * HEAD)

    head_rows = lax.map(attend, (queries.reshape(NUM_DEVS, TOK_DEV, KV_HEADS, Q_PER_KV, HEAD), positions.reshape(NUM_DEVS, TOK_DEV)))
    attn_out = jnp.dot(head_rows.reshape(SEQ_LEN, HEADS * HEAD), w_o.reshape(HEADS * HEAD, D), preferred_element_type=jnp.float32)
    hidden = (x_in.astype(jnp.float32) + attn_out).astype(jnp.bfloat16)

    flat_ids = expert_idx.reshape(NUM_DEVS, 2 * TOK_DEV)
    onehot = (flat_ids[:, :, None] == jnp.arange(EXPERTS)[None, None, :]).astype(jnp.int32)
    slot_pos = jnp.sum(jnp.cumsum(onehot, axis=1) * onehot, axis=2) - 1
    source = jnp.arange(NUM_DEVS)[:, None]
    dest_row = ((flat_ids * NUM_DEVS + source) * CAPACITY + slot_pos).reshape(-1)
    buffer = jnp.zeros((EXPERTS * NUM_DEVS * CAPACITY, D), jnp.bfloat16).at[dest_row].set(jnp.repeat(hidden, 2, axis=0))

    def expert_ffn(expert_in):
        tok_rows, gate_w, up_w, down_w = expert_in
        gate_pre = jnp.dot(tok_rows, gate_w, preferred_element_type=jnp.float32)
        up_pre = jnp.dot(tok_rows, up_w, preferred_element_type=jnp.float32)
        hid_act = (jax.nn.silu(gate_pre) * up_pre).astype(jnp.bfloat16)
        return jnp.dot(hid_act, down_w, preferred_element_type=jnp.float32).astype(jnp.bfloat16)

    expert_out = lax.map(expert_ffn, (buffer.reshape(EXPERTS, NUM_DEVS * CAPACITY, D), w_gate, w_up, w_down))
    picked = expert_out.reshape(-1, D)[dest_row].reshape(SEQ_LEN, 2, D).astype(jnp.float32)
    moe_out = jnp.sum(gate_wts[:, :, None] * picked, axis=1)
    return (hidden.astype(jnp.float32) + moe_out).astype(jnp.bfloat16)
```

```python
import functools
import math

import jax
import jax.numpy as jnp
from jax import lax
from jax.experimental import pallas as pl
from jax.experimental.pallas import tpu as pltpu
from jax.sharding import PartitionSpec as P

QB = 512


def attn_kernel(q_ref, k_ref, v_ref, o_ref, s_ref, acc_ref, *, heads, head_dim, seq):
    coef = (head_dim ** -0.5) * math.log2(math.e)
    lane = 128
    groups = QB // lane

    def lane_max(s):
        out = s[:, :lane]
        for g in range(1, groups):
            out = jnp.maximum(out, s[:, g * lane:(g + 1) * lane])
        return out

    def lane_sum(s):
        out = s[:, :lane]
        for g in range(1, groups):
            out = out + s[:, g * lane:(g + 1) * lane]
        return out

    for h in range(heads):
        cols = slice(h * head_dim, (h + 1) * head_dim)

        def q_step(i, _):
            q_rows = pl.ds(pl.multiple_of(i * QB, QB), QB)
            q = q_ref[q_rows, cols]

            def scores(j):
                k = k_ref[pl.ds(pl.multiple_of(j * QB, QB), QB), cols]
                return lax.dot_general(q, k, (((1,), (1,)), ((), ())), preferred_element_type=jnp.float32)

            def pass1(j, m):
                s = scores(j)
                s_ref[:, pl.ds(pl.multiple_of(j * QB, QB), QB)] = s
                return jnp.maximum(m, lane_max(s))

            m = lax.fori_loop(0, i, pass1, jnp.full((QB, lane), -jnp.inf, jnp.float32))
            s = scores(i)
            row = lax.broadcasted_iota(jnp.int32, (QB, QB), 0)
            col = lax.broadcasted_iota(jnp.int32, (QB, QB), 1)
            s = jnp.where(col <= row, s, -jnp.inf)
            s_ref[:, pl.ds(pl.multiple_of(i * QB, QB), QB)] = s
            m = jnp.max(jnp.maximum(m, lane_max(s)), axis=1, keepdims=True)
            acc_ref[...] = jnp.zeros_like(acc_ref)

            def pass2(j, l):
                s = s_ref[:, pl.ds(pl.multiple_of(j * QB, QB), QB)]
                e = jnp.exp2((s - m) * coef)
                v = v_ref[pl.ds(pl.multiple_of(j * QB, QB), QB), cols]
                acc_ref[...] += lax.dot_general(e.astype(jnp.bfloat16), v, (((1,), (0,)), ((), ())), preferred_element_type=jnp.float32)
                return l + lane_sum(e)

            l = lax.fori_loop(0, i + 1, pass2, jnp.zeros((QB, lane), jnp.float32))
            l = jnp.sum(l, axis=1, keepdims=True)
            o_ref[q_rows, cols] = (acc_ref[...] / l).astype(jnp.bfloat16)
            return 0

        lax.fori_loop(0, seq // QB, q_step, 0)


def attention(q, k, v, heads, head_dim):
    seq = q.shape[0]
    vm = pl.BlockSpec(memory_space=pltpu.VMEM)
    return pl.pallas_call(
        functools.partial(attn_kernel, heads=heads, head_dim=head_dim, seq=seq),
        out_shape=jax.ShapeDtypeStruct(q.shape, jnp.bfloat16),
        in_specs=[vm] * 3,
        out_specs=vm,
        scratch_shapes=[pltpu.VMEM((QB, seq), jnp.float32), pltpu.VMEM((QB, head_dim), jnp.float32)],
        compiler_params=pltpu.CompilerParams(vmem_limit_bytes=60 * 1024 * 1024),
        cost_estimate=pl.CostEstimate(flops=2 * heads * seq * seq * head_dim, bytes_accessed=4 * 2 * q.size, transcendentals=heads * seq * seq // 2),
    )(q, k, v)


def solution(mesh):
    cp_size = mesh.shape['cp']
    tp_size = mesh.shape['tp']
    num_devs = cp_size * tp_size
    row_spec = P(('data', 'cp', 'tp'), None)
    head_spec = P(None, 'tp', None)
    wo_spec = P('tp', None, None)
    expert_spec = P(('cp', 'tp'), None, None)

    def to_positions(rows, half):
        blocks = rows.reshape(cp_size, tp_size, 2, half, rows.shape[-1])
        return jnp.concatenate([blocks[:, :, 0], blocks[::-1, :, 1]], axis=0).reshape(rows.shape)

    def from_positions(rows, half):
        blocks = rows.reshape(2 * cp_size, tp_size, half, rows.shape[-1])
        return jnp.stack([blocks[:cp_size], blocks[cp_size:][::-1]], axis=2).reshape(rows.shape)

    def device_fn(x_blk, w_q, w_k, w_v, w_o, idx_blk, gate_blk, w_gate, w_up, w_down):
        tok_dev, d_model = x_blk.shape
        half = tok_dev // 2
        heads_tp, head_dim = w_q.shape[1], w_q.shape[2]
        heads = heads_tp // cp_size
        width = heads * head_dim
        exp_local = w_gate.shape[0]
        num_exp = exp_local * num_devs
        capacity = 4 * tok_dev // num_exp
        cp_rank = lax.axis_index('cp')

        x_all = lax.all_gather(x_blk, ('cp', 'tp'), axis=0, tiled=True)
        wo_all = lax.all_gather(w_o, 'tp', axis=0, tiled=True).reshape(-1, d_model)
        w_qkv = jnp.concatenate([lax.dynamic_slice_in_dim(w, cp_rank * heads, heads, 1).reshape(d_model, width) for w in (w_q, w_k, w_v)], axis=1)
        qkv = jnp.dot(x_all, w_qkv, preferred_element_type=jnp.float32).astype(jnp.bfloat16)
        qkv = to_positions(qkv, half)
        o = attention(qkv[:, :width], qkv[:, width:2 * width], qkv[:, 2 * width:], heads, head_dim)
        o = from_positions(o, half)
        o = lax.all_to_all(o, ('cp', 'tp'), 0, 0, tiled=True)
        o = o.reshape(cp_size, tp_size, tok_dev, width).transpose(2, 1, 0, 3).reshape(tok_dev, -1)
        attn_out = jnp.dot(o, wo_all, preferred_element_type=jnp.float32)
        hidden = (x_blk.astype(jnp.float32) + attn_out).astype(jnp.bfloat16)

        flat_ids = idx_blk.reshape(-1)
        num_flat = flat_ids.shape[0]
        onehot = (flat_ids[:, None] == jnp.arange(num_exp)[None, :])
        before = (jnp.arange(num_flat)[:, None] > jnp.arange(num_flat)[None, :]).astype(jnp.bfloat16)
        ranks = jnp.dot(before, onehot.astype(jnp.bfloat16), preferred_element_type=jnp.float32)
        slot_pos = jnp.sum(jnp.where(onehot, ranks, 0.0), axis=1).astype(jnp.int32)
        slot_ids = (flat_ids * capacity + slot_pos).reshape(tok_dev, 2)
        select = (slot_ids[:, :, None] == jnp.arange(num_exp * capacity)[None, None, :]).astype(jnp.bfloat16)
        send_buf = jnp.einsum('tkn,tm->nm', select, hidden, preferred_element_type=jnp.float32).astype(jnp.bfloat16)
        recv_buf = lax.all_to_all(send_buf, ('cp', 'tp'), 0, 0, tiled=True)
        tok_in = recv_buf.reshape(num_devs, exp_local, capacity, -1)
        gate_pre = jnp.einsum('secm,emf->secf', tok_in, w_gate, preferred_element_type=jnp.float32)
        up_pre = jnp.einsum('secm,emf->secf', tok_in, w_up, preferred_element_type=jnp.float32)
        hid_act = (jax.nn.silu(gate_pre) * up_pre).astype(jnp.bfloat16)
        exp_out = jnp.einsum('secf,efm->secm', hid_act, w_down, preferred_element_type=jnp.float32).astype(jnp.bfloat16)
        back_buf = lax.all_to_all(exp_out.reshape(num_devs * exp_local * capacity, -1), ('cp', 'tp'), 0, 0, tiled=True)
        picked = jnp.einsum('tkn,nm->tkm', select, back_buf, preferred_element_type=jnp.float32)
        moe_out = jnp.sum(gate_blk[:, :, None] * picked, axis=1)
        return (hidden.astype(jnp.float32) + moe_out).astype(jnp.bfloat16)

    return jax.shard_map(device_fn, mesh=mesh, in_specs=(row_spec, head_spec, head_spec, head_spec, wo_spec, row_spec, row_spec, expert_spec, expert_spec, expert_spec), out_specs=row_spec, check_vma=False)
```

```python
import functools
import math

import jax
import jax.numpy as jnp
from jax import lax
from jax.experimental import pallas as pl
from jax.experimental.pallas import tpu as pltpu
from jax.sharding import PartitionSpec as P

MESH = pl.DeviceIdType.MESH
MIB = 1024 * 1024
QB = 512


def lane_fold(s, op):
    out = s[:, :128]
    for g in range(1, s.shape[1] // 128):
        out = op(out, s[:, g * 128:(g + 1) * 128])
    return out


def attn_block(x_hbm, wqkv_ref, wo_hbm, h_ref, xbuf, qkv, s_ref, acc_ref, o_loc, o_cat, wo_buf,
               loc_sem, xs, xr, ws, wr, os_sem, or_sem, *, heads, head_dim):
    cp, tp = lax.axis_index('cp'), lax.axis_index('tp')
    xx, cc = tp // 2, tp % 2
    me = cp * 4 + tp
    ndev, rows, d_model = xbuf.shape
    half_rows = rows // 2
    quarter = half_rows // 2
    width = heads * head_dim
    seq = ndev * rows
    wrows = wo_hbm.shape[0]
    whalf, wquart = wrows // 2, wrows // 4

    def tp_of(dx, dc):
        return ((xx + dx) % 2) * 2 + (cc + dc) % 2

    def idx(dx, dy, dc):
        return ((cp + dy) % 2) * 4 + tp_of(dx, dc)

    def dev(dx, dy, dc):
        return {'cp': (cp + dy) % 2, 'tp': tp_of(dx, dc)}

    XN, YN, CN, DG = (1, 0, 0), (0, 1, 0), (0, 0, 1), (1, 1, 0)
    XC, YC, DC = (1, 0, 1), (0, 1, 1), (1, 1, 1)

    x_load = pltpu.make_async_copy(x_hbm, xbuf.at[me], loc_sem.at[0])
    wo_load = pltpu.make_async_copy(wo_hbm, wo_buf.at[pl.ds(tp * wrows, wrows)], loc_sem.at[1])
    x_load.start()
    wo_load.start()

    barrier = pltpu.get_barrier_semaphore()
    for k in range(1, ndev):
        peer = (me + k) % ndev
        pl.semaphore_signal(barrier, inc=1, device_id={'cp': peer // 4, 'tp': peer % 4}, device_id_type=MESH)
    pl.semaphore_wait(barrier, ndev - 1)

    def xcopy(slot, owner, row0, count, part, target):
        ref = xbuf.at[idx(*owner), pl.ds(row0, count)]
        return pltpu.make_async_remote_copy(src_ref=ref, dst_ref=ref, send_sem=xs.at[slot], recv_sem=xr.at[idx(*owner), part], device_id=dev(*target), device_id_type=MESH)

    sent = []

    def send(*args):
        copy = xcopy(*args)
        copy.start()
        sent.append(copy)

    def arrive(owner, row0, count, part):
        xcopy(0, owner, row0, count, part, CN).wait_recv()

    def wcopy(slot, shard, row0, count, sem, target):
        ref = wo_buf.at[pl.ds(shard * wrows + row0, count)]
        return pltpu.make_async_remote_copy(src_ref=ref, dst_ref=ref, send_sem=ws.at[slot], recv_sem=wr.at[sem], device_id=dev(*target), device_id_type=MESH)

    own = (0, 0, 0)
    x_load.wait()
    for half in range(2):
        send(0 + half, own, half * half_rows, half_rows, 2 * half, XN)
        send(2 + half, own, half * half_rows, half_rows, 2 * half, YN)
        send(4 + half, own, half * half_rows, half_rows, 2 * half, CN)
    wo_load.wait()
    w_own = wcopy(0, tp, 0, wrows, 0, CN)
    w_own.start()

    def project(owner, half):
        r, t = owner // 4, owner % 4
        seg = r + half * (3 - 2 * r)
        x = xbuf[owner, pl.ds(pl.multiple_of(half * half_rows, half_rows), half_rows), :]
        out = jnp.dot(x, wqkv_ref[...], preferred_element_type=jnp.float32).astype(jnp.bfloat16)
        qkv[pl.ds(pl.multiple_of((seg * 4 + t) * half_rows, half_rows), half_rows), :] = out

    def near(s, _):
        @pl.when(s == 2)
        def _():
            arrive(CN, 0, half_rows, 0)

        @pl.when(s == 3)
        def _():
            arrive(CN, half_rows, half_rows, 2)

        project(idx(0, 0, s // 2), s % 2)
        return 0

    lax.fori_loop(0, 4, near, 0)

    for half in range(2):
        base = half * half_rows
        arrive(XN, base, half_rows, 2 * half)
        send(6 + half, XN, base, half_rows, 2 * half, CN)
        send(12 + half, XN, base + quarter, quarter, 2 * half + 1, YN)
        arrive(YN, base, half_rows, 2 * half)
        send(8 + half, YN, base, half_rows, 2 * half, CN)
        send(10 + half, YN, base, quarter, 2 * half, XN)

        def mid(u, _):
            @pl.when(u == 2)
            def _():
                arrive(XC, base, half_rows, 2 * half)

            @pl.when(u == 3)
            def _():
                arrive(YC, base, half_rows, 2 * half)

            project(idx(1 - u % 2, u % 2, u // 2), half)
            return 0

        lax.fori_loop(0, 4, mid, 0)

    w_x = [wcopy(1 + k, tp, cp * whalf + k * wquart, wquart, 1 + k, XN) for k in range(2)]
    for copy in w_x:
        copy.start()

    for half in range(2):
        base = half * half_rows
        arrive(DG, base, quarter, 2 * half)
        arrive(DG, base + quarter, quarter, 2 * half + 1)
        send(14 + half, DG, base, half_rows, 2 * half, CN)

        def far(u, _):
            @pl.when(u == 1)
            def _():
                arrive(DC, base, half_rows, 2 * half)

            project(idx(1, 1, u), half)
            return 0

        lax.fori_loop(0, 2, far, 0)

    coef = (head_dim ** -0.5) * math.log2(math.e)
    my_col = (4 * tp + 2 * cp) * head_dim

    def o_place(b):
        seg, t = b // 4, b % 4
        half = seg // 2
        return seg + half * (3 - 2 * seg), t, half

    def o_remote(b):
        r, t, half = o_place(b)
        return pltpu.make_async_remote_copy(
            src_ref=o_loc.at[pl.ds(pl.multiple_of(b * half_rows, half_rows), half_rows)],
            dst_ref=o_cat.at[pl.ds(pl.multiple_of(half * half_rows, half_rows), half_rows), pl.ds(pl.multiple_of(my_col, width), width)],
            send_sem=os_sem.at[b], recv_sem=or_sem.at[me, half], device_id={'cp': r, 'tp': t}, device_id_type=MESH)

    def o_local(b):
        _, _, half = o_place(b)
        return pltpu.make_async_copy(
            o_loc.at[pl.ds(pl.multiple_of(b * half_rows, half_rows), half_rows)],
            o_cat.at[pl.ds(pl.multiple_of(half * half_rows, half_rows), half_rows), pl.ds(pl.multiple_of(my_col, width), width)],
            os_sem.at[b])

    def o_send(i):
        for part in range(QB // half_rows):
            b = i * (QB // half_rows) + part
            r, t, _ = o_place(b)

            @pl.when(r * 4 + t != me)
            def _():
                o_remote(b).start()

            @pl.when(r * 4 + t == me)
            def _():
                o_local(b).start()

    peer_t = tp_of(1, 0)
    peer_c = tp_of(1, 1)

    def w_pass(k):
        wcopy(1, peer_t, cp * whalf + k * wquart, wquart, 1 + k, CN).wait_recv()
        wcopy(3 + k, peer_t, cp * whalf + k * wquart, wquart, 3 + k, YN).start()
        wcopy(5 + k, peer_t, cp * whalf + k * wquart, wquart, 5 + k, CN).start()

    def w_last(k):
        wcopy(1, peer_t, (1 - cp) * whalf + k * wquart, wquart, 3 + k, CN).wait_recv()
        wcopy(7 + k, peer_t, (1 - cp) * whalf + k * wquart, wquart, 7 + k, CN).start()

    blocks = seq // QB

    def q_step(i, _):
        @pl.when(i == blocks - 3)
        def _():
            w_pass(0)

        @pl.when(i == blocks - 2)
        def _():
            w_pass(1)

        @pl.when(i == blocks - 1)
        def _():
            w_last(0)

        q_rows = pl.ds(pl.multiple_of(i * QB, QB), QB)

        def cols(kind, h):
            return slice(kind * width + h * head_dim, kind * width + (h + 1) * head_dim)

        def scores(h, j):
            k = qkv[pl.ds(pl.multiple_of(j * QB, QB), QB), cols(1, h)]
            return lax.dot_general(qkv[q_rows, cols(0, h)], k, (((1,), (1,)), ((), ())), preferred_element_type=jnp.float32)

        def pass1(j, ms):
            out = []
            for h in range(heads):
                s = scores(h, j)
                s_ref[h, :, pl.ds(pl.multiple_of(j * QB, QB), QB)] = s
                out.append(jnp.maximum(ms[h], lane_fold(s, jnp.maximum)))
            return tuple(out)

        ms = lax.fori_loop(0, i, pass1, tuple(jnp.full((QB, 128), -jnp.inf, jnp.float32) for _ in range(heads)))
        keep = lax.broadcasted_iota(jnp.int32, (QB, QB), 1) <= lax.broadcasted_iota(jnp.int32, (QB, QB), 0)
        tops = []
        for h in range(heads):
            s = jnp.where(keep, scores(h, i), -jnp.inf)
            s_ref[h, :, pl.ds(pl.multiple_of(i * QB, QB), QB)] = s
            tops.append(jnp.max(jnp.maximum(ms[h], lane_fold(s, jnp.maximum)), axis=1, keepdims=True))
        acc_ref[...] = jnp.zeros_like(acc_ref)

        def pass2(j, ls):
            out = []
            for h in range(heads):
                e = jnp.exp2((s_ref[h, :, pl.ds(pl.multiple_of(j * QB, QB), QB)] - tops[h]) * coef)
                v = qkv[pl.ds(pl.multiple_of(j * QB, QB), QB), cols(2, h)]
                acc_ref[h] += jnp.dot(e.astype(jnp.bfloat16), v, preferred_element_type=jnp.float32)
                out.append(ls[h] + lane_fold(e, jnp.add))
            return tuple(out)

        ls = lax.fori_loop(0, i + 1, pass2, tuple(jnp.zeros((QB, 128), jnp.float32) for _ in range(heads)))
        for h in range(heads):
            total = jnp.sum(ls[h], axis=1, keepdims=True)
            o_loc[q_rows, h * head_dim:(h + 1) * head_dim] = (acc_ref[h] / total).astype(jnp.bfloat16)
        o_send(i)
        return 0

    lax.fori_loop(0, blocks, q_step, 0)

    w_last(1)
    wcopy(1, tp_of(0, 1), 0, wrows, 0, CN).wait_recv()
    for k in range(2):
        wcopy(1, peer_c, cp * whalf + k * wquart, wquart, 5 + k, CN).wait_recv()
        wcopy(1, peer_c, (1 - cp) * whalf + k * wquart, wquart, 7 + k, CN).wait_recv()
    for k in range(1, ndev):
        src = (me + k) % ndev
        col = (4 * (src % 4) + 2 * (src // 4)) * head_dim
        for half in range(2):
            ref = o_cat.at[pl.ds(half * half_rows, half_rows), pl.ds(pl.multiple_of(col, width), width)]
            pltpu.make_async_remote_copy(src_ref=ref, dst_ref=ref, send_sem=os_sem.at[0], recv_sem=or_sem.at[src, half], device_id=dev(0, 0, 1), device_id_type=MESH).wait_recv()

    def drain(b, _):
        r, t, _half = o_place(b)

        @pl.when(r * 4 + t != me)
        def _():
            o_remote(b).wait_send()

        @pl.when(r * 4 + t == me)
        def _():
            o_local(b).wait()

        return 0

    lax.fori_loop(0, seq // half_rows, drain, 0)

    tile = 256

    def out_step(n, _):
        c = pl.ds(pl.multiple_of(n * tile, tile), tile)
        a = jnp.dot(o_cat[...], wo_buf[:, c], preferred_element_type=jnp.float32)
        h_ref[:, c] = (xbuf[me, :, c].astype(jnp.float32) + a).astype(jnp.bfloat16)
        return 0

    lax.fori_loop(0, d_model // tile, out_step, 0)

    for copy in sent:
        copy.wait_send()
    w_own.wait_send()
    for copy in w_x:
        copy.wait_send()
    for k in range(2):
        wcopy(3 + k, peer_t, cp * whalf + k * wquart, wquart, 3 + k, YN).wait_send()
        wcopy(5 + k, peer_t, cp * whalf + k * wquart, wquart, 5 + k, CN).wait_send()
        wcopy(7 + k, peer_t, (1 - cp) * whalf + k * wquart, wquart, 7 + k, CN).wait_send()


def attention_block(x_blk, w_qkv, w_o, heads, head_dim, ndev):
    rows, d_model = x_blk.shape
    seq = rows * ndev
    width = heads * head_dim
    vm = pl.BlockSpec(memory_space=pltpu.VMEM)
    hbm = pl.BlockSpec(memory_space=pl.ANY)
    bf16, f32 = jnp.bfloat16, jnp.float32
    dma = pltpu.SemaphoreType.DMA
    return pl.pallas_call(
        functools.partial(attn_block, heads=heads, head_dim=head_dim),
        name='attn_block',
        out_shape=jax.ShapeDtypeStruct((rows, d_model), bf16),
        in_specs=[hbm, vm, hbm],
        out_specs=vm,
        scratch_shapes=[
            pltpu.VMEM((ndev, rows, d_model), bf16), pltpu.VMEM((seq, 3 * width), bf16),
            pltpu.VMEM((heads, QB, seq), f32), pltpu.VMEM((heads, QB, head_dim), f32),
            pltpu.VMEM((seq, width), bf16), pltpu.VMEM((rows, ndev * width), bf16),
            pltpu.VMEM((ndev * width, d_model), bf16),
            dma((2,)), dma((16,)), dma((ndev, 4)), dma((9,)), dma((9,)), dma((16,)), dma((ndev, 2)),
        ],
        compiler_params=pltpu.CompilerParams(collective_id=0, has_side_effects=True, vmem_limit_bytes=63 * MIB),
        cost_estimate=pl.CostEstimate(flops=2 * seq * d_model * width * 3 + 4 * seq * seq * width, bytes_accessed=16 * MIB, transcendentals=0),
    )(x_blk, w_qkv, w_o)


def solution(mesh):
    cp_size = mesh.shape['cp']
    tp_size = mesh.shape['tp']
    num_devs = cp_size * tp_size
    row_spec = P(('data', 'cp', 'tp'), None)
    head_spec = P(None, 'tp', None)
    wo_spec = P('tp', None, None)
    expert_spec = P(('cp', 'tp'), None, None)

    def device_fn(x_blk, w_q, w_k, w_v, w_o, idx_blk, gate_blk, w_gate, w_up, w_down):
        tok_dev, d_model = x_blk.shape
        heads_tp, head_dim = w_q.shape[1], w_q.shape[2]
        heads = heads_tp // cp_size
        width = heads * head_dim
        exp_local = w_gate.shape[0]
        num_exp = exp_local * num_devs
        capacity = 4 * tok_dev // num_exp
        cp_rank = lax.axis_index('cp')

        w_qkv = jnp.concatenate([lax.dynamic_slice_in_dim(w, cp_rank * heads, heads, 1).reshape(d_model, width) for w in (w_q, w_k, w_v)], axis=1)
        hidden = attention_block(x_blk, w_qkv, w_o.reshape(-1, d_model), heads, head_dim, num_devs)

        flat_ids = idx_blk.reshape(-1)
        num_flat = flat_ids.shape[0]
        onehot = (flat_ids[:, None] == jnp.arange(num_exp)[None, :])
        before = (jnp.arange(num_flat)[:, None] > jnp.arange(num_flat)[None, :]).astype(jnp.bfloat16)
        ranks = jnp.dot(before, onehot.astype(jnp.bfloat16), preferred_element_type=jnp.float32)
        slot_pos = jnp.sum(jnp.where(onehot, ranks, 0.0), axis=1).astype(jnp.int32)
        slot_ids = (flat_ids * capacity + slot_pos).reshape(tok_dev, 2)
        select = (slot_ids[:, :, None] == jnp.arange(num_exp * capacity)[None, None, :]).astype(jnp.bfloat16)
        send_buf = jnp.einsum('tkn,tm->nm', select, hidden, preferred_element_type=jnp.float32).astype(jnp.bfloat16)
        recv_buf = lax.all_to_all(send_buf, ('cp', 'tp'), 0, 0, tiled=True)
        tok_in = recv_buf.reshape(num_devs, exp_local, capacity, -1)
        gate_pre = jnp.einsum('secm,emf->secf', tok_in, w_gate, preferred_element_type=jnp.float32)
        up_pre = jnp.einsum('secm,emf->secf', tok_in, w_up, preferred_element_type=jnp.float32)
        hid_act = (jax.nn.silu(gate_pre) * up_pre).astype(jnp.bfloat16)
        exp_out = jnp.einsum('secf,efm->secm', hid_act, w_down, preferred_element_type=jnp.float32).astype(jnp.bfloat16)
        back_buf = lax.all_to_all(exp_out.reshape(num_devs * exp_local * capacity, -1), ('cp', 'tp'), 0, 0, tiled=True)
        picked = jnp.einsum('tkn,nm->tkm', select, back_buf, preferred_element_type=jnp.float32)
        moe_out = jnp.sum(gate_blk[:, :, None] * picked, axis=1)
        return (hidden.astype(jnp.float32) + moe_out).astype(jnp.bfloat16)

    return jax.shard_map(device_fn, mesh=mesh, in_specs=(row_spec, head_spec, head_spec, head_spec, wo_spec, row_spec, row_spec, expert_spec, expert_spec, expert_spec), out_specs=row_spec, check_vma=False)
```

```python
import functools
import math

import jax
import jax.numpy as jnp
from jax import lax
from jax.experimental import pallas as pl
from jax.experimental.pallas import tpu as pltpu
from jax.sharding import PartitionSpec as P

MESH = pl.DeviceIdType.MESH
MIB = 1024 * 1024
QB = 512


def lane_fold(s, op):
    out = s[:, :128]
    for g in range(1, s.shape[1] // 128):
        out = op(out, s[:, g * 128:(g + 1) * 128])
    return out


def attn_block(x_hbm, wqkv_ref, wo_hbm, flag_ref, h_ref, any_ref, xbuf, qkv, s_ref, acc_ref, o_loc, o_cat, wo_buf,
               flags, loc_sem, xs, xr, ws, wr, os_sem, or_sem, fs, fr, *, heads, head_dim):
    cp, tp = lax.axis_index('cp'), lax.axis_index('tp')
    xx, cc = tp // 2, tp % 2
    me = cp * 4 + tp
    ndev, rows, d_model = xbuf.shape
    half_rows = rows // 2
    quarter = half_rows // 2
    width = heads * head_dim
    seq = ndev * rows
    wrows = wo_hbm.shape[0]
    whalf, wquart = wrows // 2, wrows // 4

    def tp_of(dx, dc):
        return ((xx + dx) % 2) * 2 + (cc + dc) % 2

    def idx(dx, dy, dc):
        return ((cp + dy) % 2) * 4 + tp_of(dx, dc)

    def dev(dx, dy, dc):
        return {'cp': (cp + dy) % 2, 'tp': tp_of(dx, dc)}

    XN, YN, CN, DG = (1, 0, 0), (0, 1, 0), (0, 0, 1), (1, 1, 0)
    XC, YC, DC = (1, 0, 1), (0, 1, 1), (1, 1, 1)

    x_load = pltpu.make_async_copy(x_hbm, xbuf.at[me], loc_sem.at[0])
    wo_load = pltpu.make_async_copy(wo_hbm, wo_buf.at[pl.ds(tp * wrows, wrows)], loc_sem.at[1])
    x_load.start()
    wo_load.start()

    barrier = pltpu.get_barrier_semaphore()
    for k in range(1, ndev):
        peer = (me + k) % ndev
        pl.semaphore_signal(barrier, inc=1, device_id={'cp': peer // 4, 'tp': peer % 4}, device_id_type=MESH)
    pl.semaphore_wait(barrier, ndev - 1)

    def xcopy(slot, owner, row0, count, part, target):
        ref = xbuf.at[idx(*owner), pl.ds(row0, count)]
        return pltpu.make_async_remote_copy(src_ref=ref, dst_ref=ref, send_sem=xs.at[slot], recv_sem=xr.at[idx(*owner), part], device_id=dev(*target), device_id_type=MESH)

    sent = []

    def send(*args):
        copy = xcopy(*args)
        copy.start()
        sent.append(copy)

    def arrive(owner, row0, count, part):
        xcopy(0, owner, row0, count, part, CN).wait_recv()

    def wcopy(slot, shard, row0, count, sem, target):
        ref = wo_buf.at[pl.ds(shard * wrows + row0, count)]
        return pltpu.make_async_remote_copy(src_ref=ref, dst_ref=ref, send_sem=ws.at[slot], recv_sem=wr.at[sem], device_id=dev(*target), device_id_type=MESH)

    def flag_copy(j):
        peer = (me + j) % ndev
        return pltpu.make_async_remote_copy(src_ref=flag_ref, dst_ref=flags.at[me], send_sem=fs.at[j], recv_sem=fr.at[me], device_id={'cp': peer // 4, 'tp': peer % 4}, device_id_type=MESH)

    for j in range(1, ndev):
        flag_copy(j).start()

    own = (0, 0, 0)
    x_load.wait()
    for half in range(2):
        send(0 + half, own, half * half_rows, half_rows, 2 * half, XN)
        send(2 + half, own, half * half_rows, half_rows, 2 * half, YN)
        send(4 + half, own, half * half_rows, half_rows, 2 * half, CN)
    wo_load.wait()
    w_own = wcopy(0, tp, 0, wrows, 0, CN)
    w_own.start()

    def project(owner, half):
        r, t = owner // 4, owner % 4
        seg = r + half * (3 - 2 * r)
        x = xbuf[owner, pl.ds(pl.multiple_of(half * half_rows, half_rows), half_rows), :]
        out = jnp.dot(x, wqkv_ref[...], preferred_element_type=jnp.float32).astype(jnp.bfloat16)
        qkv[pl.ds(pl.multiple_of((seg * 4 + t) * half_rows, half_rows), half_rows), :] = out

    def near(s, _):
        @pl.when(s == 2)
        def _():
            arrive(CN, 0, half_rows, 0)

        @pl.when(s == 3)
        def _():
            arrive(CN, half_rows, half_rows, 2)

        project(idx(0, 0, s // 2), s % 2)
        return 0

    lax.fori_loop(0, 4, near, 0)

    for half in range(2):
        base = half * half_rows
        arrive(XN, base, half_rows, 2 * half)
        send(6 + half, XN, base, half_rows, 2 * half, CN)
        send(12 + half, XN, base + quarter, quarter, 2 * half + 1, YN)
        arrive(YN, base, half_rows, 2 * half)
        send(8 + half, YN, base, half_rows, 2 * half, CN)
        send(10 + half, YN, base, quarter, 2 * half, XN)

        def mid(u, _):
            @pl.when(u == 2)
            def _():
                arrive(XC, base, half_rows, 2 * half)

            @pl.when(u == 3)
            def _():
                arrive(YC, base, half_rows, 2 * half)

            project(idx(1 - u % 2, u % 2, u // 2), half)
            return 0

        lax.fori_loop(0, 4, mid, 0)

    w_x = [wcopy(1 + k, tp, cp * whalf + k * wquart, wquart, 1 + k, XN) for k in range(2)]
    for copy in w_x:
        copy.start()

    for half in range(2):
        base = half * half_rows
        arrive(DG, base, quarter, 2 * half)
        arrive(DG, base + quarter, quarter, 2 * half + 1)
        send(14 + half, DG, base, half_rows, 2 * half, CN)

        def far(u, _):
            @pl.when(u == 1)
            def _():
                arrive(DC, base, half_rows, 2 * half)

            project(idx(1, 1, u), half)
            return 0

        lax.fori_loop(0, 2, far, 0)

    coef = (head_dim ** -0.5) * math.log2(math.e)
    my_col = (4 * tp + 2 * cp) * head_dim

    def o_place(b):
        seg, t = b // 4, b % 4
        half = seg // 2
        return seg + half * (3 - 2 * seg), t, half

    def o_remote(b):
        r, t, half = o_place(b)
        return pltpu.make_async_remote_copy(
            src_ref=o_loc.at[pl.ds(pl.multiple_of(b * half_rows, half_rows), half_rows)],
            dst_ref=o_cat.at[pl.ds(pl.multiple_of(half * half_rows, half_rows), half_rows), pl.ds(pl.multiple_of(my_col, width), width)],
            send_sem=os_sem.at[b], recv_sem=or_sem.at[me, half], device_id={'cp': r, 'tp': t}, device_id_type=MESH)

    def o_local(b):
        _, _, half = o_place(b)
        return pltpu.make_async_copy(
            o_loc.at[pl.ds(pl.multiple_of(b * half_rows, half_rows), half_rows)],
            o_cat.at[pl.ds(pl.multiple_of(half * half_rows, half_rows), half_rows), pl.ds(pl.multiple_of(my_col, width), width)],
            os_sem.at[b])

    def o_send(i):
        for part in range(QB // half_rows):
            b = i * (QB // half_rows) + part
            r, t, _ = o_place(b)

            @pl.when(r * 4 + t != me)
            def _():
                o_remote(b).start()

            @pl.when(r * 4 + t == me)
            def _():
                o_local(b).start()

    peer_t = tp_of(1, 0)
    peer_c = tp_of(1, 1)

    def w_pass(k):
        wcopy(1, peer_t, cp * whalf + k * wquart, wquart, 1 + k, CN).wait_recv()
        wcopy(3 + k, peer_t, cp * whalf + k * wquart, wquart, 3 + k, YN).start()
        wcopy(5 + k, peer_t, cp * whalf + k * wquart, wquart, 5 + k, CN).start()

    def w_last(k):
        wcopy(1, peer_t, (1 - cp) * whalf + k * wquart, wquart, 3 + k, CN).wait_recv()
        wcopy(7 + k, peer_t, (1 - cp) * whalf + k * wquart, wquart, 7 + k, CN).start()

    blocks = seq // QB

    def q_step(i, _):
        @pl.when(i == blocks - 3)
        def _():
            w_pass(0)

        @pl.when(i == blocks - 2)
        def _():
            w_pass(1)

        @pl.when(i == blocks - 1)
        def _():
            w_last(0)

        q_rows = pl.ds(pl.multiple_of(i * QB, QB), QB)

        def cols(kind, h):
            return slice(kind * width + h * head_dim, kind * width + (h + 1) * head_dim)

        def scores(h, j):
            k = qkv[pl.ds(pl.multiple_of(j * QB, QB), QB), cols(1, h)]
            return lax.dot_general(qkv[q_rows, cols(0, h)], k, (((1,), (1,)), ((), ())), preferred_element_type=jnp.float32)

        def pass1(j, ms):
            out = []
            for h in range(heads):
                s = scores(h, j)
                s_ref[h, :, pl.ds(pl.multiple_of(j * QB, QB), QB)] = s
                out.append(jnp.maximum(ms[h], lane_fold(s, jnp.maximum)))
            return tuple(out)

        ms = lax.fori_loop(0, i, pass1, tuple(jnp.full((QB, 128), -jnp.inf, jnp.float32) for _ in range(heads)))
        keep = lax.broadcasted_iota(jnp.int32, (QB, QB), 1) <= lax.broadcasted_iota(jnp.int32, (QB, QB), 0)
        tops = []
        for h in range(heads):
            s = jnp.where(keep, scores(h, i), -jnp.inf)
            s_ref[h, :, pl.ds(pl.multiple_of(i * QB, QB), QB)] = s
            tops.append(jnp.max(jnp.maximum(ms[h], lane_fold(s, jnp.maximum)), axis=1, keepdims=True))
        acc_ref[...] = jnp.zeros_like(acc_ref)

        def pass2(j, ls):
            out = []
            for h in range(heads):
                e = jnp.exp2((s_ref[h, :, pl.ds(pl.multiple_of(j * QB, QB), QB)] - tops[h]) * coef)
                v = qkv[pl.ds(pl.multiple_of(j * QB, QB), QB), cols(2, h)]
                acc_ref[h] += jnp.dot(e.astype(jnp.bfloat16), v, preferred_element_type=jnp.float32)
                out.append(ls[h] + lane_fold(e, jnp.add))
            return tuple(out)

        ls = lax.fori_loop(0, i + 1, pass2, tuple(jnp.zeros((QB, 128), jnp.float32) for _ in range(heads)))
        for h in range(heads):
            total = jnp.sum(ls[h], axis=1, keepdims=True)
            o_loc[q_rows, h * head_dim:(h + 1) * head_dim] = (acc_ref[h] / total).astype(jnp.bfloat16)
        o_send(i)
        return 0

    lax.fori_loop(0, blocks, q_step, 0)

    w_last(1)
    wcopy(1, tp_of(0, 1), 0, wrows, 0, CN).wait_recv()
    for k in range(2):
        wcopy(1, peer_c, cp * whalf + k * wquart, wquart, 5 + k, CN).wait_recv()
        wcopy(1, peer_c, (1 - cp) * whalf + k * wquart, wquart, 7 + k, CN).wait_recv()
    for k in range(1, ndev):
        src = (me + k) % ndev
        col = (4 * (src % 4) + 2 * (src // 4)) * head_dim
        for half in range(2):
            ref = o_cat.at[pl.ds(half * half_rows, half_rows), pl.ds(pl.multiple_of(col, width), width)]
            pltpu.make_async_remote_copy(src_ref=ref, dst_ref=ref, send_sem=os_sem.at[0], recv_sem=or_sem.at[src, half], device_id=dev(0, 0, 1), device_id_type=MESH).wait_recv()

    def drain(b, _):
        r, t, _half = o_place(b)

        @pl.when(r * 4 + t != me)
        def _():
            o_remote(b).wait_send()

        @pl.when(r * 4 + t == me)
        def _():
            o_local(b).wait()

        return 0

    lax.fori_loop(0, seq // half_rows, drain, 0)

    tile = 256

    def out_step(n, _):
        c = pl.ds(pl.multiple_of(n * tile, tile), tile)
        a = jnp.dot(o_cat[...], wo_buf[:, c], preferred_element_type=jnp.float32)
        h_ref[:, c] = (xbuf[me, :, c].astype(jnp.float32) + a).astype(jnp.bfloat16)
        return 0

    lax.fori_loop(0, d_model // tile, out_step, 0)

    most = flag_ref[...]
    for j in range(1, ndev):
        peer = (me + j) % ndev
        pltpu.make_async_remote_copy(src_ref=flag_ref, dst_ref=flags.at[peer], send_sem=fs.at[j], recv_sem=fr.at[peer], device_id=dev(0, 0, 1), device_id_type=MESH).wait_recv()
        most = jnp.maximum(most, flags[peer])
        flag_copy(j).wait_send()
    any_ref[...] = most

    for copy in sent:
        copy.wait_send()
    w_own.wait_send()
    for copy in w_x:
        copy.wait_send()
    for k in range(2):
        wcopy(3 + k, peer_t, cp * whalf + k * wquart, wquart, 3 + k, YN).wait_send()
        wcopy(5 + k, peer_t, cp * whalf + k * wquart, wquart, 5 + k, CN).wait_send()
        wcopy(7 + k, peer_t, (1 - cp) * whalf + k * wquart, wquart, 7 + k, CN).wait_send()


def attention_block(x_blk, w_qkv, w_o, flag, heads, head_dim, ndev):
    rows, d_model = x_blk.shape
    seq = rows * ndev
    width = heads * head_dim
    vm = pl.BlockSpec(memory_space=pltpu.VMEM)
    hbm = pl.BlockSpec(memory_space=pl.ANY)
    bf16, f32 = jnp.bfloat16, jnp.float32
    dma = pltpu.SemaphoreType.DMA
    return pl.pallas_call(
        functools.partial(attn_block, heads=heads, head_dim=head_dim),
        name='attn_block',
        out_shape=(jax.ShapeDtypeStruct((rows, d_model), bf16), jax.ShapeDtypeStruct(flag.shape, f32)),
        in_specs=[hbm, vm, hbm, vm],
        out_specs=(vm, vm),
        scratch_shapes=[
            pltpu.VMEM((ndev, rows, d_model), bf16), pltpu.VMEM((seq, 3 * width), bf16),
            pltpu.VMEM((heads, QB, seq), f32), pltpu.VMEM((heads, QB, head_dim), f32),
            pltpu.VMEM((seq, width), bf16), pltpu.VMEM((rows, ndev * width), bf16),
            pltpu.VMEM((ndev * width, d_model), bf16),
            pltpu.VMEM((ndev,) + flag.shape, f32),
            dma((2,)), dma((16,)), dma((ndev, 4)), dma((9,)), dma((9,)), dma((16,)), dma((ndev, 2)), dma((ndev,)), dma((ndev,)),
        ],
        compiler_params=pltpu.CompilerParams(collective_id=0, has_side_effects=True, vmem_limit_bytes=63 * MIB),
        cost_estimate=pl.CostEstimate(flops=2 * seq * d_model * width * 3 + 4 * seq * seq * width, bytes_accessed=16 * MIB, transcendentals=0),
    )(x_blk, w_qkv, w_o, flag)


def moe_block(h_ref, rl_ref, rc_ref, g_ref, meta_ref, wg_hbm, wu_hbm, wd_hbm, y_ref, send, recv, zbuf, ret,
              meta_in, xs, zacc, acc, wg, wu, wd, ds, dr, rs, rr, ls, ms, mr, wsem, *, main, spill):
    cp, tp = lax.axis_index('cp'), lax.axis_index('tp')
    me = cp * 4 + tp
    chunks, ndev, crow, d_model = send.shape
    rows_all = ndev * crow
    toks = h_ref.shape[0]
    experts = wg_hbm.shape[0]
    slots, _, ff_half = wg.shape
    first = 1 if spill else 0
    steps = 2 * experts
    tile = 512
    f32, bf16 = jnp.float32, jnp.bfloat16

    def weights(n):
        e, f, slot = n // 2, n % 2, n % slots
        fcols = pl.ds(pl.multiple_of(f * ff_half, ff_half), ff_half)
        return (pltpu.make_async_copy(wg_hbm.at[e, :, fcols], wg.at[slot], wsem.at[slot, 0]),
                pltpu.make_async_copy(wu_hbm.at[e, :, fcols], wu.at[slot], wsem.at[slot, 1]),
                pltpu.make_async_copy(wd_hbm.at[e, fcols, :], wd.at[slot], wsem.at[slot, 2]))

    def fetch(n):
        for copy in weights(n):
            copy.start()

    for n in range(slots - 1):
        fetch(n)

    def peer_of(j):
        return (me + j) % ndev

    def dev(p):
        return {'cp': p // 4, 'tp': p % 4}

    barrier = pltpu.get_barrier_semaphore()
    for j in range(1, ndev):
        pl.semaphore_signal(barrier, inc=1, device_id=dev(peer_of(j)), device_id_type=MESH)
    pl.semaphore_wait(barrier, ndev - 1)

    def meta_copy(j):
        return pltpu.make_async_remote_copy(src_ref=meta_ref.at[peer_of(j)], dst_ref=meta_in.at[me], send_sem=ms.at[j], recv_sem=mr.at[me], device_id=dev(peer_of(j)), device_id_type=MESH)

    if spill:
        for j in range(1, ndev):
            meta_copy(j).start()

    def exchange(src, dst, ssem, rsem, k):
        def copy(j):
            return pltpu.make_async_remote_copy(src_ref=src.at[k, peer_of(j)], dst_ref=dst.at[k, me], send_sem=ssem.at[k, j], recv_sem=rsem.at[k, me], device_id=dev(peer_of(j)), device_id_type=MESH)

        local = pltpu.make_async_copy(src.at[k, me], dst.at[k, me], ssem.at[k, 0])
        return copy, local

    def begin(src, dst, ssem, rsem, k):
        copy, local = exchange(src, dst, ssem, rsem, k)
        local.start()
        for j in range(1, ndev):
            copy(j).start()

    def arrived(src, dst, ssem, rsem, k):
        for j in range(1, ndev):
            pltpu.make_async_remote_copy(src_ref=src.at[k, peer_of(j)], dst_ref=dst.at[k, peer_of(j)], send_sem=ssem.at[k, j], recv_sem=rsem.at[k, peer_of(j)], device_id=dev(peer_of(j)), device_id_type=MESH).wait_recv()
        exchange(src, dst, ssem, rsem, k)[1].wait()

    def left(src, dst, ssem, rsem, k):
        copy, _ = exchange(src, dst, ssem, rsem, k)
        for j in range(1, ndev):
            copy(j).wait_send()

    out_way = (send, recv, ds, dr)
    back_way = (zbuf, ret, rs, rr)

    def pack(k, _):
        ids = lax.broadcasted_iota(jnp.int32, (rows_all, toks), 0) + k * rows_all
        pick = ((ids == rl_ref[0:1, :]) | (ids == rl_ref[1:2, :])).astype(f32).astype(bf16)

        def cols(n, _):
            c = pl.ds(pl.multiple_of(n * tile, tile), tile)
            rows = jnp.dot(pick, h_ref[:, c], preferred_element_type=f32).astype(bf16)
            send[k, :, :, c] = rows.reshape(ndev, crow, tile)
            return 0

        lax.fori_loop(0, d_model // tile, cols, 0)

        @pl.when(k > 0)
        def _():
            begin(*out_way, k - 1)

        return 0

    lax.fori_loop(0, chunks, pack, 0)
    begin(*out_way, chunks - 1)

    if spill:
        for j in range(1, ndev):
            p = peer_of(j)
            pltpu.make_async_remote_copy(src_ref=meta_ref.at[p], dst_ref=meta_in.at[p], send_sem=ms.at[j], recv_sem=mr.at[p], device_id=dev(p), device_id_type=MESH).wait_recv()
        arrived(*out_way, 0)
        total = meta_ref[me]
        for j in range(1, ndev):
            total = total + meta_in[peer_of(j)]
        code = total[0:1, :].astype(jnp.int32) - 1
        lane = lax.broadcasted_iota(jnp.int32, code.shape, 1)
        place = (lane // crow) * main + (code & (main - 1))
        owner = code // main
        zbuf[0] = jnp.zeros((ndev, crow, d_model), bf16)
    body = ndev * main

    def expert(e, _):
        k = first + e // 2
        part = pl.ds(pl.multiple_of((e % 2) * main, main), main)

        @pl.when(e % 2 == 0)
        def _():
            arrived(*out_way, k)

        xs[0:body, :] = recv[k, :, part, :].reshape(body, d_model)
        if spill:
            slot_id = lax.broadcasted_iota(jnp.int32, (body, rows_all), 0)
            pick = ((slot_id == place) & (owner == e)).astype(f32).astype(bf16)

            def gather(n, _):
                c = pl.ds(pl.multiple_of(n * tile, tile), tile)
                xs[body:2 * body, c] = jnp.dot(pick, recv[0, :, :, c].reshape(rows_all, tile), preferred_element_type=f32).astype(bf16)
                return 0

            lax.fori_loop(0, d_model // tile, gather, 0)

        for f in range(2):
            n = 2 * e + f
            slot = n % slots
            for copy in weights(n):
                copy.wait()

            @pl.when(n + slots - 1 < steps)
            def _():
                fetch(n + slots - 1)

            x = xs[...]
            gate = jnp.dot(x, wg[slot], preferred_element_type=f32)
            up = jnp.dot(x, wu[slot], preferred_element_type=f32)
            u = (gate * jax.nn.sigmoid(gate) * up).astype(bf16)

            def down(n, _):
                c = pl.ds(pl.multiple_of(n * tile, tile), tile)
                z = jnp.dot(u, wd[slot, :, c], preferred_element_type=f32)
                if f == 0:
                    zacc[:, c] = z
                else:
                    z = (zacc[:, c] + z).astype(bf16)
                    zbuf[k, :, part, c] = z[0:body].reshape(ndev, main, tile)
                    if spill:
                        spread = lax.dot_general(pick, z[body:], (((0,), (0,)), ((), ())), preferred_element_type=f32)
                        zbuf[0, :, :, c] = zbuf[0, :, :, c] + spread.astype(bf16).reshape(ndev, crow, tile)
                return 0

            lax.fori_loop(0, d_model // tile, down, 0)
            if f == 0:
                @pl.when((e % 2 == 0) & (e > 0))
                def _():
                    begin(*back_way, k - 1)

        return 0

    lax.fori_loop(0, experts, expert, 0)
    begin(*back_way, chunks - 1)
    if spill:
        begin(*back_way, 0)

    acc[...] = jnp.zeros_like(acc)

    def combine(kk, _):
        k = (kk + first) % chunks
        arrived(*back_way, k)
        ids = lax.broadcasted_iota(jnp.int32, (toks, rows_all), 1) + k * rows_all
        pick0 = (ids == rc_ref[:, 0:1]).astype(f32).astype(bf16)
        pick1 = (ids == rc_ref[:, 1:2]).astype(f32).astype(bf16)

        def cols(n, _):
            c = pl.ds(pl.multiple_of(n * tile, tile), tile)
            z = ret[k, :, :, c].reshape(rows_all, tile)
            z0 = jnp.dot(pick0, z, preferred_element_type=f32)
            z1 = jnp.dot(pick1, z, preferred_element_type=f32)
            acc[:, c] += g_ref[:, 0:1] * z0 + g_ref[:, 1:2] * z1
            return 0

        lax.fori_loop(0, d_model // tile, cols, 0)
        return 0

    lax.fori_loop(0, chunks, combine, 0)

    def finish(n, _):
        c = pl.ds(pl.multiple_of(n * tile, tile), tile)
        y_ref[:, c] = (h_ref[:, c].astype(f32) + acc[:, c]).astype(bf16)
        return 0

    lax.fori_loop(0, d_model // tile, finish, 0)

    def drain(k, _):
        left(*out_way, k)
        left(*back_way, k)
        return 0

    lax.fori_loop(0, chunks, drain, 0)
    if spill:
        for j in range(1, ndev):
            meta_copy(j).wait_send()


def moe(hidden, rows, gates, meta, w_gate, w_up, w_down, ndev, main, spill):
    toks, d_model = hidden.shape
    experts, _, ff = w_gate.shape
    crow = 2 * main
    chunks = experts // 2 + (1 if spill else 0)
    slots = 3 if spill else 2
    vm = pl.BlockSpec(memory_space=pltpu.VMEM)
    hbm = pl.BlockSpec(memory_space=pl.ANY)
    bf16, f32 = jnp.bfloat16, jnp.float32
    dma = pltpu.SemaphoreType.DMA
    buf = pltpu.VMEM((chunks, ndev, crow, d_model), bf16)
    tile_rows = 2 * ndev * main if spill else ndev * main
    rows_lane = jnp.pad(rows.T, ((0, 6), (0, 0)), constant_values=-1)
    return pl.pallas_call(
        functools.partial(moe_block, main=main, spill=spill),
        name='moe_spill' if spill else 'moe_full',
        out_shape=jax.ShapeDtypeStruct((toks, d_model), bf16),
        in_specs=[vm] * 5 + [hbm] * 3,
        out_specs=vm,
        scratch_shapes=[
            buf, buf, buf, buf, pltpu.VMEM(meta.shape, f32),
            pltpu.VMEM((tile_rows, d_model), bf16), pltpu.VMEM((tile_rows, d_model), f32), pltpu.VMEM((toks, d_model), f32),
            pltpu.VMEM((slots, d_model, ff // 2), bf16), pltpu.VMEM((slots, d_model, ff // 2), bf16), pltpu.VMEM((slots, ff // 2, d_model), bf16),
            dma((chunks, ndev)), dma((chunks, ndev)), dma((chunks, ndev)), dma((chunks, ndev)), dma((1,)), dma((ndev,)), dma((ndev,)), dma((slots, 3)),
        ],
        compiler_params=pltpu.CompilerParams(collective_id=1 if spill else 2, has_side_effects=True, vmem_limit_bytes=63 * MIB),
        cost_estimate=pl.CostEstimate(flops=6 * tile_rows * experts * d_model * ff, bytes_accessed=6 * experts * d_model * ff, transcendentals=0),
    )(hidden, rows_lane, rows, gates, meta, w_gate, w_up, w_down)


def solution(mesh):
    cp_size = mesh.shape['cp']
    tp_size = mesh.shape['tp']
    num_devs = cp_size * tp_size
    row_spec = P(('data', 'cp', 'tp'), None)
    head_spec = P(None, 'tp', None)
    wo_spec = P('tp', None, None)
    expert_spec = P(('cp', 'tp'), None, None)

    def device_fn(x_blk, w_q, w_k, w_v, w_o, idx_blk, gate_blk, w_gate, w_up, w_down):
        tok_dev, d_model = x_blk.shape
        heads_tp, head_dim = w_q.shape[1], w_q.shape[2]
        heads = heads_tp // cp_size
        width = heads * head_dim
        exp_local = w_gate.shape[0]
        num_exp = exp_local * num_devs
        capacity = 4 * tok_dev // num_exp
        mean = capacity // 2
        crow = 2 * mean
        cp_rank = lax.axis_index('cp')
        me = cp_rank * tp_size + lax.axis_index('tp')

        flat = idx_blk.reshape(-1)
        count = flat.shape[0]
        onehot = flat[:, None] == jnp.arange(num_exp)[None, :]
        before = (jnp.arange(count)[:, None] > jnp.arange(count)[None, :]).astype(jnp.bfloat16)
        ranks = jnp.dot(before, onehot.astype(jnp.bfloat16), preferred_element_type=jnp.float32)
        pos = jnp.sum(jnp.where(onehot, ranks, 0.0), axis=1).astype(jnp.int32)
        dest, local = flat // exp_local, flat % exp_local
        over = pos >= mean
        onehot = (dest[:, None] == jnp.arange(num_devs)[None, :]) & over[:, None]
        ranks = jnp.dot(before, onehot.astype(jnp.bfloat16), preferred_element_type=jnp.float32)
        spill_pos = jnp.sum(jnp.where(onehot, ranks, 0.0), axis=1).astype(jnp.int32)
        flag = jnp.full((8, 128), jnp.max(jnp.sum(onehot.astype(jnp.float32), axis=0)))
        rows_spill = jnp.where(over, dest * crow + spill_pos, ((1 + local // 2) * num_devs + dest) * crow + (local % 2) * mean + pos)
        rows_full = ((local // 2) * num_devs + dest) * (2 * capacity) + (local % 2) * capacity + pos
        slot = jnp.arange(num_devs * crow)
        code = jnp.sum(jnp.where((rows_spill[:, None] == slot[None, :]) & over[:, None], (1 + local * mean + pos - mean)[:, None], 0), axis=0).astype(jnp.float32)
        meta = jnp.where(slot[None, :] // crow == me, jnp.tile(code.reshape(num_devs, crow), (1, num_devs)), 0.0)
        meta = jnp.broadcast_to(meta[:, None, :], (num_devs, 8, num_devs * crow))

        w_qkv = jnp.concatenate([lax.dynamic_slice_in_dim(w, cp_rank * heads, heads, 1).reshape(d_model, width) for w in (w_q, w_k, w_v)], axis=1)
        hidden, most = attention_block(x_blk, w_qkv, w_o.reshape(-1, d_model), flag, heads, head_dim, num_devs)

        def run(rows, main, spill):
            return lambda h: moe(h, rows.reshape(tok_dev, 2), gate_blk, meta, w_gate, w_up, w_down, num_devs, main, spill)

        return lax.cond(most[0, 0] <= crow, run(rows_spill, mean, True), run(rows_full, capacity, False), hidden)

    return jax.shard_map(device_fn, mesh=mesh, in_specs=(row_spec, head_spec, head_spec, head_spec, wo_spec, row_spec, row_spec, expert_spec, expert_spec, expert_spec), out_specs=row_spec, check_vma=False)
```

```python
import functools
import math

import jax
import jax.numpy as jnp
from jax import lax
from jax.experimental import pallas as pl
from jax.experimental.pallas import tpu as pltpu
from jax.sharding import PartitionSpec as P

MESH = pl.DeviceIdType.MESH
MIB = 1024 * 1024
QB = 512


def lane_fold(s, op):
    out = s[:, :128]
    for g in range(1, s.shape[1] // 128):
        out = op(out, s[:, g * 128:(g + 1) * 128])
    return out


def attn_block(x_hbm, wq_hbm, wk_hbm, wv_hbm, wo_hbm, flag_ref, h_ref, any_ref, xbuf, wqkv_ref, w_pair, qkv, s_ref, acc_ref, o_loc, o_cat, wo_buf,
               flags, loc_sem, xs, xr, ws, wr, os_sem, or_sem, fs, fr, *, heads, head_dim):
    cp, tp = lax.axis_index('cp'), lax.axis_index('tp')
    xx, cc = tp // 2, tp % 2
    me = cp * 4 + tp
    ndev, rows, d_model = xbuf.shape
    half_rows = rows // 2
    quarter = half_rows // 2
    width = heads * head_dim
    seq = ndev * rows
    wrows = wo_hbm.shape[0]
    whalf, wquart = wrows // 2, wrows // 4

    def tp_of(dx, dc):
        return ((xx + dx) % 2) * 2 + (cc + dc) % 2

    def idx(dx, dy, dc):
        return ((cp + dy) % 2) * 4 + tp_of(dx, dc)

    def dev(dx, dy, dc):
        return {'cp': (cp + dy) % 2, 'tp': tp_of(dx, dc)}

    x_load = pltpu.make_async_copy(x_hbm, xbuf.at[me], loc_sem.at[0])
    wo_load = pltpu.make_async_copy(wo_hbm, wo_buf.at[pl.ds(tp * wrows, wrows)], loc_sem.at[1])
    x_load.start()
    wo_load.start()
    w_loads = [pltpu.make_async_copy(w.at[:, pl.ds(heads * cp, heads), :], w_pair, loc_sem.at[2]) for w in (wq_hbm, wk_hbm, wv_hbm)]
    w_loads[0].start()

    barrier = pltpu.get_barrier_semaphore()
    for k in range(1, ndev):
        peer = (me + k) % ndev
        pl.semaphore_signal(barrier, inc=1, device_id={'cp': peer // 4, 'tp': peer % 4}, device_id_type=MESH)
    pl.semaphore_wait(barrier, ndev - 1)

    def xcopy(slot, owner, row0, count, part, target):
        ref = xbuf.at[idx(*owner), pl.ds(row0 if isinstance(row0, int) else pl.multiple_of(row0, quarter), count)]
        return pltpu.make_async_remote_copy(src_ref=ref, dst_ref=ref, send_sem=xs.at[slot], recv_sem=xr.at[idx(*owner), part], device_id=dev(*target), device_id_type=MESH)

    XN, YN, CN, DG, OWN = (1, 0, 0), (0, 1, 0), (0, 0, 1), (1, 1, 0), (0, 0, 0)
    XC, YC, DC = (1, 0, 1), (0, 1, 1), (1, 1, 1)
    H, Q = half_rows, quarter
    sends = [
        (OWN, 0, H, 0, XN), (OWN, H, Q, 2, XN), (OWN, 0, H, 0, YN), (OWN, H, Q, 2, YN), (OWN, 0, H, 0, CN), (OWN, H, H, 2, CN),
        (XN, 0, H, 0, CN), (XN, H, H, 2, CN), (YN, 0, H, 0, CN), (YN, H, H, 2, CN),
        (YN, 0, Q, 0, XN), (YN, H, Q, 2, XN), (XN, Q, Q, 1, YN), (XN, H + Q, Q, 3, YN),
        (DG, 0, H, 0, CN), (DG, H, H, 2, CN), (OWN, H + Q, Q, 3, XN), (OWN, H + Q, Q, 3, YN),
    ]

    def send(*slots):
        for slot in slots:
            xcopy(slot, *sends[slot]).start()

    def arrive(owner, row0, count, part):
        xcopy(0, owner, row0, count, part, CN).wait_recv()

    def wcopy(slot, shard, row0, count, sem, target):
        ref = wo_buf.at[pl.ds(shard * wrows + row0, count)]
        return pltpu.make_async_remote_copy(src_ref=ref, dst_ref=ref, send_sem=ws.at[slot], recv_sem=wr.at[sem], device_id=dev(*target), device_id_type=MESH)

    def flag_copy(j):
        peer = (me + j) % ndev
        return pltpu.make_async_remote_copy(src_ref=flag_ref, dst_ref=flags.at[me], send_sem=fs.at[j], recv_sem=fr.at[me], device_id={'cp': peer // 4, 'tp': peer % 4}, device_id_type=MESH)

    for j in range(1, ndev):
        flag_copy(j).start()

    x_load.wait()
    send(0, 2, 4, 1, 3, 5)
    wo_load.wait()
    w_own = wcopy(0, tp, 0, wrows, 0, CN)
    w_own.start()

    for kind in range(3):
        w_loads[kind].wait()

        def relayout(n, _):
            r = pl.ds(pl.multiple_of(n * 256, 256), 256)
            for h in range(heads):
                c = kind * width + h * head_dim
                wqkv_ref[r, c:c + head_dim] = w_pair[r, h, :]
            return 0

        lax.fori_loop(0, d_model // 256, relayout, 0)
        if kind < 2:
            w_loads[kind + 1].start()

    def project(owner, half):
        r, t = owner // 4, owner % 4
        seg = r + half * (3 - 2 * r)
        x = xbuf[owner, pl.ds(pl.multiple_of(half * half_rows, half_rows), half_rows), :]
        out = jnp.dot(x, wqkv_ref[...], preferred_element_type=jnp.float32).astype(jnp.bfloat16)
        qkv[pl.ds(pl.multiple_of((seg * 4 + t) * half_rows, half_rows), half_rows), :] = out

    def near(s, _):
        @pl.when(s == 2)
        def _():
            arrive(CN, 0, half_rows, 0)

        @pl.when(s == 3)
        def _():
            arrive(CN, half_rows, half_rows, 2)

        project(idx(0, 0, s // 2), s % 2)
        return 0

    lax.fori_loop(0, 4, near, 0)

    w_x = [(1 + k, tp, cp * whalf + k * wquart, wquart, 1 + k, XN) for k in range(2)]

    def gather(p):
        base = p * half_rows

        @pl.when(p == 0)
        def _():
            arrive(XN, 0, H, 0)
            arrive(YN, 0, H, 0)
            send(12, 10, 16, 17, 6, 8)

        def mid(u, _):
            @pl.when(u == 2)
            def _():
                arrive(XC, base, H, 2 * p)

            @pl.when(u == 3)
            def _():
                arrive(YC, base, H, 2 * p)

            project(idx(1 - u % 2, u % 2, u // 2), p)
            return 0

        lax.fori_loop(0, 4, mid, 0)

        @pl.when(p == 0)
        def _():
            arrive(XN, H, Q, 2)
            arrive(YN, H, Q, 2)
            send(11)

        arrive(DG, base, Q, 2 * p)
        arrive(DG, base + Q, Q, 2 * p + 1)

        @pl.when(p == 0)
        def _():
            send(14)

        @pl.when(p == 1)
        def _():
            send(15)

        def far(u, _):
            @pl.when(u == 1)
            def _():
                arrive(DC, base, H, 2 * p)

            project(idx(1, 1, u), p)
            return 0

        lax.fori_loop(0, 2, far, 0)

    def late():
        arrive(XN, H + Q, Q, 3)
        arrive(YN, H + Q, Q, 3)
        send(13, 7, 9)
        for spec in w_x:
            wcopy(*spec).start()

    coef = (head_dim ** -0.5) * math.log2(math.e)
    my_col = (4 * tp + 2 * cp) * head_dim

    def o_place(b):
        seg, t = b // 4, b % 4
        half = seg // 2
        return seg + half * (3 - 2 * seg), t, half

    def o_remote(b):
        r, t, half = o_place(b)
        return pltpu.make_async_remote_copy(
            src_ref=o_loc.at[pl.ds(pl.multiple_of(b * half_rows, half_rows), half_rows)],
            dst_ref=o_cat.at[pl.ds(pl.multiple_of(half * half_rows, half_rows), half_rows), pl.ds(pl.multiple_of(my_col, width), width)],
            send_sem=os_sem.at[b], recv_sem=or_sem.at[me, half], device_id={'cp': r, 'tp': t}, device_id_type=MESH)

    def o_local(b):
        _, _, half = o_place(b)
        return pltpu.make_async_copy(
            o_loc.at[pl.ds(pl.multiple_of(b * half_rows, half_rows), half_rows)],
            o_cat.at[pl.ds(pl.multiple_of(half * half_rows, half_rows), half_rows), pl.ds(pl.multiple_of(my_col, width), width)],
            os_sem.at[b])

    def o_send(i):
        for part in range(QB // half_rows):
            b = i * (QB // half_rows) + part
            r, t, _ = o_place(b)

            @pl.when(r * 4 + t != me)
            def _():
                o_remote(b).start()

            @pl.when(r * 4 + t == me)
            def _():
                o_local(b).start()

    peer_t = tp_of(1, 0)
    peer_c = tp_of(1, 1)

    def w_pass(k):
        wcopy(1, peer_t, cp * whalf + k * wquart, wquart, 1 + k, CN).wait_recv()
        wcopy(3 + k, peer_t, cp * whalf + k * wquart, wquart, 3 + k, YN).start()
        wcopy(5 + k, peer_t, cp * whalf + k * wquart, wquart, 5 + k, CN).start()

    def w_last(k):
        wcopy(1, peer_t, (1 - cp) * whalf + k * wquart, wquart, 3 + k, CN).wait_recv()
        wcopy(7 + k, peer_t, (1 - cp) * whalf + k * wquart, wquart, 7 + k, CN).start()

    blocks = seq // QB

    def q_step(i, _):
        @pl.when(i == blocks // 2 - 1)
        def _():
            late()
            for early in range(blocks // 2 - 1):
                o_send(early)

        @pl.when(i == blocks - 2)
        def _():
            w_pass(0)

        @pl.when(i == blocks - 1)
        def _():
            w_pass(1)

        q_rows = pl.ds(pl.multiple_of(i * QB, QB), QB)

        def cols(kind, h):
            return slice(kind * width + h * head_dim, kind * width + (h + 1) * head_dim)

        def scores(h, j):
            k = qkv[pl.ds(pl.multiple_of(j * QB, QB), QB), cols(1, h)]
            return lax.dot_general(qkv[q_rows, cols(0, h)], k, (((1,), (1,)), ((), ())), preferred_element_type=jnp.float32)

        def pass1(j, ms):
            out = []
            for h in range(heads):
                s = scores(h, j)
                s_ref[h, :, pl.ds(pl.multiple_of(j * QB, QB), QB)] = s
                out.append(jnp.maximum(ms[h], lane_fold(s, jnp.maximum)))
            return tuple(out)

        ms = lax.fori_loop(0, i, pass1, tuple(jnp.full((QB, 128), -jnp.inf, jnp.float32) for _ in range(heads)))
        keep = lax.broadcasted_iota(jnp.int32, (QB, QB), 1) <= lax.broadcasted_iota(jnp.int32, (QB, QB), 0)
        tops = []
        for h in range(heads):
            s = jnp.where(keep, scores(h, i), -jnp.inf)
            s_ref[h, :, pl.ds(pl.multiple_of(i * QB, QB), QB)] = s
            tops.append(jnp.max(jnp.maximum(ms[h], lane_fold(s, jnp.maximum)), axis=1, keepdims=True))
        acc_ref[...] = jnp.zeros_like(acc_ref)

        def pass2(j, ls):
            out = []
            for h in range(heads):
                e = jnp.exp2((s_ref[h, :, pl.ds(pl.multiple_of(j * QB, QB), QB)] - tops[h]) * coef)
                v = qkv[pl.ds(pl.multiple_of(j * QB, QB), QB), cols(2, h)]
                acc_ref[h] += jnp.dot(e.astype(jnp.bfloat16), v, preferred_element_type=jnp.float32)
                out.append(ls[h] + lane_fold(e, jnp.add))
            return tuple(out)

        ls = lax.fori_loop(0, i + 1, pass2, tuple(jnp.zeros((QB, 128), jnp.float32) for _ in range(heads)))
        for h in range(heads):
            total = jnp.sum(ls[h], axis=1, keepdims=True)
            o_loc[q_rows, h * head_dim:(h + 1) * head_dim] = (acc_ref[h] / total).astype(jnp.bfloat16)

        @pl.when(i >= blocks // 2 - 1)
        def _():
            o_send(i)

        return 0

    def phase(p, _):
        gather(p)
        lax.fori_loop(p * (blocks // 2), (p + 1) * (blocks // 2), q_step, 0)
        return 0

    lax.fori_loop(0, 2, phase, 0)

    w_last(0)
    w_last(1)
    wcopy(1, tp_of(0, 1), 0, wrows, 0, CN).wait_recv()
    for k in range(2):
        wcopy(1, peer_c, cp * whalf + k * wquart, wquart, 5 + k, CN).wait_recv()
        wcopy(1, peer_c, (1 - cp) * whalf + k * wquart, wquart, 7 + k, CN).wait_recv()
    for k in range(1, ndev):
        src = (me + k) % ndev
        col = (4 * (src % 4) + 2 * (src // 4)) * head_dim
        for half in range(2):
            ref = o_cat.at[pl.ds(half * half_rows, half_rows), pl.ds(pl.multiple_of(col, width), width)]
            pltpu.make_async_remote_copy(src_ref=ref, dst_ref=ref, send_sem=os_sem.at[0], recv_sem=or_sem.at[src, half], device_id=dev(0, 0, 1), device_id_type=MESH).wait_recv()

    def drain(b, _):
        r, t, _half = o_place(b)

        @pl.when(r * 4 + t != me)
        def _():
            o_remote(b).wait_send()

        @pl.when(r * 4 + t == me)
        def _():
            o_local(b).wait()

        return 0

    lax.fori_loop(0, seq // half_rows, drain, 0)

    tile = 256

    def out_step(n, _):
        c = pl.ds(pl.multiple_of(n * tile, tile), tile)
        a = jnp.dot(o_cat[...], wo_buf[:, c], preferred_element_type=jnp.float32)
        h_ref[:, c] = (xbuf[me, :, c].astype(jnp.float32) + a).astype(jnp.bfloat16)
        return 0

    lax.fori_loop(0, d_model // tile, out_step, 0)

    most = flag_ref[...]
    for j in range(1, ndev):
        peer = (me + j) % ndev
        pltpu.make_async_remote_copy(src_ref=flag_ref, dst_ref=flags.at[peer], send_sem=fs.at[j], recv_sem=fr.at[peer], device_id=dev(0, 0, 1), device_id_type=MESH).wait_recv()
        most = jnp.maximum(most, flags[peer])
        flag_copy(j).wait_send()
    any_ref[...] = most

    for slot in range(len(sends)):
        xcopy(slot, *sends[slot]).wait_send()
    w_own.wait_send()
    for spec in w_x:
        wcopy(*spec).wait_send()
    for k in range(2):
        wcopy(3 + k, peer_t, cp * whalf + k * wquart, wquart, 3 + k, YN).wait_send()
        wcopy(5 + k, peer_t, cp * whalf + k * wquart, wquart, 5 + k, CN).wait_send()
        wcopy(7 + k, peer_t, (1 - cp) * whalf + k * wquart, wquart, 7 + k, CN).wait_send()


def attention_block(x_blk, w_q, w_k, w_v, w_o, flag, heads, head_dim, ndev):
    rows, d_model = x_blk.shape
    seq = rows * ndev
    width = heads * head_dim
    vm = pl.BlockSpec(memory_space=pltpu.VMEM)
    hbm = pl.BlockSpec(memory_space=pl.ANY)
    bf16, f32 = jnp.bfloat16, jnp.float32
    dma = pltpu.SemaphoreType.DMA
    return pl.pallas_call(
        functools.partial(attn_block, heads=heads, head_dim=head_dim),
        name='attn_block',
        out_shape=(jax.ShapeDtypeStruct((rows, d_model), bf16), jax.ShapeDtypeStruct(flag.shape, f32)),
        in_specs=[hbm] * 5 + [vm],
        out_specs=(vm, vm),
        scratch_shapes=[
            pltpu.VMEM((ndev, rows, d_model), bf16), pltpu.VMEM((d_model, 3 * width), bf16), pltpu.VMEM((d_model, heads, head_dim), bf16), pltpu.VMEM((seq, 3 * width), bf16),
            pltpu.VMEM((heads, QB, seq), f32), pltpu.VMEM((heads, QB, head_dim), f32),
            pltpu.VMEM((seq, width), bf16), pltpu.VMEM((rows, ndev * width), bf16),
            pltpu.VMEM((ndev * width, d_model), bf16),
            pltpu.VMEM((ndev,) + flag.shape, f32),
            dma((3,)), dma((18,)), dma((ndev, 4)), dma((9,)), dma((9,)), dma((16,)), dma((ndev, 2)), dma((ndev,)), dma((ndev,)),
        ],
        compiler_params=pltpu.CompilerParams(collective_id=0, has_side_effects=True, vmem_limit_bytes=63 * MIB),
        cost_estimate=pl.CostEstimate(flops=2 * seq * d_model * width * 3 + 4 * seq * seq * width, bytes_accessed=16 * MIB, transcendentals=0),
    )(x_blk, w_q, w_k, w_v, w_o, flag)


def moe_block(h_ref, rl_ref, rc_ref, g_ref, meta_ref, wg_hbm, wu_hbm, wd_hbm, y_ref, send, recv, zbuf, ret,
              meta_in, xs, zacc, acc, wg, wu, wd, ds, dr, rs, rr, ls, ms, mr, wsem, *, main, spill):
    cp, tp = lax.axis_index('cp'), lax.axis_index('tp')
    me = cp * 4 + tp
    chunks, ndev, crow, d_model = send.shape
    rows_all = ndev * crow
    toks = h_ref.shape[0]
    experts = wg_hbm.shape[0]
    slots, _, ff_half = wg.shape
    first = 1 if spill else 0
    steps = 2 * experts
    tile = 512
    f32, bf16 = jnp.float32, jnp.bfloat16

    def weights(n):
        e, f, slot = n // 2, n % 2, n % slots
        fcols = pl.ds(pl.multiple_of(f * ff_half, ff_half), ff_half)
        return (pltpu.make_async_copy(wg_hbm.at[e, :, fcols], wg.at[slot], wsem.at[slot, 0]),
                pltpu.make_async_copy(wu_hbm.at[e, :, fcols], wu.at[slot], wsem.at[slot, 1]),
                pltpu.make_async_copy(wd_hbm.at[e, fcols, :], wd.at[slot], wsem.at[slot, 2]))

    def fetch(n):
        for copy in weights(n):
            copy.start()

    for n in range(slots - 1):
        fetch(n)

    def peer_of(j):
        return (me + j) % ndev

    def dev(p):
        return {'cp': p // 4, 'tp': p % 4}

    barrier = pltpu.get_barrier_semaphore()
    for j in range(1, ndev):
        pl.semaphore_signal(barrier, inc=1, device_id=dev(peer_of(j)), device_id_type=MESH)
    pl.semaphore_wait(barrier, ndev - 1)

    def meta_copy(j):
        return pltpu.make_async_remote_copy(src_ref=meta_ref.at[peer_of(j)], dst_ref=meta_in.at[me], send_sem=ms.at[j], recv_sem=mr.at[me], device_id=dev(peer_of(j)), device_id_type=MESH)

    if spill:
        for j in range(1, ndev):
            meta_copy(j).start()

    def exchange(src, dst, ssem, rsem, k):
        def copy(j):
            return pltpu.make_async_remote_copy(src_ref=src.at[k, peer_of(j)], dst_ref=dst.at[k, me], send_sem=ssem.at[k, j], recv_sem=rsem.at[k, me], device_id=dev(peer_of(j)), device_id_type=MESH)

        local = pltpu.make_async_copy(src.at[k, me], dst.at[k, me], ssem.at[k, 0])
        return copy, local

    def begin(src, dst, ssem, rsem, k):
        copy, local = exchange(src, dst, ssem, rsem, k)
        local.start()
        for j in range(1, ndev):
            copy(j).start()

    def arrived(src, dst, ssem, rsem, k):
        for j in range(1, ndev):
            pltpu.make_async_remote_copy(src_ref=src.at[k, peer_of(j)], dst_ref=dst.at[k, peer_of(j)], send_sem=ssem.at[k, j], recv_sem=rsem.at[k, peer_of(j)], device_id=dev(peer_of(j)), device_id_type=MESH).wait_recv()
        exchange(src, dst, ssem, rsem, k)[1].wait()

    def left(src, dst, ssem, rsem, k):
        copy, _ = exchange(src, dst, ssem, rsem, k)
        for j in range(1, ndev):
            copy(j).wait_send()

    out_way = (send, recv, ds, dr)
    back_way = (zbuf, ret, rs, rr)

    def pack(k, _):
        ids = lax.broadcasted_iota(jnp.int32, (rows_all, toks), 0) + k * rows_all
        pick = ((ids == rl_ref[0:1, :]) | (ids == rl_ref[1:2, :])).astype(f32).astype(bf16)

        def cols(n, _):
            c = pl.ds(pl.multiple_of(n * tile, tile), tile)
            rows = jnp.dot(pick, h_ref[:, c], preferred_element_type=f32).astype(bf16)
            send[k, :, :, c] = rows.reshape(ndev, crow, tile)
            return 0

        lax.fori_loop(0, d_model // tile, cols, 0)

        @pl.when(k > 0)
        def _():
            begin(*out_way, k - 1)

        return 0

    lax.fori_loop(0, chunks, pack, 0)
    begin(*out_way, chunks - 1)

    if spill:
        for j in range(1, ndev):
            p = peer_of(j)
            pltpu.make_async_remote_copy(src_ref=meta_ref.at[p], dst_ref=meta_in.at[p], send_sem=ms.at[j], recv_sem=mr.at[p], device_id=dev(p), device_id_type=MESH).wait_recv()
        arrived(*out_way, 0)
        total = meta_ref[me]
        for j in range(1, ndev):
            total = total + meta_in[peer_of(j)]
        code = total[0:1, :].astype(jnp.int32) - 1
        lane = lax.broadcasted_iota(jnp.int32, code.shape, 1)
        place = (lane // crow) * main + (code & (main - 1))
        owner = code // main
        zbuf[0] = jnp.zeros((ndev, crow, d_model), bf16)
    body = ndev * main

    def expert(e, _):
        k = first + e // 2
        part = pl.ds(pl.multiple_of((e % 2) * main, main), main)

        @pl.when(e % 2 == 0)
        def _():
            arrived(*out_way, k)

        xs[0:body, :] = recv[k, :, part, :].reshape(body, d_model)
        if spill:
            slot_id = lax.broadcasted_iota(jnp.int32, (body, rows_all), 0)
            pick = ((slot_id == place) & (owner == e)).astype(f32).astype(bf16)

            def gather(n, _):
                c = pl.ds(pl.multiple_of(n * tile, tile), tile)
                xs[body:2 * body, c] = jnp.dot(pick, recv[0, :, :, c].reshape(rows_all, tile), preferred_element_type=f32).astype(bf16)
                return 0

            lax.fori_loop(0, d_model // tile, gather, 0)

        for f in range(2):
            n = 2 * e + f
            slot = n % slots
            for copy in weights(n):
                copy.wait()

            @pl.when(n + slots - 1 < steps)
            def _():
                fetch(n + slots - 1)

            x = xs[...]
            gate = jnp.dot(x, wg[slot], preferred_element_type=f32)
            up = jnp.dot(x, wu[slot], preferred_element_type=f32)
            u = (gate * jax.nn.sigmoid(gate) * up).astype(bf16)

            def down(n, _):
                c = pl.ds(pl.multiple_of(n * tile, tile), tile)
                z = jnp.dot(u, wd[slot, :, c], preferred_element_type=f32)
                if f == 0:
                    zacc[:, c] = z
                else:
                    z = (zacc[:, c] + z).astype(bf16)
                    zbuf[k, :, part, c] = z[0:body].reshape(ndev, main, tile)
                    if spill:
                        spread = lax.dot_general(pick, z[body:], (((0,), (0,)), ((), ())), preferred_element_type=f32)
                        zbuf[0, :, :, c] = zbuf[0, :, :, c] + spread.astype(bf16).reshape(ndev, crow, tile)
                return 0

            lax.fori_loop(0, d_model // tile, down, 0)
            if f == 0:
                @pl.when((e % 2 == 0) & (e > 0))
                def _():
                    begin(*back_way, k - 1)

        return 0

    lax.fori_loop(0, experts, expert, 0)
    begin(*back_way, chunks - 1)
    if spill:
        begin(*back_way, 0)

    acc[...] = jnp.zeros_like(acc)

    def combine(kk, _):
        k = (kk + first) % chunks
        arrived(*back_way, k)
        ids = lax.broadcasted_iota(jnp.int32, (toks, rows_all), 1) + k * rows_all
        pick0 = (ids == rc_ref[:, 0:1]).astype(f32).astype(bf16)
        pick1 = (ids == rc_ref[:, 1:2]).astype(f32).astype(bf16)

        def cols(n, _):
            c = pl.ds(pl.multiple_of(n * tile, tile), tile)
            z = ret[k, :, :, c].reshape(rows_all, tile)
            z0 = jnp.dot(pick0, z, preferred_element_type=f32)
            z1 = jnp.dot(pick1, z, preferred_element_type=f32)
            acc[:, c] += g_ref[:, 0:1] * z0 + g_ref[:, 1:2] * z1
            return 0

        lax.fori_loop(0, d_model // tile, cols, 0)
        return 0

    lax.fori_loop(0, chunks, combine, 0)

    def finish(n, _):
        c = pl.ds(pl.multiple_of(n * tile, tile), tile)
        y_ref[:, c] = (h_ref[:, c].astype(f32) + acc[:, c]).astype(bf16)
        return 0

    lax.fori_loop(0, d_model // tile, finish, 0)

    def drain(k, _):
        left(*out_way, k)
        left(*back_way, k)
        return 0

    lax.fori_loop(0, chunks, drain, 0)
    if spill:
        for j in range(1, ndev):
            meta_copy(j).wait_send()


def moe(hidden, rows, gates, meta, w_gate, w_up, w_down, ndev, main, spill):
    toks, d_model = hidden.shape
    experts, _, ff = w_gate.shape
    crow = 2 * main
    chunks = experts // 2 + (1 if spill else 0)
    slots = 3 if spill else 2
    vm = pl.BlockSpec(memory_space=pltpu.VMEM)
    hbm = pl.BlockSpec(memory_space=pl.ANY)
    bf16, f32 = jnp.bfloat16, jnp.float32
    dma = pltpu.SemaphoreType.DMA
    buf = pltpu.VMEM((chunks, ndev, crow, d_model), bf16)
    tile_rows = 2 * ndev * main if spill else ndev * main
    rows_lane = jnp.pad(rows.T, ((0, 6), (0, 0)), constant_values=-1)
    return pl.pallas_call(
        functools.partial(moe_block, main=main, spill=spill),
        name='moe_spill' if spill else 'moe_full',
        out_shape=jax.ShapeDtypeStruct((toks, d_model), bf16),
        in_specs=[vm] * 5 + [hbm] * 3,
        out_specs=vm,
        scratch_shapes=[
            buf, buf, buf, buf, pltpu.VMEM(meta.shape, f32),
            pltpu.VMEM((tile_rows, d_model), bf16), pltpu.VMEM((tile_rows, d_model), f32), pltpu.VMEM((toks, d_model), f32),
            pltpu.VMEM((slots, d_model, ff // 2), bf16), pltpu.VMEM((slots, d_model, ff // 2), bf16), pltpu.VMEM((slots, ff // 2, d_model), bf16),
            dma((chunks, ndev)), dma((chunks, ndev)), dma((chunks, ndev)), dma((chunks, ndev)), dma((1,)), dma((ndev,)), dma((ndev,)), dma((slots, 3)),
        ],
        compiler_params=pltpu.CompilerParams(collective_id=1 if spill else 2, has_side_effects=True, vmem_limit_bytes=63 * MIB),
        cost_estimate=pl.CostEstimate(flops=6 * tile_rows * experts * d_model * ff, bytes_accessed=6 * experts * d_model * ff, transcendentals=0),
    )(hidden, rows_lane, rows, gates, meta, w_gate, w_up, w_down)


def solution(mesh):
    cp_size = mesh.shape['cp']
    tp_size = mesh.shape['tp']
    num_devs = cp_size * tp_size
    row_spec = P(('data', 'cp', 'tp'), None)
    head_spec = P(None, 'tp', None)
    wo_spec = P('tp', None, None)
    expert_spec = P(('cp', 'tp'), None, None)

    def device_fn(x_blk, w_q, w_k, w_v, w_o, idx_blk, gate_blk, w_gate, w_up, w_down):
        tok_dev, d_model = x_blk.shape
        heads_tp, head_dim = w_q.shape[1], w_q.shape[2]
        heads = heads_tp // cp_size
        exp_local = w_gate.shape[0]
        num_exp = exp_local * num_devs
        capacity = 4 * tok_dev // num_exp
        mean = capacity // 2
        crow = 2 * mean
        cp_rank = lax.axis_index('cp')
        me = cp_rank * tp_size + lax.axis_index('tp')

        flat = idx_blk.reshape(-1)
        count = flat.shape[0]
        onehot = flat[:, None] == jnp.arange(num_exp)[None, :]
        before = (jnp.arange(count)[:, None] > jnp.arange(count)[None, :]).astype(jnp.bfloat16)
        ranks = jnp.dot(before, onehot.astype(jnp.bfloat16), preferred_element_type=jnp.float32)
        pos = jnp.sum(jnp.where(onehot, ranks, 0.0), axis=1).astype(jnp.int32)
        dest, local = flat // exp_local, flat % exp_local
        over = pos >= mean
        onehot = (dest[:, None] == jnp.arange(num_devs)[None, :]) & over[:, None]
        ranks = jnp.dot(before, onehot.astype(jnp.bfloat16), preferred_element_type=jnp.float32)
        spill_pos = jnp.sum(jnp.where(onehot, ranks, 0.0), axis=1).astype(jnp.int32)
        flag = jnp.full((8, 128), jnp.max(jnp.sum(onehot.astype(jnp.float32), axis=0)))
        rows_spill = jnp.where(over, dest * crow + spill_pos, ((1 + local // 2) * num_devs + dest) * crow + (local % 2) * mean + pos)
        rows_full = ((local // 2) * num_devs + dest) * (2 * capacity) + (local % 2) * capacity + pos
        slot = jnp.arange(num_devs * crow)
        code = jnp.sum(jnp.where((rows_spill[:, None] == slot[None, :]) & over[:, None], (1 + local * mean + pos - mean)[:, None], 0), axis=0).astype(jnp.float32)
        meta = jnp.where(slot[None, :] // crow == me, jnp.tile(code.reshape(num_devs, crow), (1, num_devs)), 0.0)
        meta = jnp.broadcast_to(meta[:, None, :], (num_devs, 8, num_devs * crow))

        hidden, most = attention_block(x_blk, w_q, w_k, w_v, w_o.reshape(-1, d_model), flag, heads, head_dim, num_devs)

        def run(rows, main, spill):
            return lambda h: moe(h, rows.reshape(tok_dev, 2), gate_blk, meta, w_gate, w_up, w_down, num_devs, main, spill)

        return lax.cond(most[0, 0] <= crow, run(rows_spill, mean, True), run(rows_full, capacity, False), hidden)

    return jax.shard_map(device_fn, mesh=mesh, in_specs=(row_spec, head_spec, head_spec, head_spec, wo_spec, row_spec, row_spec, expert_spec, expert_spec, expert_spec), out_specs=row_spec, check_vma=False)
```

```python
import functools
import math

import jax
import jax.numpy as jnp
from jax import lax
from jax.experimental import pallas as pl
from jax.experimental.pallas import tpu as pltpu
from jax.sharding import PartitionSpec as P

MESH = pl.DeviceIdType.MESH
MIB = 1024 * 1024
QB = 512


def lane_fold(s, op):
    out = s[:, :128]
    for g in range(1, s.shape[1] // 128):
        out = op(out, s[:, g * 128:(g + 1) * 128])
    return out


def attn_block(x_hbm, wq_hbm, wk_hbm, wv_hbm, wo_hbm, flag_ref, h_ref, any_ref, xbuf, wqkv_ref, w_pair, qkv, s_ref, acc_ref, o_loc, o_cat, wo_buf,
               flags, loc_sem, xs, xr, ws, wr, os_sem, or_sem, fs, fr, *, heads, head_dim):
    cp, tp = lax.axis_index('cp'), lax.axis_index('tp')
    xx, cc = tp // 2, tp % 2
    me = cp * 4 + tp
    ndev, rows, d_model = xbuf.shape
    half_rows = rows // 2
    quarter = half_rows // 2
    width = heads * head_dim
    seq = ndev * rows
    wrows = wo_hbm.shape[0]
    whalf, wquart = wrows // 2, wrows // 4

    def tp_of(dx, dc):
        return ((xx + dx) % 2) * 2 + (cc + dc) % 2

    def idx(dx, dy, dc):
        return ((cp + dy) % 2) * 4 + tp_of(dx, dc)

    def dev(dx, dy, dc):
        return {'cp': (cp + dy) % 2, 'tp': tp_of(dx, dc)}

    x_load = pltpu.make_async_copy(x_hbm, xbuf.at[me], loc_sem.at[0])
    wo_load = pltpu.make_async_copy(wo_hbm, wo_buf.at[pl.ds(tp * wrows, wrows)], loc_sem.at[1])
    x_load.start()
    wo_load.start()
    w_loads = [pltpu.make_async_copy(w.at[:, pl.ds(heads * cp, heads), :], w_pair, loc_sem.at[2]) for w in (wq_hbm, wk_hbm, wv_hbm)]
    w_loads[0].start()

    barrier = pltpu.get_barrier_semaphore()
    for k in range(1, ndev):
        peer = (me + k) % ndev
        pl.semaphore_signal(barrier, inc=1, device_id={'cp': peer // 4, 'tp': peer % 4}, device_id_type=MESH)
    pl.semaphore_wait(barrier, ndev - 1)

    def xcopy(slot, owner, row0, count, part, target):
        ref = xbuf.at[idx(*owner), pl.ds(row0 if isinstance(row0, int) else pl.multiple_of(row0, quarter), count)]
        return pltpu.make_async_remote_copy(src_ref=ref, dst_ref=ref, send_sem=xs.at[slot], recv_sem=xr.at[idx(*owner), part], device_id=dev(*target), device_id_type=MESH)

    XN, YN, CN, DG, OWN = (1, 0, 0), (0, 1, 0), (0, 0, 1), (1, 1, 0), (0, 0, 0)
    XC, YC, DC = (1, 0, 1), (0, 1, 1), (1, 1, 1)
    H, Q = half_rows, quarter
    sends = [
        (OWN, 0, H, 0, XN), (OWN, H, Q, 2, XN), (OWN, 0, H, 0, YN), (OWN, H, Q, 2, YN), (OWN, 0, H, 0, CN), (OWN, H, H, 2, CN),
        (XN, 0, H, 0, CN), (XN, H, H, 2, CN), (YN, 0, H, 0, CN), (YN, H, H, 2, CN),
        (YN, 0, Q, 0, XN), (YN, H, Q, 2, XN), (XN, Q, Q, 1, YN), (XN, H + Q, Q, 3, YN),
        (DG, 0, H, 0, CN), (DG, H, H, 2, CN), (OWN, H + Q, Q, 3, XN), (OWN, H + Q, Q, 3, YN),
    ]

    def send(*slots):
        for slot in slots:
            xcopy(slot, *sends[slot]).start()

    def arrive(owner, row0, count, part):
        xcopy(0, owner, row0, count, part, CN).wait_recv()

    def wcopy(slot, shard, row0, count, sem, target):
        ref = wo_buf.at[pl.ds(shard * wrows + row0, count)]
        return pltpu.make_async_remote_copy(src_ref=ref, dst_ref=ref, send_sem=ws.at[slot], recv_sem=wr.at[sem], device_id=dev(*target), device_id_type=MESH)

    def flag_copy(j):
        peer = (me + j) % ndev
        return pltpu.make_async_remote_copy(src_ref=flag_ref, dst_ref=flags.at[me], send_sem=fs.at[j], recv_sem=fr.at[me], device_id={'cp': peer // 4, 'tp': peer % 4}, device_id_type=MESH)

    for j in range(1, ndev):
        flag_copy(j).start()

    x_load.wait()
    send(0, 2, 4, 1, 3, 5)
    wo_load.wait()
    w_own = wcopy(0, tp, 0, wrows, 0, CN)
    w_own.start()

    for kind in range(3):
        w_loads[kind].wait()

        def relayout(n, _):
            r = pl.ds(pl.multiple_of(n * 256, 256), 256)
            for h in range(heads):
                c = kind * width + h * head_dim
                wqkv_ref[r, c:c + head_dim] = w_pair[r, h, :]
            return 0

        lax.fori_loop(0, d_model // 256, relayout, 0)
        if kind < 2:
            w_loads[kind + 1].start()

    def project(owner, half):
        r, t = owner // 4, owner % 4
        seg = r + half * (3 - 2 * r)
        x = xbuf[owner, pl.ds(pl.multiple_of(half * half_rows, half_rows), half_rows), :]
        out = jnp.dot(x, wqkv_ref[...], preferred_element_type=jnp.float32).astype(jnp.bfloat16)
        qkv[pl.ds(pl.multiple_of((seg * 4 + t) * half_rows, half_rows), half_rows), :] = out

    def near(s, _):
        @pl.when(s == 2)
        def _():
            arrive(CN, 0, half_rows, 0)

        @pl.when(s == 3)
        def _():
            arrive(CN, half_rows, half_rows, 2)

        project(idx(0, 0, s // 2), s % 2)
        return 0

    lax.fori_loop(0, 4, near, 0)

    w_x = [(1 + k, tp, cp * whalf + k * wquart, wquart, 1 + k, XN) for k in range(2)]

    def gather(p):
        base = p * half_rows

        @pl.when(p == 0)
        def _():
            arrive(XN, 0, H, 0)
            arrive(YN, 0, H, 0)
            send(12, 10, 16, 17, 6, 8)

        def mid(u, _):
            @pl.when(u == 2)
            def _():
                arrive(XC, base, H, 2 * p)

            @pl.when(u == 3)
            def _():
                arrive(YC, base, H, 2 * p)

            project(idx(1 - u % 2, u % 2, u // 2), p)
            return 0

        lax.fori_loop(0, 4, mid, 0)

        @pl.when(p == 0)
        def _():
            arrive(XN, H, Q, 2)
            arrive(YN, H, Q, 2)
            send(11)

        arrive(DG, base, Q, 2 * p)
        arrive(DG, base + Q, Q, 2 * p + 1)

        @pl.when(p == 0)
        def _():
            send(14)

        @pl.when(p == 1)
        def _():
            send(15)

        def far(u, _):
            @pl.when(u == 1)
            def _():
                arrive(DC, base, H, 2 * p)

            project(idx(1, 1, u), p)
            return 0

        lax.fori_loop(0, 2, far, 0)

    def late():
        arrive(XN, H + Q, Q, 3)
        arrive(YN, H + Q, Q, 3)
        send(13, 7, 9)
        for spec in w_x:
            wcopy(*spec).start()

    coef = (head_dim ** -0.5) * math.log2(math.e)
    my_col = (4 * tp + 2 * cp) * head_dim

    def o_place(b):
        seg, t = b // 4, b % 4
        half = seg // 2
        return seg + half * (3 - 2 * seg), t, half

    def o_remote(b):
        r, t, half = o_place(b)
        return pltpu.make_async_remote_copy(
            src_ref=o_loc.at[pl.ds(pl.multiple_of(b * half_rows, half_rows), half_rows)],
            dst_ref=o_cat.at[pl.ds(pl.multiple_of(half * half_rows, half_rows), half_rows), pl.ds(pl.multiple_of(my_col, width), width)],
            send_sem=os_sem.at[b], recv_sem=or_sem.at[me, half], device_id={'cp': r, 'tp': t}, device_id_type=MESH)

    def o_local(b):
        _, _, half = o_place(b)
        return pltpu.make_async_copy(
            o_loc.at[pl.ds(pl.multiple_of(b * half_rows, half_rows), half_rows)],
            o_cat.at[pl.ds(pl.multiple_of(half * half_rows, half_rows), half_rows), pl.ds(pl.multiple_of(my_col, width), width)],
            os_sem.at[b])

    def o_send(i):
        for part in range(QB // half_rows):
            b = i * (QB // half_rows) + part
            r, t, _ = o_place(b)

            @pl.when(r * 4 + t != me)
            def _():
                o_remote(b).start()

            @pl.when(r * 4 + t == me)
            def _():
                o_local(b).start()

    peer_t = tp_of(1, 0)
    peer_c = tp_of(1, 1)

    def w_pass(k):
        wcopy(1, peer_t, cp * whalf + k * wquart, wquart, 1 + k, CN).wait_recv()
        wcopy(3 + k, peer_t, cp * whalf + k * wquart, wquart, 3 + k, YN).start()
        wcopy(5 + k, peer_t, cp * whalf + k * wquart, wquart, 5 + k, CN).start()

    def w_last(k):
        wcopy(1, peer_t, (1 - cp) * whalf + k * wquart, wquart, 3 + k, CN).wait_recv()
        wcopy(7 + k, peer_t, (1 - cp) * whalf + k * wquart, wquart, 7 + k, CN).start()

    blocks = seq // QB

    def q_step(i, _):
        @pl.when(i == blocks // 2 - 1)
        def _():
            late()
            for early in range(blocks // 2 - 1):
                o_send(early)

        @pl.when(i == blocks - 3)
        def _():
            w_pass(0)

        @pl.when(i == blocks - 1)
        def _():
            w_pass(1)

        q_rows = pl.ds(pl.multiple_of(i * QB, QB), QB)

        def cols(kind, h):
            return slice(kind * width + h * head_dim, kind * width + (h + 1) * head_dim)

        def scores(h, j):
            k = qkv[pl.ds(pl.multiple_of(j * QB, QB), QB), cols(1, h)]
            return lax.dot_general(qkv[q_rows, cols(0, h)], k, (((1,), (1,)), ((), ())), preferred_element_type=jnp.float32)

        def pass1(j, ms):
            out = []
            for h in range(heads):
                s = scores(h, j)
                s_ref[h, :, pl.ds(pl.multiple_of(j * QB, QB), QB)] = s
                out.append(jnp.maximum(ms[h], lane_fold(s, jnp.maximum)))
            return tuple(out)

        ms = lax.fori_loop(0, i, pass1, tuple(jnp.full((QB, 128), -jnp.inf, jnp.float32) for _ in range(heads)))
        keep = lax.broadcasted_iota(jnp.int32, (QB, QB), 1) <= lax.broadcasted_iota(jnp.int32, (QB, QB), 0)
        tops = []
        for h in range(heads):
            s = jnp.where(keep, scores(h, i), -jnp.inf)
            s_ref[h, :, pl.ds(pl.multiple_of(i * QB, QB), QB)] = s
            tops.append(jnp.max(jnp.maximum(ms[h], lane_fold(s, jnp.maximum)), axis=1, keepdims=True))
        acc_ref[...] = jnp.zeros_like(acc_ref)

        def pass2(j, ls):
            out = []
            for h in range(heads):
                e = jnp.exp2((s_ref[h, :, pl.ds(pl.multiple_of(j * QB, QB), QB)] - tops[h]) * coef)
                v = qkv[pl.ds(pl.multiple_of(j * QB, QB), QB), cols(2, h)]
                acc_ref[h] += jnp.dot(e.astype(jnp.bfloat16), v, preferred_element_type=jnp.float32)
                out.append(ls[h] + lane_fold(e, jnp.add))
            return tuple(out)

        ls = lax.fori_loop(0, i + 1, pass2, tuple(jnp.zeros((QB, 128), jnp.float32) for _ in range(heads)))
        for h in range(heads):
            total = jnp.sum(ls[h], axis=1, keepdims=True)
            o_loc[q_rows, h * head_dim:(h + 1) * head_dim] = (acc_ref[h] / total).astype(jnp.bfloat16)

        @pl.when(i >= blocks // 2 - 1)
        def _():
            o_send(i)

        return 0

    def phase(p, _):
        gather(p)
        lax.fori_loop(p * (blocks // 2), (p + 1) * (blocks // 2), q_step, 0)
        return 0

    lax.fori_loop(0, 2, phase, 0)

    w_last(0)
    w_last(1)
    wcopy(1, tp_of(0, 1), 0, wrows, 0, CN).wait_recv()
    for k in range(2):
        wcopy(1, peer_c, cp * whalf + k * wquart, wquart, 5 + k, CN).wait_recv()
        wcopy(1, peer_c, (1 - cp) * whalf + k * wquart, wquart, 7 + k, CN).wait_recv()
    for k in range(1, ndev):
        src = (me + k) % ndev
        col = (4 * (src % 4) + 2 * (src // 4)) * head_dim
        for half in range(2):
            ref = o_cat.at[pl.ds(half * half_rows, half_rows), pl.ds(pl.multiple_of(col, width), width)]
            pltpu.make_async_remote_copy(src_ref=ref, dst_ref=ref, send_sem=os_sem.at[0], recv_sem=or_sem.at[src, half], device_id=dev(0, 0, 1), device_id_type=MESH).wait_recv()

    def drain(b, _):
        r, t, _half = o_place(b)

        @pl.when(r * 4 + t != me)
        def _():
            o_remote(b).wait_send()

        @pl.when(r * 4 + t == me)
        def _():
            o_local(b).wait()

        return 0

    lax.fori_loop(0, seq // half_rows, drain, 0)

    tile = 256

    def out_step(n, _):
        c = pl.ds(pl.multiple_of(n * tile, tile), tile)
        a = jnp.dot(o_cat[...], wo_buf[:, c], preferred_element_type=jnp.float32)
        h_ref[:, c] = (xbuf[me, :, c].astype(jnp.float32) + a).astype(jnp.bfloat16)
        return 0

    lax.fori_loop(0, d_model // tile, out_step, 0)

    most = flag_ref[...]
    for j in range(1, ndev):
        peer = (me + j) % ndev
        pltpu.make_async_remote_copy(src_ref=flag_ref, dst_ref=flags.at[peer], send_sem=fs.at[j], recv_sem=fr.at[peer], device_id=dev(0, 0, 1), device_id_type=MESH).wait_recv()
        most = jnp.maximum(most, flags[peer])
        flag_copy(j).wait_send()
    any_ref[...] = most

    for slot in range(len(sends)):
        xcopy(slot, *sends[slot]).wait_send()
    w_own.wait_send()
    for spec in w_x:
        wcopy(*spec).wait_send()
    for k in range(2):
        wcopy(3 + k, peer_t, cp * whalf + k * wquart, wquart, 3 + k, YN).wait_send()
        wcopy(5 + k, peer_t, cp * whalf + k * wquart, wquart, 5 + k, CN).wait_send()
        wcopy(7 + k, peer_t, (1 - cp) * whalf + k * wquart, wquart, 7 + k, CN).wait_send()


def attention_block(x_blk, w_q, w_k, w_v, w_o, flag, heads, head_dim, ndev):
    rows, d_model = x_blk.shape
    seq = rows * ndev
    width = heads * head_dim
    vm = pl.BlockSpec(memory_space=pltpu.VMEM)
    hbm = pl.BlockSpec(memory_space=pl.ANY)
    bf16, f32 = jnp.bfloat16, jnp.float32
    dma = pltpu.SemaphoreType.DMA
    return pl.pallas_call(
        functools.partial(attn_block, heads=heads, head_dim=head_dim),
        name='attn_block',
        out_shape=(jax.ShapeDtypeStruct((rows, d_model), bf16), jax.ShapeDtypeStruct(flag.shape, f32)),
        in_specs=[hbm] * 5 + [vm],
        out_specs=(vm, vm),
        scratch_shapes=[
            pltpu.VMEM((ndev, rows, d_model), bf16), pltpu.VMEM((d_model, 3 * width), bf16), pltpu.VMEM((d_model, heads, head_dim), bf16), pltpu.VMEM((seq, 3 * width), bf16),
            pltpu.VMEM((heads, QB, seq), f32), pltpu.VMEM((heads, QB, head_dim), f32),
            pltpu.VMEM((seq, width), bf16), pltpu.VMEM((rows, ndev * width), bf16),
            pltpu.VMEM((ndev * width, d_model), bf16),
            pltpu.VMEM((ndev,) + flag.shape, f32),
            dma((3,)), dma((18,)), dma((ndev, 4)), dma((9,)), dma((9,)), dma((16,)), dma((ndev, 2)), dma((ndev,)), dma((ndev,)),
        ],
        compiler_params=pltpu.CompilerParams(collective_id=0, has_side_effects=True, vmem_limit_bytes=63 * MIB),
        cost_estimate=pl.CostEstimate(flops=2 * seq * d_model * width * 3 + 4 * seq * seq * width, bytes_accessed=16 * MIB, transcendentals=0),
    )(x_blk, w_q, w_k, w_v, w_o, flag)


def moe_block(h_ref, rl_ref, rc_ref, g_ref, meta_ref, wg_hbm, wu_hbm, wd_hbm, y_ref, send, recv, zbuf, ret,
              meta_in, sp_send, sp_recv, sp_z, sp_ret, pool_in, xs, zacc, acc, wg, wu, wd, ds, dr, rs, rr, ms, mr, sp_sem, sp_dr, pool_s, pool_r, sp_rs, sp_rr, wsem, *, main, spill):
    cp, tp = lax.axis_index('cp'), lax.axis_index('tp')
    xx, cc = tp // 2, tp % 2
    me = cp * 4 + tp
    chunks, ndev, crow, d_model = send.shape
    rows_all = ndev * crow
    toks = h_ref.shape[0]
    experts = wg_hbm.shape[0]
    slots, _, ff_half = wg.shape
    sp_rows = sp_send.shape[1]
    sp_base = chunks * rows_all
    steps = 2 * experts
    tile = 512
    f32, bf16 = jnp.float32, jnp.bfloat16

    def weights(n):
        e, f, slot = n // 2, n % 2, n % slots
        fcols = pl.ds(pl.multiple_of(f * ff_half, ff_half), ff_half)
        return (pltpu.make_async_copy(wg_hbm.at[e, :, fcols], wg.at[slot], wsem.at[slot, 0]),
                pltpu.make_async_copy(wu_hbm.at[e, :, fcols], wu.at[slot], wsem.at[slot, 1]),
                pltpu.make_async_copy(wd_hbm.at[e, fcols, :], wd.at[slot], wsem.at[slot, 2]))

    def fetch(n):
        for copy in weights(n):
            copy.start()

    for n in range(slots - 1):
        fetch(n)

    def peer_of(j):
        return (me + j) % ndev

    def dev(p):
        return {'cp': p // 4, 'tp': p % 4}

    barrier = pltpu.get_barrier_semaphore()
    for j in range(1, ndev):
        pl.semaphore_signal(barrier, inc=1, device_id=dev(peer_of(j)), device_id_type=MESH)
    pl.semaphore_wait(barrier, ndev - 1)

    AWAY = [(1, 0), (0, 1), (1, 1)]

    def chip(dx, dy):
        return ((cp + dy) % 2) * 2 + (xx + dx) % 2

    def idx(dx, dy, dc):
        return chip(dx, dy) * 2 + (cc + dc) % 2

    def sp_copy(src, dst, ssem, rsem, target):
        return pltpu.make_async_remote_copy(src_ref=src, dst_ref=dst, send_sem=ssem, recv_sem=rsem, device_id=dev(idx(*target)), device_id_type=MESH)

    def sp_out(n):
        if n < 3:
            return sp_copy(sp_send.at[chip(*AWAY[n])], sp_recv.at[me], sp_sem.at[n], sp_dr.at[me], AWAY[n] + (0,))
        return sp_copy(sp_send.at[chip(0, 0)], sp_recv.at[me], sp_sem.at[3], sp_dr.at[me], (0, 0, 1))

    def sp_pass(n):
        ref = sp_recv.at[idx(*AWAY[n], 0)]
        return sp_copy(ref, ref, sp_sem.at[4 + n], sp_dr.at[idx(*AWAY[n], 0)], (0, 0, 1))

    def sp_arrived(source):
        ref = sp_recv.at[idx(*source)]
        sp_copy(ref, ref, sp_sem.at[0], sp_dr.at[idx(*source)], (0, 0, 1)).wait_recv()

    def sp_pool(n):
        side = ([(0, 0)] + AWAY)[n]
        return sp_copy(sp_z.at[idx(*side, 1)], pool_in.at[n], pool_s.at[n], pool_r.at[n], (0, 0, 1))

    def sp_back(n):
        side = AWAY[n]
        return sp_copy(sp_z.at[idx(*side, 0)], sp_ret.at[chip(0, 0)], sp_rs.at[n], sp_rr.at[chip(0, 0)], side + (0,))

    def meta_copy(j):
        return pltpu.make_async_remote_copy(src_ref=meta_ref.at[peer_of(j) // 2], dst_ref=meta_in.at[me], send_sem=ms.at[j], recv_sem=mr.at[me], device_id=dev(peer_of(j)), device_id_type=MESH)

    if spill:
        for j in range(1, ndev):
            meta_copy(j).start()

    def exchange(src, dst, ssem, rsem, k):
        def copy(j):
            return pltpu.make_async_remote_copy(src_ref=src.at[k, peer_of(j)], dst_ref=dst.at[k, me], send_sem=ssem.at[k, j], recv_sem=rsem.at[k, me], device_id=dev(peer_of(j)), device_id_type=MESH)

        local = pltpu.make_async_copy(src.at[k, me], dst.at[k, me], ssem.at[k, 0])
        return copy, local

    def begin(src, dst, ssem, rsem, k):
        copy, local = exchange(src, dst, ssem, rsem, k)
        local.start()
        for j in range(1, ndev):
            copy(j).start()

    def arrived(src, dst, ssem, rsem, k):
        for j in range(1, ndev):
            pltpu.make_async_remote_copy(src_ref=src.at[k, peer_of(j)], dst_ref=dst.at[k, peer_of(j)], send_sem=ssem.at[k, j], recv_sem=rsem.at[k, peer_of(j)], device_id=dev(peer_of(j)), device_id_type=MESH).wait_recv()
        exchange(src, dst, ssem, rsem, k)[1].wait()

    def left(src, dst, ssem, rsem, k):
        copy, _ = exchange(src, dst, ssem, rsem, k)
        for j in range(1, ndev):
            copy(j).wait_send()

    out_way = (send, recv, ds, dr)
    back_way = (zbuf, ret, rs, rr)

    def sp_own():
        return pltpu.make_async_copy(sp_send.at[chip(0, 0)], sp_recv.at[me], sp_sem.at[7])

    if spill:
        ids = lax.broadcasted_iota(jnp.int32, (4 * sp_rows, toks), 0) + sp_base
        pick = ((ids == rl_ref[0:1, :]) | (ids == rl_ref[1:2, :])).astype(f32).astype(bf16)

        def sp_cols(n, _):
            c = pl.ds(pl.multiple_of(n * tile, tile), tile)
            sp_send[:, :, c] = jnp.dot(pick, h_ref[:, c], preferred_element_type=f32).astype(bf16).reshape(4, sp_rows, tile)
            return 0

        lax.fori_loop(0, d_model // tile, sp_cols, 0)

    def pack(k, _):
        ids = lax.broadcasted_iota(jnp.int32, (rows_all, toks), 0) + k * rows_all
        pick = ((ids == rl_ref[0:1, :]) | (ids == rl_ref[1:2, :])).astype(f32).astype(bf16)

        def cols(n, _):
            c = pl.ds(pl.multiple_of(n * tile, tile), tile)
            rows = jnp.dot(pick, h_ref[:, c], preferred_element_type=f32).astype(bf16)
            send[k, :, :, c] = rows.reshape(ndev, crow, tile)
            return 0

        lax.fori_loop(0, d_model // tile, cols, 0)

        @pl.when(k > 0)
        def _():
            begin(*out_way, k - 1)

        if spill:
            @pl.when(k == 0)
            def _():
                for n in range(4):
                    sp_out(n).start()
                sp_own().start()

        return 0

    lax.fori_loop(0, chunks, pack, 0)
    begin(*out_way, chunks - 1)

    if spill:
        for j in range(1, ndev):
            p = peer_of(j)
            pltpu.make_async_remote_copy(src_ref=meta_in.at[p], dst_ref=meta_in.at[p], send_sem=ms.at[j], recv_sem=mr.at[p], device_id=dev(p), device_id_type=MESH).wait_recv()
        for n in range(3):
            sp_arrived(AWAY[n] + (0,))
            sp_pass(n).start()
        sp_own().wait()
        sp_arrived((0, 0, 1))
        for n in range(3):
            sp_arrived(AWAY[n] + (1,))
        total = meta_ref[me // 2]
        for j in range(1, ndev):
            total = total + meta_in[peer_of(j)]
        code = total[0:1, :].astype(jnp.int32) - 1 - cc * (experts * main)
        lane = lax.broadcasted_iota(jnp.int32, code.shape, 1)
        place = (lane // sp_rows) * main + (code & (main - 1))
        owner = code // main
        sp_z[...] = jnp.zeros_like(sp_z)
    body = ndev * main

    def expert(e, _):
        k = e // 2
        part = pl.ds(pl.multiple_of((e % 2) * main, main), main)

        @pl.when(e % 2 == 0)
        def _():
            arrived(*out_way, k)

        xs[0:body, :] = recv[k, :, part, :].reshape(body, d_model)
        if spill:
            slot_id = lax.broadcasted_iota(jnp.int32, (body, ndev * sp_rows), 0)
            pick = ((slot_id == place) & (owner == e)).astype(f32).astype(bf16)

            def gather(n, _):
                c = pl.ds(pl.multiple_of(n * tile, tile), tile)
                xs[body:2 * body, c] = jnp.dot(pick, sp_recv[:, :, c].reshape(ndev * sp_rows, tile), preferred_element_type=f32).astype(bf16)
                return 0

            lax.fori_loop(0, d_model // tile, gather, 0)

        for f in range(2):
            n = 2 * e + f
            slot = n % slots
            for copy in weights(n):
                copy.wait()

            @pl.when(n + slots - 1 < steps)
            def _():
                fetch(n + slots - 1)

            x = xs[...]
            gate = jnp.dot(x, wg[slot], preferred_element_type=f32)
            up = jnp.dot(x, wu[slot], preferred_element_type=f32)
            u = (gate * jax.nn.sigmoid(gate) * up).astype(bf16)

            def down(n, _):
                c = pl.ds(pl.multiple_of(n * tile, tile), tile)
                z = jnp.dot(u, wd[slot, :, c], preferred_element_type=f32)
                if f == 0:
                    zacc[:, c] = z
                else:
                    z = (zacc[:, c] + z).astype(bf16)
                    zbuf[k, :, part, c] = z[0:body].reshape(ndev, main, tile)
                    if spill:
                        spread = lax.dot_general(pick, z[body:], (((0,), (0,)), ((), ())), preferred_element_type=f32)
                        sp_z[:, :, c] = sp_z[:, :, c] + spread.astype(bf16).reshape(ndev, sp_rows, tile)
                return 0

            lax.fori_loop(0, d_model // tile, down, 0)
            if f == 0:
                @pl.when((e % 2 == 0) & (e > 0))
                def _():
                    begin(*back_way, k - 1)

        return 0

    lax.fori_loop(0, experts, expert, 0)
    if spill:
        for n in range(4):
            sp_pool(n).start()
    begin(*back_way, chunks - 1)
    acc[...] = jnp.zeros_like(acc)

    def sp_home():
        return pltpu.make_async_copy(sp_z.at[me], sp_ret.at[chip(0, 0)], sp_rs.at[3])

    if spill:
        for n in range(4):
            sp_pool(n).wait_recv()
            at = idx(*([(0, 0)] + AWAY)[n], 0)
            sp_z[at] = sp_z[at] + pool_in[n]
        for n in range(3):
            sp_back(n).start()
        sp_home().start()

    def chosen(ids, z):
        z0 = jnp.dot((ids == rc_ref[:, 0:1]).astype(f32).astype(bf16), z, preferred_element_type=f32)
        z1 = jnp.dot((ids == rc_ref[:, 1:2]).astype(f32).astype(bf16), z, preferred_element_type=f32)
        return g_ref[:, 0:1] * z0 + g_ref[:, 1:2] * z1

    def combine(k, _):
        arrived(*back_way, k)
        ids = lax.broadcasted_iota(jnp.int32, (toks, rows_all), 1) + k * rows_all

        def cols(n, _):
            c = pl.ds(pl.multiple_of(n * tile, tile), tile)
            acc[:, c] += chosen(ids, ret[k, :, :, c].reshape(rows_all, tile))
            return 0

        lax.fori_loop(0, d_model // tile, cols, 0)
        return 0

    lax.fori_loop(0, chunks, combine, 0)
    if spill:
        sp_home().wait()
        for n in range(3):
            ref = sp_ret.at[chip(*AWAY[n])]
            sp_copy(ref, ref, sp_rs.at[n], sp_rr.at[chip(*AWAY[n])], (0, 0, 1)).wait_recv()

    def finish(n, _):
        c = pl.ds(pl.multiple_of(n * tile, tile), tile)
        moe_out = acc[:, c]
        if spill:
            ids = lax.broadcasted_iota(jnp.int32, (toks, 4 * sp_rows), 1) + sp_base
            moe_out += chosen(ids, sp_ret[:, :, c].reshape(4 * sp_rows, tile))
        y_ref[:, c] = (h_ref[:, c].astype(f32) + moe_out).astype(bf16)
        return 0

    lax.fori_loop(0, d_model // tile, finish, 0)

    def drain(k, _):
        left(*out_way, k)
        left(*back_way, k)
        return 0

    lax.fori_loop(0, chunks, drain, 0)
    if spill:
        for j in range(1, ndev):
            meta_copy(j).wait_send()
        for n in range(4):
            sp_out(n).wait_send()
            sp_pool(n).wait_send()
        for n in range(3):
            sp_pass(n).wait_send()
            sp_back(n).wait_send()


def moe(hidden, rows, gates, meta, w_gate, w_up, w_down, ndev, main, spill):
    toks, d_model = hidden.shape
    experts, _, ff = w_gate.shape
    crow = 2 * main
    chunks = experts // 2
    sp_rows = 2 * main if spill else 16
    slots = 3 if spill else 2
    vm = pl.BlockSpec(memory_space=pltpu.VMEM)
    hbm = pl.BlockSpec(memory_space=pl.ANY)
    bf16, f32 = jnp.bfloat16, jnp.float32
    dma = pltpu.SemaphoreType.DMA
    buf = pltpu.VMEM((chunks, ndev, crow, d_model), bf16)
    tile_rows = 2 * ndev * main if spill else ndev * main
    rows_lane = jnp.pad(rows.T, ((0, 6), (0, 0)), constant_values=-1)
    return pl.pallas_call(
        functools.partial(moe_block, main=main, spill=spill),
        name='moe_spill' if spill else 'moe_full',
        out_shape=jax.ShapeDtypeStruct((toks, d_model), bf16),
        in_specs=[vm] * 5 + [hbm] * 3,
        out_specs=vm,
        scratch_shapes=[
            buf, buf, buf, buf, pltpu.VMEM((ndev,) + meta.shape[1:], f32),
            pltpu.VMEM((4, sp_rows, d_model), bf16), pltpu.VMEM((ndev, sp_rows, d_model), bf16), pltpu.VMEM((ndev, sp_rows, d_model), bf16),
            pltpu.VMEM((4, sp_rows, d_model), bf16), pltpu.VMEM((4, sp_rows, d_model), bf16),
            pltpu.VMEM((tile_rows, d_model), bf16), pltpu.VMEM((tile_rows, d_model), f32), pltpu.VMEM((toks, d_model), f32),
            pltpu.VMEM((slots, d_model, ff // 2), bf16), pltpu.VMEM((slots, d_model, ff // 2), bf16), pltpu.VMEM((slots, ff // 2, d_model), bf16),
            dma((chunks, ndev)), dma((chunks, ndev)), dma((chunks, ndev)), dma((chunks, ndev)), dma((ndev,)), dma((ndev,)),
            dma((8,)), dma((ndev,)), dma((4,)), dma((4,)), dma((4,)), dma((4,)), dma((slots, 3)),
        ],
        compiler_params=pltpu.CompilerParams(collective_id=1 if spill else 2, has_side_effects=True, vmem_limit_bytes=63 * MIB),
        cost_estimate=pl.CostEstimate(flops=6 * tile_rows * experts * d_model * ff, bytes_accessed=6 * experts * d_model * ff, transcendentals=0),
    )(hidden, rows_lane, rows, gates, meta, w_gate, w_up, w_down)


def solution(mesh):
    cp_size = mesh.shape['cp']
    tp_size = mesh.shape['tp']
    num_devs = cp_size * tp_size
    row_spec = P(('data', 'cp', 'tp'), None)
    head_spec = P(None, 'tp', None)
    wo_spec = P('tp', None, None)
    expert_spec = P(('cp', 'tp'), None, None)

    def device_fn(x_blk, w_q, w_k, w_v, w_o, idx_blk, gate_blk, w_gate, w_up, w_down):
        tok_dev, d_model = x_blk.shape
        heads_tp, head_dim = w_q.shape[1], w_q.shape[2]
        heads = heads_tp // cp_size
        exp_local = w_gate.shape[0]
        num_exp = exp_local * num_devs
        capacity = 4 * tok_dev // num_exp
        mean = capacity // 2
        crow = 2 * mean
        cp_rank = lax.axis_index('cp')
        me = cp_rank * tp_size + lax.axis_index('tp')

        flat = idx_blk.reshape(-1)
        count = flat.shape[0]
        onehot = flat[:, None] == jnp.arange(num_exp)[None, :]
        before = (jnp.arange(count)[:, None] > jnp.arange(count)[None, :]).astype(jnp.bfloat16)
        ranks = jnp.dot(before, onehot.astype(jnp.bfloat16), preferred_element_type=jnp.float32)
        pos = jnp.sum(jnp.where(onehot, ranks, 0.0), axis=1).astype(jnp.int32)
        dest, local = flat // exp_local, flat % exp_local
        over = pos >= mean
        chips = num_devs // 2
        onehot = (dest[:, None] // 2 == jnp.arange(chips)[None, :]) & over[:, None]
        ranks = jnp.dot(before, onehot.astype(jnp.bfloat16), preferred_element_type=jnp.float32)
        spill_pos = jnp.sum(jnp.where(onehot, ranks, 0.0), axis=1).astype(jnp.int32)
        flag = jnp.full((8, 128), jnp.max(jnp.sum(onehot.astype(jnp.float32), axis=0)))
        main_rows = exp_local // 2 * num_devs * crow
        rows_spill = jnp.where(over, main_rows + dest // 2 * crow + spill_pos, ((local // 2) * num_devs + dest) * crow + (local % 2) * mean + pos)
        rows_full = ((local // 2) * num_devs + dest) * (2 * capacity) + (local % 2) * capacity + pos
        slot = main_rows + jnp.arange(chips * crow)
        lane = jnp.arange(num_devs * crow)
        code = jnp.sum(jnp.where((rows_spill[:, None] == slot[None, :]) & over[:, None], (1 + (dest % 2 * exp_local + local) * mean + pos - mean)[:, None], 0), axis=0).astype(jnp.float32)
        meta = jnp.where(lane[None, :] // crow == me, jnp.tile(code.reshape(chips, crow), (1, num_devs)), 0.0)
        meta = jnp.broadcast_to(meta[:, None, :], (chips, 8, num_devs * crow))

        hidden, most = attention_block(x_blk, w_q, w_k, w_v, w_o.reshape(-1, d_model), flag, heads, head_dim, num_devs)

        def run(rows, main, spill):
            return lambda h: moe(h, rows.reshape(tok_dev, 2), gate_blk, meta, w_gate, w_up, w_down, num_devs, main, spill)

        return lax.cond(most[0, 0] <= crow, run(rows_spill, mean, True), run(rows_full, capacity, False), hidden)

    return jax.shard_map(device_fn, mesh=mesh, in_specs=(row_spec, head_spec, head_spec, head_spec, wo_spec, row_spec, row_spec, expert_spec, expert_spec, expert_spec), out_specs=row_spec, check_vma=False)
```

```python
import functools
import math

import jax
import jax.numpy as jnp
from jax import lax
from jax.experimental import pallas as pl
from jax.experimental.pallas import tpu as pltpu
from jax.sharding import PartitionSpec as P

MESH = pl.DeviceIdType.MESH
MIB = 1024 * 1024
QB = 512


def lane_fold(s, op):
    out = s[:, :128]
    for g in range(1, s.shape[1] // 128):
        out = op(out, s[:, g * 128:(g + 1) * 128])
    return out


def attn_block(x_hbm, wq_hbm, wk_hbm, wv_hbm, wo_hbm, ids_ref, gates_ref, h_ref, any_ref, lane_ref, col_ref, meta_ref, xbuf, wqkv_ref, w_pair, qkv, s_ref, acc_ref, o_loc, o_cat, wo_buf,
               flag_ref, flags, tall, loc_sem, xs, xr, ws, wr, os_sem, or_sem, fs, fr, *, heads, head_dim, experts):
    cp, tp = lax.axis_index('cp'), lax.axis_index('tp')
    xx, cc = tp // 2, tp % 2
    me = cp * 4 + tp
    ndev, rows, d_model = xbuf.shape
    half_rows = rows // 2
    quarter = half_rows // 2
    width = heads * head_dim
    seq = ndev * rows
    wrows = wo_hbm.shape[0]
    whalf, wquart = wrows // 2, wrows // 4

    def tp_of(dx, dc):
        return ((xx + dx) % 2) * 2 + (cc + dc) % 2

    def idx(dx, dy, dc):
        return ((cp + dy) % 2) * 4 + tp_of(dx, dc)

    def dev(dx, dy, dc):
        return {'cp': (cp + dy) % 2, 'tp': tp_of(dx, dc)}

    x_load = pltpu.make_async_copy(x_hbm, xbuf.at[me], loc_sem.at[0])
    wo_load = pltpu.make_async_copy(wo_hbm, wo_buf.at[pl.ds(tp * wrows, wrows)], loc_sem.at[1])
    x_load.start()
    wo_load.start()
    w_loads = [pltpu.make_async_copy(w.at[:, pl.ds(heads * cp, heads), :], w_pair, loc_sem.at[2]) for w in (wq_hbm, wk_hbm, wv_hbm)]
    w_loads[0].start()

    barrier = pltpu.get_barrier_semaphore()
    for k in range(1, ndev):
        peer = (me + k) % ndev
        pl.semaphore_signal(barrier, inc=1, device_id={'cp': peer // 4, 'tp': peer % 4}, device_id_type=MESH)
    pl.semaphore_wait(barrier, ndev - 1)

    def xcopy(slot, owner, row0, count, part, target):
        ref = xbuf.at[idx(*owner), pl.ds(row0 if isinstance(row0, int) else pl.multiple_of(row0, quarter), count)]
        return pltpu.make_async_remote_copy(src_ref=ref, dst_ref=ref, send_sem=xs.at[slot], recv_sem=xr.at[idx(*owner), part], device_id=dev(*target), device_id_type=MESH)

    XN, YN, CN, DG, OWN = (1, 0, 0), (0, 1, 0), (0, 0, 1), (1, 1, 0), (0, 0, 0)
    XC, YC, DC = (1, 0, 1), (0, 1, 1), (1, 1, 1)
    H, Q = half_rows, quarter
    sends = [
        (OWN, 0, H, 0, XN), (OWN, H, Q, 2, XN), (OWN, 0, H, 0, YN), (OWN, H, Q, 2, YN), (OWN, 0, H, 0, CN), (OWN, H, H, 2, CN),
        (XN, 0, H, 0, CN), (XN, H, H, 2, CN), (YN, 0, H, 0, CN), (YN, H, H, 2, CN),
        (YN, 0, Q, 0, XN), (YN, H, Q, 2, XN), (XN, Q, Q, 1, YN), (XN, H + Q, Q, 3, YN),
        (DG, 0, H, 0, CN), (DG, H, H, 2, CN), (OWN, H + Q, Q, 3, XN), (OWN, H + Q, Q, 3, YN),
    ]

    def send(*slots):
        for slot in slots:
            xcopy(slot, *sends[slot]).start()

    def arrive(owner, row0, count, part):
        xcopy(0, owner, row0, count, part, CN).wait_recv()

    def wcopy(slot, shard, row0, count, sem, target):
        ref = wo_buf.at[pl.ds(shard * wrows + row0, count)]
        return pltpu.make_async_remote_copy(src_ref=ref, dst_ref=ref, send_sem=ws.at[slot], recv_sem=wr.at[sem], device_id=dev(*target), device_id_type=MESH)

    def flag_copy(j):
        peer = (me + j) % ndev
        return pltpu.make_async_remote_copy(src_ref=flag_ref, dst_ref=flags.at[me], send_sem=fs.at[j], recv_sem=fr.at[me], device_id={'cp': peer // 4, 'tp': peer % 4}, device_id_type=MESH)

    x_load.wait()
    send(0, 2, 4, 1, 3, 5)
    wo_load.wait()
    w_own = wcopy(0, tp, 0, wrows, 0, CN)
    w_own.start()

    for kind in range(3):
        w_loads[kind].wait()

        def relayout(n, _):
            r = pl.ds(pl.multiple_of(n * 256, 256), 256)
            for h in range(heads):
                c = kind * width + h * head_dim
                wqkv_ref[r, c:c + head_dim] = w_pair[r, h, :]
            return 0

        lax.fori_loop(0, d_model // 256, relayout, 0)
        if kind < 2:
            w_loads[kind + 1].start()

    def tables():
        toks = ids_ref.shape[1]
        f32, bf16 = jnp.float32, jnp.bfloat16
        cap = 4 * toks // experts
        mean = cap // 2
        per_dev = experts // ndev
        chips = ndev // 2
        crow = 2 * mean
        base = per_dev // 2 * ndev * crow
        before = (lax.broadcasted_iota(jnp.int32, (toks, toks), 0) < lax.broadcasted_iota(jnp.int32, (toks, toks), 1)).astype(f32).astype(bf16)

        def ranks(keys, keep, size):
            out, seen = [], jnp.zeros((size, 1), f32)
            for key, ok in zip(keys, keep):
                hot = jnp.where((lax.broadcasted_iota(jnp.int32, (size, toks), 0) == key) & ok, 1.0, 0.0)
                prior = jnp.dot(hot.astype(bf16), before, preferred_element_type=f32) + seen
                out.append(jnp.sum(hot * prior, axis=0, keepdims=True).astype(jnp.int32))
                seen = seen + jnp.sum(hot, axis=1, keepdims=True)
            return out, seen

        ids = [ids_ref[c:c + 1, :] for c in range(2)]
        pos, _ = ranks(ids, [i >= 0 for i in ids], experts)
        over = [p >= mean for p in pos]
        dest = [i // per_dev for i in ids]
        local = [i - d * per_dev for i, d in zip(ids, dest)]
        spot, seen = ranks([d // 2 for d in dest], over, 8)
        flag_ref[...] = jnp.broadcast_to(jnp.max(seen, axis=0, keepdims=True), flag_ref.shape)
        rows, full, codes = [], [], []
        for p, v, d, l, q in zip(pos, over, dest, local, spot):
            pair = l // 2 * ndev + d
            rows.append(jnp.where(v, base + d // 2 * crow + q, pair * crow + l % 2 * mean + p))
            full.append(pair * 2 * cap + l % 2 * cap + p)
            codes.append(jnp.where(v, 1 + (d % 2 * per_dev + l) * mean + p - mean, 0))
        for n, row in enumerate(rows + full):
            lane_ref[n:n + 1, :] = row
        tall[...] = jnp.zeros_like(tall)
        for n, row in enumerate(rows + full + [gates_ref[c:c + 1, :] for c in range(2)]):
            tall[n:n + 1, :] = row.astype(f32)
        col_ref[...] = tall[...].T
        lane = lax.broadcasted_iota(jnp.int32, (toks, ndev * crow), 1)
        for chip in range(chips):
            total = jnp.zeros(meta_ref.shape[1:], f32)
            for c in range(2):
                place = col_ref[:, c:c + 1].astype(jnp.int32) - (base + chip * crow) + me * crow
                hot = ((place == lane) & (lane // crow == me)).astype(f32).astype(bf16)
                code = jnp.broadcast_to(codes[c].astype(f32), (8, toks)).astype(bf16)
                total += jnp.dot(code, hot, preferred_element_type=f32)
            meta_ref[chip] = total

    def project(owner, half):
        r, t = owner // 4, owner % 4
        seg = r + half * (3 - 2 * r)
        x = xbuf[owner, pl.ds(pl.multiple_of(half * half_rows, half_rows), half_rows), :]
        out = jnp.dot(x, wqkv_ref[...], preferred_element_type=jnp.float32).astype(jnp.bfloat16)
        qkv[pl.ds(pl.multiple_of((seg * 4 + t) * half_rows, half_rows), half_rows), :] = out

    def near(s, _):
        @pl.when(s == 2)
        def _():
            arrive(CN, 0, half_rows, 0)

        @pl.when(s == 3)
        def _():
            arrive(CN, half_rows, half_rows, 2)

        project(idx(0, 0, s // 2), s % 2)
        return 0

    lax.fori_loop(0, 4, near, 0)
    tables()
    for j in range(1, ndev):
        flag_copy(j).start()

    w_x = [(1 + k, tp, cp * whalf + k * wquart, wquart, 1 + k, XN) for k in range(2)]

    def gather(p):
        base = p * half_rows

        @pl.when(p == 0)
        def _():
            arrive(XN, 0, H, 0)
            arrive(YN, 0, H, 0)
            send(12, 10, 16, 17, 6, 8)

        def mid(u, _):
            @pl.when(u == 2)
            def _():
                arrive(XC, base, H, 2 * p)

            @pl.when(u == 3)
            def _():
                arrive(YC, base, H, 2 * p)

            project(idx(1 - u % 2, u % 2, u // 2), p)
            return 0

        lax.fori_loop(0, 4, mid, 0)

        @pl.when(p == 0)
        def _():
            arrive(XN, H, Q, 2)
            arrive(YN, H, Q, 2)
            send(11)

        arrive(DG, base, Q, 2 * p)
        arrive(DG, base + Q, Q, 2 * p + 1)

        @pl.when(p == 0)
        def _():
            send(14)

        @pl.when(p == 1)
        def _():
            send(15)

        def far(u, _):
            @pl.when(u == 1)
            def _():
                arrive(DC, base, H, 2 * p)

            project(idx(1, 1, u), p)
            return 0

        lax.fori_loop(0, 2, far, 0)

    def late():
        arrive(XN, H + Q, Q, 3)
        arrive(YN, H + Q, Q, 3)
        send(13, 7, 9)
        for spec in w_x:
            wcopy(*spec).start()

    coef = (head_dim ** -0.5) * math.log2(math.e)
    my_col = (4 * tp + 2 * cp) * head_dim

    def o_place(b):
        seg, t = b // 4, b % 4
        half = seg // 2
        return seg + half * (3 - 2 * seg), t, half

    def o_remote(b):
        r, t, half = o_place(b)
        return pltpu.make_async_remote_copy(
            src_ref=o_loc.at[pl.ds(pl.multiple_of(b * half_rows, half_rows), half_rows)],
            dst_ref=o_cat.at[pl.ds(pl.multiple_of(half * half_rows, half_rows), half_rows), pl.ds(pl.multiple_of(my_col, width), width)],
            send_sem=os_sem.at[b], recv_sem=or_sem.at[me, half], device_id={'cp': r, 'tp': t}, device_id_type=MESH)

    def o_local(b):
        _, _, half = o_place(b)
        return pltpu.make_async_copy(
            o_loc.at[pl.ds(pl.multiple_of(b * half_rows, half_rows), half_rows)],
            o_cat.at[pl.ds(pl.multiple_of(half * half_rows, half_rows), half_rows), pl.ds(pl.multiple_of(my_col, width), width)],
            os_sem.at[b])

    def o_send(i):
        for part in range(QB // half_rows):
            b = i * (QB // half_rows) + part
            r, t, _ = o_place(b)

            @pl.when(r * 4 + t != me)
            def _():
                o_remote(b).start()

            @pl.when(r * 4 + t == me)
            def _():
                o_local(b).start()

    peer_t = tp_of(1, 0)
    peer_c = tp_of(1, 1)

    def w_pass(k):
        wcopy(1, peer_t, cp * whalf + k * wquart, wquart, 1 + k, CN).wait_recv()
        wcopy(3 + k, peer_t, cp * whalf + k * wquart, wquart, 3 + k, YN).start()
        wcopy(5 + k, peer_t, cp * whalf + k * wquart, wquart, 5 + k, CN).start()

    def w_last(k):
        wcopy(1, peer_t, (1 - cp) * whalf + k * wquart, wquart, 3 + k, CN).wait_recv()
        wcopy(7 + k, peer_t, (1 - cp) * whalf + k * wquart, wquart, 7 + k, CN).start()

    blocks = seq // QB

    def q_step(i, _):
        @pl.when(i == blocks // 2 - 1)
        def _():
            late()
            for early in range(blocks // 2 - 1):
                o_send(early)

        @pl.when(i == blocks - 3)
        def _():
            w_pass(0)

        @pl.when(i == blocks - 1)
        def _():
            w_pass(1)

        q_rows = pl.ds(pl.multiple_of(i * QB, QB), QB)

        def cols(kind, h):
            return slice(kind * width + h * head_dim, kind * width + (h + 1) * head_dim)

        def scores(h, j):
            k = qkv[pl.ds(pl.multiple_of(j * QB, QB), QB), cols(1, h)]
            return lax.dot_general(qkv[q_rows, cols(0, h)], k, (((1,), (1,)), ((), ())), preferred_element_type=jnp.float32)

        def pass1(j, ms):
            out = []
            for h in range(heads):
                s = scores(h, j)
                s_ref[h, :, pl.ds(pl.multiple_of(j * QB, QB), QB)] = s
                out.append(jnp.maximum(ms[h], lane_fold(s, jnp.maximum)))
            return tuple(out)

        ms = lax.fori_loop(0, i, pass1, tuple(jnp.full((QB, 128), -jnp.inf, jnp.float32) for _ in range(heads)))
        keep = lax.broadcasted_iota(jnp.int32, (QB, QB), 1) <= lax.broadcasted_iota(jnp.int32, (QB, QB), 0)
        tops = []
        for h in range(heads):
            s = jnp.where(keep, scores(h, i), -jnp.inf)
            s_ref[h, :, pl.ds(pl.multiple_of(i * QB, QB), QB)] = s
            tops.append(jnp.max(jnp.maximum(ms[h], lane_fold(s, jnp.maximum)), axis=1, keepdims=True))
        acc_ref[...] = jnp.zeros_like(acc_ref)

        def pass2(j, ls):
            out = []
            for h in range(heads):
                e = jnp.exp2((s_ref[h, :, pl.ds(pl.multiple_of(j * QB, QB), QB)] - tops[h]) * coef)
                v = qkv[pl.ds(pl.multiple_of(j * QB, QB), QB), cols(2, h)]
                acc_ref[h] += jnp.dot(e.astype(jnp.bfloat16), v, preferred_element_type=jnp.float32)
                out.append(ls[h] + lane_fold(e, jnp.add))
            return tuple(out)

        ls = lax.fori_loop(0, i + 1, pass2, tuple(jnp.zeros((QB, 128), jnp.float32) for _ in range(heads)))
        for h in range(heads):
            total = jnp.sum(ls[h], axis=1, keepdims=True)
            o_loc[q_rows, h * head_dim:(h + 1) * head_dim] = (acc_ref[h] / total).astype(jnp.bfloat16)

        @pl.when(i >= blocks // 2 - 1)
        def _():
            o_send(i)

        return 0

    def phase(p, _):
        gather(p)
        lax.fori_loop(p * (blocks // 2), (p + 1) * (blocks // 2), q_step, 0)
        return 0

    lax.fori_loop(0, 2, phase, 0)

    w_last(0)
    w_last(1)
    wcopy(1, tp_of(0, 1), 0, wrows, 0, CN).wait_recv()
    for k in range(2):
        wcopy(1, peer_c, cp * whalf + k * wquart, wquart, 5 + k, CN).wait_recv()
        wcopy(1, peer_c, (1 - cp) * whalf + k * wquart, wquart, 7 + k, CN).wait_recv()
    for k in range(1, ndev):
        src = (me + k) % ndev
        col = (4 * (src % 4) + 2 * (src // 4)) * head_dim
        for half in range(2):
            ref = o_cat.at[pl.ds(half * half_rows, half_rows), pl.ds(pl.multiple_of(col, width), width)]
            pltpu.make_async_remote_copy(src_ref=ref, dst_ref=ref, send_sem=os_sem.at[0], recv_sem=or_sem.at[src, half], device_id=dev(0, 0, 1), device_id_type=MESH).wait_recv()

    def drain(b, _):
        r, t, _half = o_place(b)

        @pl.when(r * 4 + t != me)
        def _():
            o_remote(b).wait_send()

        @pl.when(r * 4 + t == me)
        def _():
            o_local(b).wait()

        return 0

    lax.fori_loop(0, seq // half_rows, drain, 0)

    tile = 256

    def out_step(n, _):
        c = pl.ds(pl.multiple_of(n * tile, tile), tile)
        a = jnp.dot(o_cat[...], wo_buf[:, c], preferred_element_type=jnp.float32)
        h_ref[:, c] = (xbuf[me, :, c].astype(jnp.float32) + a).astype(jnp.bfloat16)
        return 0

    lax.fori_loop(0, d_model // tile, out_step, 0)

    most = flag_ref[...]
    for j in range(1, ndev):
        peer = (me + j) % ndev
        pltpu.make_async_remote_copy(src_ref=flag_ref, dst_ref=flags.at[peer], send_sem=fs.at[j], recv_sem=fr.at[peer], device_id=dev(0, 0, 1), device_id_type=MESH).wait_recv()
        most = jnp.maximum(most, flags[peer])
        flag_copy(j).wait_send()
    any_ref[0, 0] = jnp.max(most).astype(jnp.int32)

    for slot in range(len(sends)):
        xcopy(slot, *sends[slot]).wait_send()
    w_own.wait_send()
    for spec in w_x:
        wcopy(*spec).wait_send()
    for k in range(2):
        wcopy(3 + k, peer_t, cp * whalf + k * wquart, wquart, 3 + k, YN).wait_send()
        wcopy(5 + k, peer_t, cp * whalf + k * wquart, wquart, 5 + k, CN).wait_send()
        wcopy(7 + k, peer_t, (1 - cp) * whalf + k * wquart, wquart, 7 + k, CN).wait_send()


def attention_block(x_blk, w_q, w_k, w_v, w_o, ids, gates, heads, head_dim, ndev, experts):
    rows, d_model = x_blk.shape
    seq = rows * ndev
    width = heads * head_dim
    vm = pl.BlockSpec(memory_space=pltpu.VMEM)
    hbm = pl.BlockSpec(memory_space=pl.ANY)
    bf16, f32 = jnp.bfloat16, jnp.float32
    dma = pltpu.SemaphoreType.DMA
    return pl.pallas_call(
        functools.partial(attn_block, heads=heads, head_dim=head_dim, experts=experts),
        name='attn_block',
        out_shape=(jax.ShapeDtypeStruct((rows, d_model), bf16), jax.ShapeDtypeStruct((1, 1), jnp.int32), jax.ShapeDtypeStruct((8, rows), jnp.int32), jax.ShapeDtypeStruct((rows, 128), f32), jax.ShapeDtypeStruct((ndev // 2, 8, rows * ndev * 4 // experts), f32)),
        in_specs=[hbm] * 5 + [vm] * 2,
        out_specs=(vm, pl.BlockSpec(memory_space=pltpu.SMEM), vm, vm, vm),
        scratch_shapes=[
            pltpu.VMEM((ndev, rows, d_model), bf16), pltpu.VMEM((d_model, 3 * width), bf16), pltpu.VMEM((d_model, heads, head_dim), bf16), pltpu.VMEM((seq, 3 * width), bf16),
            pltpu.VMEM((heads, QB, seq), f32), pltpu.VMEM((heads, QB, head_dim), f32),
            pltpu.VMEM((seq, width), bf16), pltpu.VMEM((rows, ndev * width), bf16),
            pltpu.VMEM((ndev * width, d_model), bf16),
            pltpu.VMEM((8, 128), f32), pltpu.VMEM((ndev, 8, 128), f32), pltpu.VMEM((128, rows), f32),
            dma((3,)), dma((18,)), dma((ndev, 4)), dma((9,)), dma((9,)), dma((16,)), dma((ndev, 2)), dma((ndev,)), dma((ndev,)),
        ],
        compiler_params=pltpu.CompilerParams(collective_id=0, has_side_effects=True, vmem_limit_bytes=63 * MIB),
        cost_estimate=pl.CostEstimate(flops=2 * seq * d_model * width * 3 + 4 * seq * seq * width, bytes_accessed=16 * MIB, transcendentals=0),
    )(x_blk, w_q, w_k, w_v, w_o, ids, gates)


def moe_block(h_ref, rl_ref, col_ref, meta_ref, wg_hbm, wu_hbm, wd_hbm, y_ref, send, recv, zbuf, ret,
              meta_in, sp_send, sp_recv, sp_z, sp_ret, pool_in, xs, zacc, acc, wg, wu, wd, ds, dr, rs, rr, ms, mr, sp_sem, sp_dr, pool_s, pool_r, sp_rs, sp_rr, wsem, *, main, spill):
    cp, tp = lax.axis_index('cp'), lax.axis_index('tp')
    xx, cc = tp // 2, tp % 2
    me = cp * 4 + tp
    chunks, ndev, crow, d_model = send.shape
    rows_all = ndev * crow
    toks = h_ref.shape[0]
    experts = wg_hbm.shape[0]
    slots, _, ff_half = wg.shape
    sp_rows = sp_send.shape[1]
    sp_base = chunks * rows_all
    c0 = 0 if spill else 2
    steps = 2 * experts
    tile = 512
    f32, bf16 = jnp.float32, jnp.bfloat16

    def weights(n):
        e, f, slot = n // 2, n % 2, n % slots
        fcols = pl.ds(pl.multiple_of(f * ff_half, ff_half), ff_half)
        return (pltpu.make_async_copy(wg_hbm.at[e, :, fcols], wg.at[slot], wsem.at[slot, 0]),
                pltpu.make_async_copy(wu_hbm.at[e, :, fcols], wu.at[slot], wsem.at[slot, 1]),
                pltpu.make_async_copy(wd_hbm.at[e, fcols, :], wd.at[slot], wsem.at[slot, 2]))

    def fetch(n):
        for copy in weights(n):
            copy.start()

    for n in range(slots - 1):
        fetch(n)

    def peer_of(j):
        return (me + j) % ndev

    def dev(p):
        return {'cp': p // 4, 'tp': p % 4}

    barrier = pltpu.get_barrier_semaphore()
    for j in range(1, ndev):
        pl.semaphore_signal(barrier, inc=1, device_id=dev(peer_of(j)), device_id_type=MESH)
    pl.semaphore_wait(barrier, ndev - 1)

    AWAY = [(1, 0), (0, 1), (1, 1)]

    def chip(dx, dy):
        return ((cp + dy) % 2) * 2 + (xx + dx) % 2

    def idx(dx, dy, dc):
        return chip(dx, dy) * 2 + (cc + dc) % 2

    def sp_copy(src, dst, ssem, rsem, target):
        return pltpu.make_async_remote_copy(src_ref=src, dst_ref=dst, send_sem=ssem, recv_sem=rsem, device_id=dev(idx(*target)), device_id_type=MESH)

    def sp_out(n):
        if n < 3:
            return sp_copy(sp_send.at[chip(*AWAY[n])], sp_recv.at[me], sp_sem.at[n], sp_dr.at[me], AWAY[n] + (0,))
        return sp_copy(sp_send.at[chip(0, 0)], sp_recv.at[me], sp_sem.at[3], sp_dr.at[me], (0, 0, 1))

    def sp_pass(n):
        ref = sp_recv.at[idx(*AWAY[n], 0)]
        return sp_copy(ref, ref, sp_sem.at[4 + n], sp_dr.at[idx(*AWAY[n], 0)], (0, 0, 1))

    def sp_arrived(source):
        ref = sp_recv.at[idx(*source)]
        sp_copy(ref, ref, sp_sem.at[0], sp_dr.at[idx(*source)], (0, 0, 1)).wait_recv()

    def sp_pool(n):
        side = ([(0, 0)] + AWAY)[n]
        return sp_copy(sp_z.at[idx(*side, 1)], pool_in.at[n], pool_s.at[n], pool_r.at[n], (0, 0, 1))

    def sp_back(n):
        side = AWAY[n]
        return sp_copy(sp_z.at[idx(*side, 0)], sp_ret.at[chip(0, 0)], sp_rs.at[n], sp_rr.at[chip(0, 0)], side + (0,))

    def meta_copy(j):
        return pltpu.make_async_remote_copy(src_ref=meta_ref.at[peer_of(j) // 2], dst_ref=meta_in.at[me], send_sem=ms.at[j], recv_sem=mr.at[me], device_id=dev(peer_of(j)), device_id_type=MESH)

    if spill:
        for j in range(1, ndev):
            meta_copy(j).start()

    def exchange(src, dst, ssem, rsem, k):
        def copy(j):
            return pltpu.make_async_remote_copy(src_ref=src.at[k, peer_of(j)], dst_ref=dst.at[k, me], send_sem=ssem.at[k, j], recv_sem=rsem.at[k, me], device_id=dev(peer_of(j)), device_id_type=MESH)

        local = pltpu.make_async_copy(src.at[k, me], dst.at[k, me], ssem.at[k, 0])
        return copy, local

    def begin(src, dst, ssem, rsem, k):
        copy, local = exchange(src, dst, ssem, rsem, k)
        local.start()
        for j in range(1, ndev):
            copy(j).start()

    def arrived(src, dst, ssem, rsem, k):
        for j in range(1, ndev):
            pltpu.make_async_remote_copy(src_ref=src.at[k, peer_of(j)], dst_ref=dst.at[k, peer_of(j)], send_sem=ssem.at[k, j], recv_sem=rsem.at[k, peer_of(j)], device_id=dev(peer_of(j)), device_id_type=MESH).wait_recv()
        exchange(src, dst, ssem, rsem, k)[1].wait()

    def left(src, dst, ssem, rsem, k):
        copy, _ = exchange(src, dst, ssem, rsem, k)
        for j in range(1, ndev):
            copy(j).wait_send()

    out_way = (send, recv, ds, dr)
    back_way = (zbuf, ret, rs, rr)

    def sp_own():
        return pltpu.make_async_copy(sp_send.at[chip(0, 0)], sp_recv.at[me], sp_sem.at[7])

    if spill:
        ids = lax.broadcasted_iota(jnp.int32, (4 * sp_rows, toks), 0) + sp_base
        pick = ((ids == rl_ref[c0:c0 + 1, :]) | (ids == rl_ref[c0 + 1:c0 + 2, :])).astype(f32).astype(bf16)

        def sp_cols(n, _):
            c = pl.ds(pl.multiple_of(n * tile, tile), tile)
            sp_send[:, :, c] = jnp.dot(pick, h_ref[:, c], preferred_element_type=f32).astype(bf16).reshape(4, sp_rows, tile)
            return 0

        lax.fori_loop(0, d_model // tile, sp_cols, 0)

    def pack(k, _):
        ids = lax.broadcasted_iota(jnp.int32, (rows_all, toks), 0) + k * rows_all
        pick = ((ids == rl_ref[c0:c0 + 1, :]) | (ids == rl_ref[c0 + 1:c0 + 2, :])).astype(f32).astype(bf16)

        def cols(n, _):
            c = pl.ds(pl.multiple_of(n * tile, tile), tile)
            rows = jnp.dot(pick, h_ref[:, c], preferred_element_type=f32).astype(bf16)
            send[k, :, :, c] = rows.reshape(ndev, crow, tile)
            return 0

        lax.fori_loop(0, d_model // tile, cols, 0)

        @pl.when(k > 0)
        def _():
            begin(*out_way, k - 1)

        if spill:
            @pl.when(k == 0)
            def _():
                for n in range(4):
                    sp_out(n).start()
                sp_own().start()

        return 0

    lax.fori_loop(0, chunks, pack, 0)
    begin(*out_way, chunks - 1)

    if spill:
        for j in range(1, ndev):
            p = peer_of(j)
            pltpu.make_async_remote_copy(src_ref=meta_in.at[p], dst_ref=meta_in.at[p], send_sem=ms.at[j], recv_sem=mr.at[p], device_id=dev(p), device_id_type=MESH).wait_recv()
        for n in range(3):
            sp_arrived(AWAY[n] + (0,))
            sp_pass(n).start()
        sp_own().wait()
        sp_arrived((0, 0, 1))
        for n in range(3):
            sp_arrived(AWAY[n] + (1,))
        total = meta_ref[me // 2]
        for j in range(1, ndev):
            total = total + meta_in[peer_of(j)]
        code = total[0:1, :].astype(jnp.int32) - 1 - cc * (experts * main)
        lane = lax.broadcasted_iota(jnp.int32, code.shape, 1)
        place = (lane // sp_rows) * main + (code & (main - 1))
        owner = code // main
        sp_z[...] = jnp.zeros_like(sp_z)
    body = ndev * main

    def expert(e, _):
        k = e // 2
        part = pl.ds(pl.multiple_of((e % 2) * main, main), main)

        @pl.when(e % 2 == 0)
        def _():
            arrived(*out_way, k)

        xs[0:body, :] = recv[k, :, part, :].reshape(body, d_model)
        if spill:
            slot_id = lax.broadcasted_iota(jnp.int32, (body, ndev * sp_rows), 0)
            pick = ((slot_id == place) & (owner == e)).astype(f32).astype(bf16)

            def gather(n, _):
                c = pl.ds(pl.multiple_of(n * tile, tile), tile)
                xs[body:2 * body, c] = jnp.dot(pick, sp_recv[:, :, c].reshape(ndev * sp_rows, tile), preferred_element_type=f32).astype(bf16)
                return 0

            lax.fori_loop(0, d_model // tile, gather, 0)

        for f in range(2):
            n = 2 * e + f
            slot = n % slots
            for copy in weights(n):
                copy.wait()

            @pl.when(n + slots - 1 < steps)
            def _():
                fetch(n + slots - 1)

            x = xs[...]
            gate = jnp.dot(x, wg[slot], preferred_element_type=f32)
            up = jnp.dot(x, wu[slot], preferred_element_type=f32)
            u = (gate * jax.nn.sigmoid(gate) * up).astype(bf16)

            def down(n, _):
                c = pl.ds(pl.multiple_of(n * tile, tile), tile)
                z = jnp.dot(u, wd[slot, :, c], preferred_element_type=f32)
                if f == 0:
                    zacc[:, c] = z
                else:
                    z = (zacc[:, c] + z).astype(bf16)
                    zbuf[k, :, part, c] = z[0:body].reshape(ndev, main, tile)
                    if spill:
                        spread = lax.dot_general(pick, z[body:], (((0,), (0,)), ((), ())), preferred_element_type=f32)
                        sp_z[:, :, c] = sp_z[:, :, c] + spread.astype(bf16).reshape(ndev, sp_rows, tile)
                return 0

            lax.fori_loop(0, d_model // tile, down, 0)
            if f == 0:
                @pl.when((e % 2 == 0) & (e > 0))
                def _():
                    begin(*back_way, k - 1)

        return 0

    lax.fori_loop(0, experts, expert, 0)
    if spill:
        for n in range(4):
            sp_pool(n).start()
    begin(*back_way, chunks - 1)
    acc[...] = jnp.zeros_like(acc)

    def sp_home():
        return pltpu.make_async_copy(sp_z.at[me], sp_ret.at[chip(0, 0)], sp_rs.at[3])

    if spill:
        for n in range(4):
            sp_pool(n).wait_recv()
            at = idx(*([(0, 0)] + AWAY)[n], 0)
            sp_z[at] = sp_z[at] + pool_in[n]
        for n in range(3):
            sp_back(n).start()
        sp_home().start()

    row0, row1 = (col_ref[:, c:c + 1].astype(jnp.int32) for c in (c0, c0 + 1))

    def chosen(ids, z):
        z0 = jnp.dot((ids == row0).astype(f32).astype(bf16), z, preferred_element_type=f32)
        z1 = jnp.dot((ids == row1).astype(f32).astype(bf16), z, preferred_element_type=f32)
        return col_ref[:, 4:5] * z0 + col_ref[:, 5:6] * z1

    def combine(k, _):
        arrived(*back_way, k)
        ids = lax.broadcasted_iota(jnp.int32, (toks, rows_all), 1) + k * rows_all

        def cols(n, _):
            c = pl.ds(pl.multiple_of(n * tile, tile), tile)
            acc[:, c] += chosen(ids, ret[k, :, :, c].reshape(rows_all, tile))
            return 0

        lax.fori_loop(0, d_model // tile, cols, 0)
        return 0

    lax.fori_loop(0, chunks, combine, 0)
    if spill:
        sp_home().wait()
        for n in range(3):
            ref = sp_ret.at[chip(*AWAY[n])]
            sp_copy(ref, ref, sp_rs.at[n], sp_rr.at[chip(*AWAY[n])], (0, 0, 1)).wait_recv()

    def finish(n, _):
        c = pl.ds(pl.multiple_of(n * tile, tile), tile)
        moe_out = acc[:, c]
        if spill:
            ids = lax.broadcasted_iota(jnp.int32, (toks, 4 * sp_rows), 1) + sp_base
            moe_out += chosen(ids, sp_ret[:, :, c].reshape(4 * sp_rows, tile))
        y_ref[:, c] = (h_ref[:, c].astype(f32) + moe_out).astype(bf16)
        return 0

    lax.fori_loop(0, d_model // tile, finish, 0)

    def drain(k, _):
        left(*out_way, k)
        left(*back_way, k)
        return 0

    lax.fori_loop(0, chunks, drain, 0)
    if spill:
        for j in range(1, ndev):
            meta_copy(j).wait_send()
        for n in range(4):
            sp_out(n).wait_send()
            sp_pool(n).wait_send()
        for n in range(3):
            sp_pass(n).wait_send()
            sp_back(n).wait_send()


def moe(hidden, lane, col, meta, w_gate, w_up, w_down, ndev, main, spill):
    toks, d_model = hidden.shape
    experts, _, ff = w_gate.shape
    crow = 2 * main
    chunks = experts // 2
    sp_rows = 2 * main if spill else 16
    slots = 3 if spill else 2
    vm = pl.BlockSpec(memory_space=pltpu.VMEM)
    hbm = pl.BlockSpec(memory_space=pl.ANY)
    bf16, f32 = jnp.bfloat16, jnp.float32
    dma = pltpu.SemaphoreType.DMA
    buf = pltpu.VMEM((chunks, ndev, crow, d_model), bf16)
    tile_rows = 2 * ndev * main if spill else ndev * main
    return pl.pallas_call(
        functools.partial(moe_block, main=main, spill=spill),
        name='moe_spill' if spill else 'moe_full',
        out_shape=jax.ShapeDtypeStruct((toks, d_model), bf16),
        in_specs=[vm] * 4 + [hbm] * 3,
        out_specs=vm,
        scratch_shapes=[
            buf, buf, buf, buf, pltpu.VMEM((ndev,) + meta.shape[1:], f32),
            pltpu.VMEM((4, sp_rows, d_model), bf16), pltpu.VMEM((ndev, sp_rows, d_model), bf16), pltpu.VMEM((ndev, sp_rows, d_model), bf16),
            pltpu.VMEM((4, sp_rows, d_model), bf16), pltpu.VMEM((4, sp_rows, d_model), bf16),
            pltpu.VMEM((tile_rows, d_model), bf16), pltpu.VMEM((tile_rows, d_model), f32), pltpu.VMEM((toks, d_model), f32),
            pltpu.VMEM((slots, d_model, ff // 2), bf16), pltpu.VMEM((slots, d_model, ff // 2), bf16), pltpu.VMEM((slots, ff // 2, d_model), bf16),
            dma((chunks, ndev)), dma((chunks, ndev)), dma((chunks, ndev)), dma((chunks, ndev)), dma((ndev,)), dma((ndev,)),
            dma((8,)), dma((ndev,)), dma((4,)), dma((4,)), dma((4,)), dma((4,)), dma((slots, 3)),
        ],
        compiler_params=pltpu.CompilerParams(collective_id=1 if spill else 2, has_side_effects=True, vmem_limit_bytes=63 * MIB),
        cost_estimate=pl.CostEstimate(flops=6 * tile_rows * experts * d_model * ff, bytes_accessed=6 * experts * d_model * ff, transcendentals=0),
    )(hidden, lane, col, meta, w_gate, w_up, w_down)


def solution(mesh):
    cp_size = mesh.shape['cp']
    tp_size = mesh.shape['tp']
    num_devs = cp_size * tp_size
    row_spec = P(('data', 'cp', 'tp'), None)
    head_spec = P(None, 'tp', None)
    wo_spec = P('tp', None, None)
    expert_spec = P(('cp', 'tp'), None, None)

    def device_fn(x_blk, w_q, w_k, w_v, w_o, idx_blk, gate_blk, w_gate, w_up, w_down):
        tok_dev, d_model = x_blk.shape
        heads_tp, head_dim = w_q.shape[1], w_q.shape[2]
        heads = heads_tp // cp_size
        exp_local = w_gate.shape[0]
        num_exp = exp_local * num_devs
        capacity = 4 * tok_dev // num_exp
        mean = capacity // 2
        crow = 2 * mean
        hidden, most, lane, col, meta = attention_block(x_blk, w_q, w_k, w_v, w_o.reshape(-1, d_model), idx_blk.T, gate_blk.T, heads, head_dim, num_devs, num_exp)

        def run(main, spill):
            return lambda h: moe(h, lane, col, meta, w_gate, w_up, w_down, num_devs, main, spill)

        return lax.cond(most[0, 0] <= crow, run(mean, True), run(capacity, False), hidden)

    return jax.shard_map(device_fn, mesh=mesh, in_specs=(row_spec, head_spec, head_spec, head_spec, wo_spec, row_spec, row_spec, expert_spec, expert_spec, expert_spec), out_specs=row_spec, check_vma=False)
```

```python
import functools
import math

import jax
import jax.numpy as jnp
from jax import lax
from jax.experimental import pallas as pl
from jax.experimental.pallas import tpu as pltpu
from jax.sharding import PartitionSpec as P

MESH = pl.DeviceIdType.MESH
MIB = 1024 * 1024
QB = 512


def lane_fold(s, op):
    out = s[:, :128]
    for g in range(1, s.shape[1] // 128):
        out = op(out, s[:, g * 128:(g + 1) * 128])
    return out


def attn_block(x_hbm, wq_hbm, wk_hbm, wv_hbm, wo_hbm, ids_ref, gates_ref, h_hbm, any_ref, lane_ref, col_ref, meta_ref, xbuf, wqkv_ref, w_pair, qkv, s_ref, acc_ref, o_loc, o_cat, wo_buf,
               flag_ref, flags, tall, h_ref, h_sem, loc_sem, xs, xr, ws, wr, os_sem, or_sem, fs, fr, *, heads, head_dim, experts):
    cp, tp = lax.axis_index('cp'), lax.axis_index('tp')
    xx, cc = tp // 2, tp % 2
    me = cp * 4 + tp
    ndev, rows, d_model = xbuf.shape
    half_rows = rows // 2
    quarter = half_rows // 2
    width = heads * head_dim
    seq = ndev * rows
    wrows = wo_hbm.shape[0]
    parts = 4
    whalf, wpart = wrows // 2, wrows // 2 // parts

    def tp_of(dx, dc):
        return ((xx + dx) % 2) * 2 + (cc + dc) % 2

    def idx(dx, dy, dc):
        return ((cp + dy) % 2) * 4 + tp_of(dx, dc)

    def dev(dx, dy, dc):
        return {'cp': (cp + dy) % 2, 'tp': tp_of(dx, dc)}

    x_load = pltpu.make_async_copy(x_hbm, xbuf.at[me], loc_sem.at[0])
    wo_load = pltpu.make_async_copy(wo_hbm, wo_buf.at[pl.ds(tp * wrows, wrows)], loc_sem.at[1])
    x_load.start()
    wo_load.start()
    w_loads = [pltpu.make_async_copy(w.at[:, pl.ds(heads * cp, heads), :], w_pair, loc_sem.at[2]) for w in (wq_hbm, wk_hbm, wv_hbm)]
    w_loads[0].start()

    barrier = pltpu.get_barrier_semaphore()
    for k in range(1, ndev):
        peer = (me + k) % ndev
        pl.semaphore_signal(barrier, inc=1, device_id={'cp': peer // 4, 'tp': peer % 4}, device_id_type=MESH)
    pl.semaphore_wait(barrier, ndev - 1)

    def xcopy(slot, owner, row0, count, part, target):
        ref = xbuf.at[idx(*owner), pl.ds(row0 if isinstance(row0, int) else pl.multiple_of(row0, quarter), count)]
        return pltpu.make_async_remote_copy(src_ref=ref, dst_ref=ref, send_sem=xs.at[slot], recv_sem=xr.at[idx(*owner), part], device_id=dev(*target), device_id_type=MESH)

    XN, YN, CN, DG, OWN = (1, 0, 0), (0, 1, 0), (0, 0, 1), (1, 1, 0), (0, 0, 0)
    XC, YC, DC = (1, 0, 1), (0, 1, 1), (1, 1, 1)
    H, Q = half_rows, quarter
    sends = [
        (OWN, 0, H, 0, XN), (OWN, H, Q, 2, XN), (OWN, 0, H, 0, YN), (OWN, H, Q, 2, YN), (OWN, 0, H, 0, CN), (OWN, H, H, 2, CN),
        (XN, 0, H, 0, CN), (XN, H, H, 2, CN), (YN, 0, H, 0, CN), (YN, H, H, 2, CN),
        (YN, 0, Q, 0, XN), (YN, H, Q, 2, XN), (XN, Q, Q, 1, YN), (XN, H + Q, Q, 3, YN),
        (DG, 0, H, 0, CN), (DG, H, H, 2, CN), (OWN, H + Q, Q, 3, XN), (OWN, H + Q, Q, 3, YN),
    ]

    def send(*slots):
        for slot in slots:
            xcopy(slot, *sends[slot]).start()

    def arrive(owner, row0, count, part):
        xcopy(0, owner, row0, count, part, CN).wait_recv()

    def wcopy(slot, shard, row0, count, sem, target):
        ref = wo_buf.at[pl.ds(shard * wrows + row0, count)]
        return pltpu.make_async_remote_copy(src_ref=ref, dst_ref=ref, send_sem=ws.at[slot], recv_sem=wr.at[sem], device_id=dev(*target), device_id_type=MESH)

    def flag_copy(j):
        peer = (me + j) % ndev
        return pltpu.make_async_remote_copy(src_ref=flag_ref, dst_ref=flags.at[me], send_sem=fs.at[j], recv_sem=fr.at[me], device_id={'cp': peer // 4, 'tp': peer % 4}, device_id_type=MESH)

    x_load.wait()
    send(0, 2, 4, 1, 3, 5)
    wo_load.wait()
    w_own = wcopy(0, tp, 0, wrows, 0, CN)
    w_own.start()

    for kind in range(3):
        w_loads[kind].wait()

        def relayout(n, _):
            r = pl.ds(pl.multiple_of(n * 256, 256), 256)
            for h in range(heads):
                c = kind * width + h * head_dim
                wqkv_ref[r, c:c + head_dim] = w_pair[r, h, :]
            return 0

        lax.fori_loop(0, d_model // 256, relayout, 0)
        if kind < 2:
            w_loads[kind + 1].start()

    def tables():
        toks = ids_ref.shape[1]
        f32, bf16 = jnp.float32, jnp.bfloat16
        cap = 4 * toks // experts
        mean = cap // 2
        per_dev = experts // ndev
        chips = ndev // 2
        crow = 2 * mean
        base = per_dev // 2 * ndev * crow
        before = (lax.broadcasted_iota(jnp.int32, (toks, toks), 0) < lax.broadcasted_iota(jnp.int32, (toks, toks), 1)).astype(f32).astype(bf16)

        def ranks(keys, keep, size):
            out, seen = [], jnp.zeros((size, 1), f32)
            for key, ok in zip(keys, keep):
                hot = jnp.where((lax.broadcasted_iota(jnp.int32, (size, toks), 0) == key) & ok, 1.0, 0.0)
                prior = jnp.dot(hot.astype(bf16), before, preferred_element_type=f32) + seen
                out.append(jnp.sum(hot * prior, axis=0, keepdims=True).astype(jnp.int32))
                seen = seen + jnp.sum(hot, axis=1, keepdims=True)
            return out, seen

        ids = [ids_ref[c:c + 1, :] for c in range(2)]
        pos, _ = ranks(ids, [i >= 0 for i in ids], experts)
        over = [p >= mean for p in pos]
        dest = [i // per_dev for i in ids]
        local = [i - d * per_dev for i, d in zip(ids, dest)]
        spot, seen = ranks([d // 2 for d in dest], over, 8)
        flag_ref[...] = jnp.broadcast_to(jnp.max(seen, axis=0, keepdims=True), flag_ref.shape)
        rows, full, codes = [], [], []
        for p, v, d, l, q in zip(pos, over, dest, local, spot):
            pair = l // 2 * ndev + d
            rows.append(jnp.where(v, base + d // 2 * crow + q, pair * crow + l % 2 * mean + p))
            full.append(pair * 2 * cap + l % 2 * cap + p)
            codes.append(jnp.where(v, 1 + (d % 2 * per_dev + l) * mean + p - mean, 0))
        for n, row in enumerate(rows + full):
            lane_ref[n:n + 1, :] = row
        tall[...] = jnp.zeros_like(tall)
        for n, row in enumerate(rows + full + [gates_ref[c:c + 1, :] for c in range(2)]):
            tall[n:n + 1, :] = row.astype(f32)
        col_ref[...] = tall[...].T
        lane = lax.broadcasted_iota(jnp.int32, (toks, ndev * crow), 1)
        for chip in range(chips):
            total = jnp.zeros(meta_ref.shape[1:], f32)
            for c in range(2):
                place = col_ref[:, c:c + 1].astype(jnp.int32) - (base + chip * crow) + me * crow
                hot = ((place == lane) & (lane // crow == me)).astype(f32).astype(bf16)
                code = jnp.broadcast_to(codes[c].astype(f32), (8, toks)).astype(bf16)
                total += jnp.dot(code, hot, preferred_element_type=f32)
            meta_ref[chip] = total

    def project(owner, half):
        r, t = owner // 4, owner % 4
        seg = r + half * (3 - 2 * r)
        x = xbuf[owner, pl.ds(pl.multiple_of(half * half_rows, half_rows), half_rows), :]
        out = jnp.dot(x, wqkv_ref[...], preferred_element_type=jnp.float32).astype(jnp.bfloat16)
        qkv[pl.ds(pl.multiple_of((seg * 4 + t) * half_rows, half_rows), half_rows), :] = out

    def near(s, _):
        @pl.when(s == 2)
        def _():
            arrive(CN, 0, half_rows, 0)

        @pl.when(s == 3)
        def _():
            arrive(CN, half_rows, half_rows, 2)

        project(idx(0, 0, s // 2), s % 2)
        return 0

    lax.fori_loop(0, 4, near, 0)
    tables()
    for j in range(1, ndev):
        flag_copy(j).start()

    w_x = [(1 + k, tp, cp * whalf + k * wpart, wpart, 1 + k, XN) for k in range(parts)]

    def gather(p):
        base = p * half_rows

        @pl.when(p == 0)
        def _():
            arrive(XN, 0, H, 0)
            arrive(YN, 0, H, 0)
            send(12, 10, 16, 17, 6, 8)

        def mid(u, _):
            @pl.when(u == 2)
            def _():
                arrive(XC, base, H, 2 * p)

            @pl.when(u == 3)
            def _():
                arrive(YC, base, H, 2 * p)

            project(idx(1 - u % 2, u % 2, u // 2), p)
            return 0

        lax.fori_loop(0, 4, mid, 0)

        @pl.when(p == 0)
        def _():
            arrive(XN, H, Q, 2)
            arrive(YN, H, Q, 2)
            send(11)

        arrive(DG, base, Q, 2 * p)
        arrive(DG, base + Q, Q, 2 * p + 1)

        @pl.when(p == 0)
        def _():
            send(14)

        @pl.when(p == 1)
        def _():
            send(15)

        def far(u, _):
            @pl.when(u == 1)
            def _():
                arrive(DC, base, H, 2 * p)

            project(idx(1, 1, u), p)
            return 0

        lax.fori_loop(0, 2, far, 0)

    def late():
        arrive(XN, H + Q, Q, 3)
        arrive(YN, H + Q, Q, 3)
        send(13, 7, 9)
        for spec in w_x:
            wcopy(*spec).start()

    coef = (head_dim ** -0.5) * math.log2(math.e)
    my_col = (4 * tp + 2 * cp) * head_dim

    def o_place(b):
        seg, t = b // 4, b % 4
        half = seg // 2
        return seg + half * (3 - 2 * seg), t, half

    def o_remote(b):
        r, t, half = o_place(b)
        return pltpu.make_async_remote_copy(
            src_ref=o_loc.at[pl.ds(pl.multiple_of(b * half_rows, half_rows), half_rows)],
            dst_ref=o_cat.at[pl.ds(pl.multiple_of(half * half_rows, half_rows), half_rows), pl.ds(pl.multiple_of(my_col, width), width)],
            send_sem=os_sem.at[b], recv_sem=or_sem.at[me, half], device_id={'cp': r, 'tp': t}, device_id_type=MESH)

    def o_local(b):
        _, _, half = o_place(b)
        return pltpu.make_async_copy(
            o_loc.at[pl.ds(pl.multiple_of(b * half_rows, half_rows), half_rows)],
            o_cat.at[pl.ds(pl.multiple_of(half * half_rows, half_rows), half_rows), pl.ds(pl.multiple_of(my_col, width), width)],
            os_sem.at[b])

    def o_send(i):
        for part in range(QB // half_rows):
            b = i * (QB // half_rows) + part
            r, t, _ = o_place(b)

            @pl.when(r * 4 + t != me)
            def _():
                o_remote(b).start()

            @pl.when(r * 4 + t == me)
            def _():
                o_local(b).start()

    peer_t = tp_of(1, 0)
    peer_c = tp_of(1, 1)

    def w_near(k, slot, shard, target):
        return wcopy(slot * parts + 1 + k, shard, cp * whalf + k * wpart, wpart, slot * parts + 1 + k, target)

    def w_far(k, slot, shard, target):
        return wcopy(slot * parts + 1 + k, shard, (1 - cp) * whalf + k * wpart, wpart, slot * parts + 1 + k, target)

    def w_pass(k):
        w_near(k, 0, peer_t, CN).wait_recv()
        w_near(k, 1, peer_t, YN).start()
        w_near(k, 2, peer_t, CN).start()

    def w_last(k):
        w_far(k, 1, peer_t, CN).wait_recv()
        w_far(k, 3, peer_t, CN).start()

    def at(i, step, *work):
        @pl.when(i == step)
        def _():
            for job, k in work:
                job(k)

    blocks = seq // QB

    def block_of(step):
        p, n = step // 4, step % 4
        y, x = (cp + 1 - n % 2) % 2, (xx + 1 - n // 2) % 2
        return 2 * (y + p * (3 - 2 * y)) + x

    def q_step(step, _):
        i = block_of(step)

        @pl.when(step == blocks // 2 - 1)
        def _():
            late()
            for early in range(blocks // 2 - 1):
                o_send(block_of(early))

        at(step, 5, (w_pass, 1))
        at(step, 6, (w_pass, 3))
        at(step, 7, (w_last, 1))

        q_rows = pl.ds(pl.multiple_of(i * QB, QB), QB)

        def cols(kind, h):
            return slice(kind * width + h * head_dim, kind * width + (h + 1) * head_dim)

        def scores(h, j):
            k = qkv[pl.ds(pl.multiple_of(j * QB, QB), QB), cols(1, h)]
            return lax.dot_general(qkv[q_rows, cols(0, h)], k, (((1,), (1,)), ((), ())), preferred_element_type=jnp.float32)

        def pass1(j, ms):
            out = []
            for h in range(heads):
                s = scores(h, j)
                s_ref[h, :, pl.ds(pl.multiple_of(j * QB, QB), QB)] = s
                out.append(jnp.maximum(ms[h], lane_fold(s, jnp.maximum)))
            return tuple(out)

        ms = lax.fori_loop(0, i, pass1, tuple(jnp.full((QB, 128), -jnp.inf, jnp.float32) for _ in range(heads)))
        keep = lax.broadcasted_iota(jnp.int32, (QB, QB), 1) <= lax.broadcasted_iota(jnp.int32, (QB, QB), 0)
        tops = []
        for h in range(heads):
            s = jnp.where(keep, scores(h, i), -jnp.inf)
            s_ref[h, :, pl.ds(pl.multiple_of(i * QB, QB), QB)] = s
            tops.append(jnp.max(jnp.maximum(ms[h], lane_fold(s, jnp.maximum)), axis=1, keepdims=True))
        acc_ref[...] = jnp.zeros_like(acc_ref)
        at(step, 4, (w_pass, 0))
        at(step, 5, (w_pass, 2))
        at(step, 6, (w_last, 0))
        at(step, 7, (w_last, 2))


        def pass2(j, ls):
            out = []
            for h in range(heads):
                e = jnp.exp2((s_ref[h, :, pl.ds(pl.multiple_of(j * QB, QB), QB)] - tops[h]) * coef)
                v = qkv[pl.ds(pl.multiple_of(j * QB, QB), QB), cols(2, h)]
                acc_ref[h] += jnp.dot(e.astype(jnp.bfloat16), v, preferred_element_type=jnp.float32)
                out.append(ls[h] + lane_fold(e, jnp.add))
            return tuple(out)

        ls = lax.fori_loop(0, i + 1, pass2, tuple(jnp.zeros((QB, 128), jnp.float32) for _ in range(heads)))
        for h in range(heads):
            total = jnp.sum(ls[h], axis=1, keepdims=True)
            o_loc[q_rows, h * head_dim:(h + 1) * head_dim] = (acc_ref[h] / total).astype(jnp.bfloat16)

        @pl.when(step >= blocks // 2 - 1)
        def _():
            o_send(i)

        return 0

    def phase(p, _):
        gather(p)
        lax.fori_loop(p * (blocks // 2), (p + 1) * (blocks // 2), q_step, 0)
        return 0

    lax.fori_loop(0, 2, phase, 0)

    w_last(3)
    wcopy(0, tp_of(0, 1), 0, wrows, 0, CN).wait_recv()
    for k in range(parts):
        w_near(k, 2, peer_c, CN).wait_recv()
        w_far(k, 3, peer_c, CN).wait_recv()

    def o_arrived(half):
        for k in range(1, ndev):
            src = (me + k) % ndev
            col = (4 * (src % 4) + 2 * (src // 4)) * head_dim
            ref = o_cat.at[pl.ds(half * half_rows, half_rows), pl.ds(pl.multiple_of(col, width), width)]
            pltpu.make_async_remote_copy(src_ref=ref, dst_ref=ref, send_sem=os_sem.at[0], recv_sem=or_sem.at[src, half], device_id=dev(0, 0, 1), device_id_type=MESH).wait_recv()

    my_seg = [cp, 3 - cp]
    tile = 512
    for half in range(2):
        o_arrived(half)
        o_local(my_seg[half] * 4 + tp).wait()
        r = slice(half * half_rows, (half + 1) * half_rows)

        def out_step(n, _):
            c = pl.ds(pl.multiple_of(n * tile, tile), tile)
            a = jnp.dot(o_cat[r, :], wo_buf[:, c], preferred_element_type=jnp.float32)
            h_ref[r, c] = (xbuf[me, r, c].astype(jnp.float32) + a).astype(jnp.bfloat16)
            return 0

        lax.fori_loop(0, d_model // tile, out_step, 0)
        pltpu.make_async_copy(h_ref.at[r], h_hbm.at[r], h_sem.at[half]).start()

    def drain(b, _):
        r, t, _half = o_place(b)

        @pl.when(r * 4 + t != me)
        def _():
            o_remote(b).wait_send()

        return 0

    lax.fori_loop(0, seq // half_rows, drain, 0)

    most = flag_ref[...]
    for j in range(1, ndev):
        peer = (me + j) % ndev
        pltpu.make_async_remote_copy(src_ref=flag_ref, dst_ref=flags.at[peer], send_sem=fs.at[j], recv_sem=fr.at[peer], device_id=dev(0, 0, 1), device_id_type=MESH).wait_recv()
        most = jnp.maximum(most, flags[peer])
        flag_copy(j).wait_send()
    any_ref[0, 0] = jnp.max(most).astype(jnp.int32)

    for slot in range(len(sends)):
        xcopy(slot, *sends[slot]).wait_send()
    w_own.wait_send()
    for spec in w_x:
        wcopy(*spec).wait_send()
    for k in range(parts):
        w_near(k, 1, peer_t, YN).wait_send()
        w_near(k, 2, peer_t, CN).wait_send()
        w_far(k, 3, peer_t, CN).wait_send()
    for half in range(2):
        r = slice(half * half_rows, (half + 1) * half_rows)
        pltpu.make_async_copy(h_ref.at[r], h_hbm.at[r], h_sem.at[half]).wait()


def attention_block(x_blk, w_q, w_k, w_v, w_o, ids, gates, heads, head_dim, ndev, experts):
    rows, d_model = x_blk.shape
    seq = rows * ndev
    width = heads * head_dim
    vm = pl.BlockSpec(memory_space=pltpu.VMEM)
    hbm = pl.BlockSpec(memory_space=pl.ANY)
    bf16, f32 = jnp.bfloat16, jnp.float32
    dma = pltpu.SemaphoreType.DMA
    return pl.pallas_call(
        functools.partial(attn_block, heads=heads, head_dim=head_dim, experts=experts),
        name='attn_block',
        out_shape=(jax.ShapeDtypeStruct((rows, d_model), bf16), jax.ShapeDtypeStruct((1, 1), jnp.int32), jax.ShapeDtypeStruct((8, rows), jnp.int32), jax.ShapeDtypeStruct((rows, 128), f32), jax.ShapeDtypeStruct((ndev // 2, 8, rows * ndev * 4 // experts), f32)),
        in_specs=[hbm] * 5 + [vm] * 2,
        out_specs=(hbm, pl.BlockSpec(memory_space=pltpu.SMEM), vm, vm, vm),
        scratch_shapes=[
            pltpu.VMEM((ndev, rows, d_model), bf16), pltpu.VMEM((d_model, 3 * width), bf16), pltpu.VMEM((d_model, heads, head_dim), bf16), pltpu.VMEM((seq, 3 * width), bf16),
            pltpu.VMEM((heads, QB, seq), f32), pltpu.VMEM((heads, QB, head_dim), f32),
            pltpu.VMEM((seq, width), bf16), pltpu.VMEM((rows, ndev * width), bf16),
            pltpu.VMEM((ndev * width, d_model), bf16),
            pltpu.VMEM((8, 128), f32), pltpu.VMEM((ndev, 8, 128), f32), pltpu.VMEM((128, rows), f32), pltpu.VMEM((rows, d_model), bf16), dma((2,)),
            dma((3,)), dma((18,)), dma((ndev, 4)), dma((17,)), dma((17,)), dma((16,)), dma((ndev, 2)), dma((ndev,)), dma((ndev,)),
        ],
        compiler_params=pltpu.CompilerParams(collective_id=0, has_side_effects=True, vmem_limit_bytes=63 * MIB),
        cost_estimate=pl.CostEstimate(flops=2 * seq * d_model * width * 3 + 4 * seq * seq * width, bytes_accessed=16 * MIB, transcendentals=0),
    )(x_blk, w_q, w_k, w_v, w_o, ids, gates)


def moe_block(h_hbm, rl_ref, col_ref, meta_ref, wg_hbm, wu_hbm, wd_hbm, y_hbm, h_ref, y_ref, io_sem, send, recv, zbuf, ret,
              meta_in, sp_send, sp_recv, sp_z, sp_ret, pool_in, xs, zacc, acc, wg, wu, wd, ds, dr, rs, rr, ms, mr, sp_sem, sp_dr, pool_s, pool_r, sp_rs, sp_rr, wsem, *, main, spill):
    cp, tp = lax.axis_index('cp'), lax.axis_index('tp')
    xx, cc = tp // 2, tp % 2
    me = cp * 4 + tp
    chunks, ndev, crow, d_model = send.shape
    rows_all = ndev * crow
    toks = h_ref.shape[0]
    experts = wg_hbm.shape[0]
    slots, _, ff_half = wg.shape
    sp_rows = sp_send.shape[1]
    sp_base = chunks * rows_all
    c0 = 0 if spill else 2
    steps = 2 * experts
    tile = 512
    f32, bf16 = jnp.float32, jnp.bfloat16

    def weights(n):
        e, f, slot = n // 2, n % 2, n % slots
        fcols = pl.ds(pl.multiple_of(f * ff_half, ff_half), ff_half)
        return (pltpu.make_async_copy(wg_hbm.at[e, :, fcols], wg.at[slot], wsem.at[slot, 0]),
                pltpu.make_async_copy(wu_hbm.at[e, :, fcols], wu.at[slot], wsem.at[slot, 1]),
                pltpu.make_async_copy(wd_hbm.at[e, fcols, :], wd.at[slot], wsem.at[slot, 2]))

    def fetch(n):
        for copy in weights(n):
            copy.start()

    h_load = pltpu.make_async_copy(h_hbm, h_ref, io_sem.at[0])
    h_load.start()
    for n in range(slots - 1):
        fetch(n)

    def peer_of(j):
        return (me + j) % ndev

    def dev(p):
        return {'cp': p // 4, 'tp': p % 4}

    barrier = pltpu.get_barrier_semaphore()
    for j in range(1, ndev):
        pl.semaphore_signal(barrier, inc=1, device_id=dev(peer_of(j)), device_id_type=MESH)
    pl.semaphore_wait(barrier, ndev - 1)

    AWAY = [(1, 0), (0, 1), (1, 1)]

    def chip(dx, dy):
        return ((cp + dy) % 2) * 2 + (xx + dx) % 2

    def idx(dx, dy, dc):
        return chip(dx, dy) * 2 + (cc + dc) % 2

    def sp_copy(src, dst, ssem, rsem, target):
        return pltpu.make_async_remote_copy(src_ref=src, dst_ref=dst, send_sem=ssem, recv_sem=rsem, device_id=dev(idx(*target)), device_id_type=MESH)

    def sp_out(n):
        if n < 3:
            return sp_copy(sp_send.at[chip(*AWAY[n])], sp_recv.at[me], sp_sem.at[n], sp_dr.at[me], AWAY[n] + (0,))
        return sp_copy(sp_send.at[chip(0, 0)], sp_recv.at[me], sp_sem.at[3], sp_dr.at[me], (0, 0, 1))

    def sp_pass(n):
        ref = sp_recv.at[idx(*AWAY[n], 0)]
        return sp_copy(ref, ref, sp_sem.at[4 + n], sp_dr.at[idx(*AWAY[n], 0)], (0, 0, 1))

    def sp_arrived(source):
        ref = sp_recv.at[idx(*source)]
        sp_copy(ref, ref, sp_sem.at[0], sp_dr.at[idx(*source)], (0, 0, 1)).wait_recv()

    def sp_pool(n):
        side = ([(0, 0)] + AWAY)[n]
        return sp_copy(sp_z.at[idx(*side, 1)], pool_in.at[n], pool_s.at[n], pool_r.at[n], (0, 0, 1))

    def sp_back(n):
        side = AWAY[n]
        return sp_copy(sp_z.at[idx(*side, 0)], sp_ret.at[chip(0, 0)], sp_rs.at[n], sp_rr.at[chip(0, 0)], side + (0,))

    def meta_copy(j):
        return pltpu.make_async_remote_copy(src_ref=meta_ref.at[peer_of(j) // 2], dst_ref=meta_in.at[me], send_sem=ms.at[j], recv_sem=mr.at[me], device_id=dev(peer_of(j)), device_id_type=MESH)

    if spill:
        for j in range(1, ndev):
            meta_copy(j).start()

    def exchange(src, dst, ssem, rsem, k):
        def copy(j):
            return pltpu.make_async_remote_copy(src_ref=src.at[k, peer_of(j)], dst_ref=dst.at[k, me], send_sem=ssem.at[k, j], recv_sem=rsem.at[k, me], device_id=dev(peer_of(j)), device_id_type=MESH)

        local = pltpu.make_async_copy(src.at[k, me], dst.at[k, me], ssem.at[k, 0])
        return copy, local

    def begin(src, dst, ssem, rsem, k):
        copy, local = exchange(src, dst, ssem, rsem, k)
        local.start()
        for j in range(1, ndev):
            copy(j).start()

    def arrived(src, dst, ssem, rsem, k):
        for j in range(1, ndev):
            pltpu.make_async_remote_copy(src_ref=src.at[k, peer_of(j)], dst_ref=dst.at[k, peer_of(j)], send_sem=ssem.at[k, j], recv_sem=rsem.at[k, peer_of(j)], device_id=dev(peer_of(j)), device_id_type=MESH).wait_recv()
        exchange(src, dst, ssem, rsem, k)[1].wait()

    def left(src, dst, ssem, rsem, k):
        copy, _ = exchange(src, dst, ssem, rsem, k)
        for j in range(1, ndev):
            copy(j).wait_send()

    out_way = (send, recv, ds, dr)
    back_way = (zbuf, ret, rs, rr)

    def sp_own():
        return pltpu.make_async_copy(sp_send.at[chip(0, 0)], sp_recv.at[me], sp_sem.at[7])

    h_load.wait()
    if spill:
        ids = lax.broadcasted_iota(jnp.int32, (4 * sp_rows, toks), 0) + sp_base
        pick = ((ids == rl_ref[c0:c0 + 1, :]) | (ids == rl_ref[c0 + 1:c0 + 2, :])).astype(f32).astype(bf16)

        def sp_cols(n, _):
            c = pl.ds(pl.multiple_of(n * tile, tile), tile)
            sp_send[:, :, c] = jnp.dot(pick, h_ref[:, c], preferred_element_type=f32).astype(bf16).reshape(4, sp_rows, tile)
            return 0

        lax.fori_loop(0, d_model // tile, sp_cols, 0)
        for n in range(4):
            sp_out(n).start()
        sp_own().start()

    def pack(k, _):
        ids = lax.broadcasted_iota(jnp.int32, (rows_all, toks), 0) + k * rows_all
        pick = ((ids == rl_ref[c0:c0 + 1, :]) | (ids == rl_ref[c0 + 1:c0 + 2, :])).astype(f32).astype(bf16)

        def cols(n, _):
            c = pl.ds(pl.multiple_of(n * tile, tile), tile)
            rows = jnp.dot(pick, h_ref[:, c], preferred_element_type=f32).astype(bf16)
            send[k, :, :, c] = rows.reshape(ndev, crow, tile)
            return 0

        lax.fori_loop(0, d_model // tile, cols, 0)

        @pl.when(k > 0)
        def _():
            begin(*out_way, k - 1)

        return 0

    lax.fori_loop(0, chunks, pack, 0)
    begin(*out_way, chunks - 1)

    if spill:
        for j in range(1, ndev):
            p = peer_of(j)
            pltpu.make_async_remote_copy(src_ref=meta_in.at[p], dst_ref=meta_in.at[p], send_sem=ms.at[j], recv_sem=mr.at[p], device_id=dev(p), device_id_type=MESH).wait_recv()
        for n in range(3):
            sp_arrived(AWAY[n] + (0,))
            sp_pass(n).start()
        sp_own().wait()
        sp_arrived((0, 0, 1))
        for n in range(3):
            sp_arrived(AWAY[n] + (1,))
        total = meta_ref[me // 2]
        for j in range(1, ndev):
            total = total + meta_in[peer_of(j)]
        code = total[0:1, :].astype(jnp.int32) - 1 - cc * (experts * main)
        lane = lax.broadcasted_iota(jnp.int32, code.shape, 1)
        place = (lane // sp_rows) * main + (code & (main - 1))
        owner = code // main
        sp_z[...] = jnp.zeros_like(sp_z)
    body = ndev * main

    def expert(e, _):
        k = e // 2
        part = pl.ds(pl.multiple_of((e % 2) * main, main), main)

        @pl.when(e % 2 == 0)
        def _():
            arrived(*out_way, k)

        xs[0:body, :] = recv[k, :, part, :].reshape(body, d_model)
        if spill:
            slot_id = lax.broadcasted_iota(jnp.int32, (body, ndev * sp_rows), 0)
            pick = ((slot_id == place) & (owner == e)).astype(f32).astype(bf16)

            def gather(n, _):
                c = pl.ds(pl.multiple_of(n * tile, tile), tile)
                xs[body:2 * body, c] = jnp.dot(pick, sp_recv[:, :, c].reshape(ndev * sp_rows, tile), preferred_element_type=f32).astype(bf16)
                return 0

            lax.fori_loop(0, d_model // tile, gather, 0)

        for f in range(2):
            n = 2 * e + f
            slot = n % slots
            for copy in weights(n):
                copy.wait()

            @pl.when(n + slots - 1 < steps)
            def _():
                fetch(n + slots - 1)

            x = xs[...]
            gate = jnp.dot(x, wg[slot], preferred_element_type=f32)
            up = jnp.dot(x, wu[slot], preferred_element_type=f32)
            u = (gate * jax.nn.sigmoid(gate) * up).astype(bf16)

            def down(n, _):
                c = pl.ds(pl.multiple_of(n * tile, tile), tile)
                z = jnp.dot(u, wd[slot, :, c], preferred_element_type=f32)
                if f == 0:
                    zacc[:, c] = z
                else:
                    z = (zacc[:, c] + z).astype(bf16)
                    zbuf[k, :, part, c] = z[0:body].reshape(ndev, main, tile)
                    if spill:
                        spread = lax.dot_general(pick, z[body:], (((0,), (0,)), ((), ())), preferred_element_type=f32)
                        sp_z[:, :, c] = sp_z[:, :, c] + spread.astype(bf16).reshape(ndev, sp_rows, tile)
                return 0

            lax.fori_loop(0, d_model // tile, down, 0)
            if f == 0:
                @pl.when((e % 2 == 0) & (e > 0))
                def _():
                    begin(*back_way, k - 1)

        return 0

    lax.fori_loop(0, experts, expert, 0)
    if spill:
        for n in range(4):
            sp_pool(n).start()
    begin(*back_way, chunks - 1)
    acc[...] = jnp.zeros_like(acc)

    def sp_home():
        return pltpu.make_async_copy(sp_z.at[me], sp_ret.at[chip(0, 0)], sp_rs.at[3])

    if spill:
        for n in range(4):
            sp_pool(n).wait_recv()
            at = idx(*([(0, 0)] + AWAY)[n], 0)
            sp_z[at] = sp_z[at] + pool_in[n]
        for n in range(3):
            sp_back(n).start()
        sp_home().start()

    row0, row1 = (col_ref[:, c:c + 1].astype(jnp.int32) for c in (c0, c0 + 1))

    def chosen(ids, z):
        z0 = jnp.dot((ids == row0).astype(f32).astype(bf16), z, preferred_element_type=f32)
        z1 = jnp.dot((ids == row1).astype(f32).astype(bf16), z, preferred_element_type=f32)
        return col_ref[:, 4:5] * z0 + col_ref[:, 5:6] * z1

    def combine(k, _):
        arrived(*back_way, k)
        ids = lax.broadcasted_iota(jnp.int32, (toks, rows_all), 1) + k * rows_all

        def cols(n, _):
            c = pl.ds(pl.multiple_of(n * tile, tile), tile)
            acc[:, c] += chosen(ids, ret[k, :, :, c].reshape(rows_all, tile))
            return 0

        lax.fori_loop(0, d_model // tile, cols, 0)
        return 0

    lax.fori_loop(0, chunks, combine, 0)
    if spill:
        sp_home().wait()
        for n in range(3):
            ref = sp_ret.at[chip(*AWAY[n])]
            sp_copy(ref, ref, sp_rs.at[n], sp_rr.at[chip(*AWAY[n])], (0, 0, 1)).wait_recv()

    def y_copy(n):
        c = pl.ds(pl.multiple_of(n * tile, tile), tile)
        return pltpu.make_async_copy(y_ref.at[:, c], y_hbm.at[:, c], io_sem.at[n])

    def finish(n, _):
        c = pl.ds(pl.multiple_of(n * tile, tile), tile)
        moe_out = acc[:, c]
        if spill:
            ids = lax.broadcasted_iota(jnp.int32, (toks, 4 * sp_rows), 1) + sp_base
            moe_out += chosen(ids, sp_ret[:, :, c].reshape(4 * sp_rows, tile))
        y_ref[:, c] = (h_ref[:, c].astype(f32) + moe_out).astype(bf16)
        y_copy(n).start()
        return 0

    lax.fori_loop(0, d_model // tile, finish, 0)

    def drain(k, _):
        left(*out_way, k)
        left(*back_way, k)
        return 0

    lax.fori_loop(0, chunks, drain, 0)
    for n in range(d_model // tile):
        y_copy(n).wait()
    if spill:
        for j in range(1, ndev):
            meta_copy(j).wait_send()
        for n in range(4):
            sp_out(n).wait_send()
            sp_pool(n).wait_send()
        for n in range(3):
            sp_pass(n).wait_send()
            sp_back(n).wait_send()


def moe(hidden, lane, col, meta, w_gate, w_up, w_down, ndev, main, spill):
    toks, d_model = hidden.shape
    experts, _, ff = w_gate.shape
    crow = 2 * main
    chunks = experts // 2
    sp_rows = 2 * main if spill else 16
    slots = 3 if spill else 2
    vm = pl.BlockSpec(memory_space=pltpu.VMEM)
    hbm = pl.BlockSpec(memory_space=pl.ANY)
    bf16, f32 = jnp.bfloat16, jnp.float32
    dma = pltpu.SemaphoreType.DMA
    buf = pltpu.VMEM((chunks, ndev, crow, d_model), bf16)
    tile_rows = 2 * ndev * main if spill else ndev * main
    return pl.pallas_call(
        functools.partial(moe_block, main=main, spill=spill),
        name='moe_spill' if spill else 'moe_full',
        out_shape=jax.ShapeDtypeStruct((toks, d_model), bf16),
        in_specs=[hbm] + [vm] * 3 + [hbm] * 3,
        out_specs=hbm,
        scratch_shapes=[
            pltpu.VMEM((toks, d_model), bf16), pltpu.VMEM((toks, d_model), bf16), dma((d_model // 512,)),
            buf, buf, buf, buf, pltpu.VMEM((ndev,) + meta.shape[1:], f32),
            pltpu.VMEM((4, sp_rows, d_model), bf16), pltpu.VMEM((ndev, sp_rows, d_model), bf16), pltpu.VMEM((ndev, sp_rows, d_model), bf16),
            pltpu.VMEM((4, sp_rows, d_model), bf16), pltpu.VMEM((4, sp_rows, d_model), bf16),
            pltpu.VMEM((tile_rows, d_model), bf16), pltpu.VMEM((tile_rows, d_model), f32), pltpu.VMEM((toks, d_model), f32),
            pltpu.VMEM((slots, d_model, ff // 2), bf16), pltpu.VMEM((slots, d_model, ff // 2), bf16), pltpu.VMEM((slots, ff // 2, d_model), bf16),
            dma((chunks, ndev)), dma((chunks, ndev)), dma((chunks, ndev)), dma((chunks, ndev)), dma((ndev,)), dma((ndev,)),
            dma((8,)), dma((ndev,)), dma((4,)), dma((4,)), dma((4,)), dma((4,)), dma((slots, 3)),
        ],
        compiler_params=pltpu.CompilerParams(collective_id=1 if spill else 2, has_side_effects=True, vmem_limit_bytes=63 * MIB),
        cost_estimate=pl.CostEstimate(flops=6 * tile_rows * experts * d_model * ff, bytes_accessed=6 * experts * d_model * ff, transcendentals=0),
    )(hidden, lane, col, meta, w_gate, w_up, w_down)


def solution(mesh):
    cp_size = mesh.shape['cp']
    tp_size = mesh.shape['tp']
    num_devs = cp_size * tp_size
    row_spec = P(('data', 'cp', 'tp'), None)
    head_spec = P(None, 'tp', None)
    wo_spec = P('tp', None, None)
    expert_spec = P(('cp', 'tp'), None, None)

    def device_fn(x_blk, w_q, w_k, w_v, w_o, idx_blk, gate_blk, w_gate, w_up, w_down):
        tok_dev, d_model = x_blk.shape
        heads_tp, head_dim = w_q.shape[1], w_q.shape[2]
        heads = heads_tp // cp_size
        exp_local = w_gate.shape[0]
        num_exp = exp_local * num_devs
        capacity = 4 * tok_dev // num_exp
        mean = capacity // 2
        crow = 2 * mean
        hidden, most, lane, col, meta = attention_block(x_blk, w_q, w_k, w_v, w_o.reshape(-1, d_model), idx_blk.T, gate_blk.T, heads, head_dim, num_devs, num_exp)

        def run(main, spill):
            return lambda h: moe(h, lane, col, meta, w_gate, w_up, w_down, num_devs, main, spill)

        return lax.cond(most[0, 0] <= crow, run(mean, True), run(capacity, False), hidden)

    return jax.shard_map(device_fn, mesh=mesh, in_specs=(row_spec, head_spec, head_spec, head_spec, wo_spec, row_spec, row_spec, expert_spec, expert_spec, expert_spec), out_specs=row_spec, check_vma=False)
```

```python
import functools
import math

import jax
import jax.numpy as jnp
from jax import lax
from jax.experimental import pallas as pl
from jax.experimental.pallas import tpu as pltpu
from jax.sharding import PartitionSpec as P

MESH = pl.DeviceIdType.MESH
MIB = 1024 * 1024
QB = 512


def lane_fold(s, op):
    out = s[:, :128]
    for g in range(1, s.shape[1] // 128):
        out = op(out, s[:, g * 128:(g + 1) * 128])
    return out


def attn_block(x_hbm, wq_hbm, wk_hbm, wv_hbm, wo_hbm, ids_ref, gates_ref, h_hbm, any_ref, lane_ref, col_ref, meta_ref, xbuf, wqkv_ref, w_pair, qkv, s_ref, acc_ref, o_loc, o_cat, wo_buf,
               flag_ref, flags, tall, h_ref, h_sem, loc_sem, xs, xr, ws, wr, os_sem, or_sem, fs, fr, *, heads, head_dim, experts):
    cp, tp = lax.axis_index('cp'), lax.axis_index('tp')
    xx, cc = tp // 2, tp % 2
    me = cp * 4 + tp
    ndev, rows, d_model = xbuf.shape
    half_rows = rows // 2
    quarter = half_rows // 2
    width = heads * head_dim
    seq = ndev * rows
    wrows = wo_hbm.shape[0]
    parts = 4
    whalf, wpart = wrows // 2, wrows // 2 // parts

    def tp_of(dx, dc):
        return ((xx + dx) % 2) * 2 + (cc + dc) % 2

    def idx(dx, dy, dc):
        return ((cp + dy) % 2) * 4 + tp_of(dx, dc)

    def dev(dx, dy, dc):
        return {'cp': (cp + dy) % 2, 'tp': tp_of(dx, dc)}

    x_load = pltpu.make_async_copy(x_hbm, xbuf.at[me], loc_sem.at[0])
    wo_load = pltpu.make_async_copy(wo_hbm, wo_buf.at[pl.ds(tp * wrows, wrows)], loc_sem.at[1])
    x_load.start()
    wo_load.start()
    w_loads = [pltpu.make_async_copy(w.at[:, pl.ds(heads * cp, heads), :], w_pair, loc_sem.at[2]) for w in (wq_hbm, wk_hbm, wv_hbm)]
    w_loads[0].start()

    barrier = pltpu.get_barrier_semaphore()
    for k in range(1, ndev):
        peer = (me + k) % ndev
        pl.semaphore_signal(barrier, inc=1, device_id={'cp': peer // 4, 'tp': peer % 4}, device_id_type=MESH)
    pl.semaphore_wait(barrier, ndev - 1)

    def xcopy(slot, owner, row0, count, part, target):
        ref = xbuf.at[idx(*owner), pl.ds(row0 if isinstance(row0, int) else pl.multiple_of(row0, quarter), count)]
        return pltpu.make_async_remote_copy(src_ref=ref, dst_ref=ref, send_sem=xs.at[slot], recv_sem=xr.at[idx(*owner), part], device_id=dev(*target), device_id_type=MESH)

    XN, YN, CN, DG, OWN = (1, 0, 0), (0, 1, 0), (0, 0, 1), (1, 1, 0), (0, 0, 0)
    XC, YC, DC = (1, 0, 1), (0, 1, 1), (1, 1, 1)
    H, Q = half_rows, quarter
    sends = [
        (OWN, 0, H, 0, XN), (OWN, H, Q, 2, XN), (OWN, 0, H, 0, YN), (OWN, H, Q, 2, YN), (OWN, 0, H, 0, CN), (OWN, H, H, 2, CN),
        (XN, 0, H, 0, CN), (XN, H, H, 2, CN), (YN, 0, H, 0, CN), (YN, H, H, 2, CN),
        (YN, 0, Q, 0, XN), (YN, H, Q, 2, XN), (XN, Q, Q, 1, YN), (XN, H + Q, Q, 3, YN),
        (DG, 0, H, 0, CN), (DG, H, H, 2, CN), (OWN, H + Q, Q, 3, XN), (OWN, H + Q, Q, 3, YN),
    ]

    def send(*slots):
        for slot in slots:
            xcopy(slot, *sends[slot]).start()

    def arrive(owner, row0, count, part):
        xcopy(0, owner, row0, count, part, CN).wait_recv()

    def wcopy(slot, shard, row0, count, sem, target):
        ref = wo_buf.at[pl.ds(shard * wrows + row0, count)]
        return pltpu.make_async_remote_copy(src_ref=ref, dst_ref=ref, send_sem=ws.at[slot], recv_sem=wr.at[sem], device_id=dev(*target), device_id_type=MESH)

    def flag_copy(j):
        peer = (me + j) % ndev
        return pltpu.make_async_remote_copy(src_ref=flag_ref, dst_ref=flags.at[me], send_sem=fs.at[j], recv_sem=fr.at[me], device_id={'cp': peer // 4, 'tp': peer % 4}, device_id_type=MESH)

    x_load.wait()
    send(0, 2, 4, 1, 3, 5)
    wo_load.wait()
    w_own = wcopy(0, tp, 0, wrows, 0, CN)
    w_own.start()

    for kind in range(3):
        w_loads[kind].wait()

        def relayout(n, _):
            r = pl.ds(pl.multiple_of(n * 256, 256), 256)
            for h in range(heads):
                c = kind * width + h * head_dim
                wqkv_ref[r, c:c + head_dim] = w_pair[r, h, :]
            return 0

        lax.fori_loop(0, d_model // 256, relayout, 0)
        if kind < 2:
            w_loads[kind + 1].start()

    def tables():
        toks = ids_ref.shape[1]
        f32, bf16 = jnp.float32, jnp.bfloat16
        cap = 4 * toks // experts
        mean = cap // 2
        per_dev = experts // ndev
        chips = ndev // 2
        crow = 2 * mean
        base = per_dev // 2 * ndev * crow
        before = (lax.broadcasted_iota(jnp.int32, (toks, toks), 0) < lax.broadcasted_iota(jnp.int32, (toks, toks), 1)).astype(f32).astype(bf16)

        def ranks(keys, keep, size):
            out, seen = [], jnp.zeros((size, 1), f32)
            for key, ok in zip(keys, keep):
                hot = jnp.where((lax.broadcasted_iota(jnp.int32, (size, toks), 0) == key) & ok, 1.0, 0.0)
                prior = jnp.dot(hot.astype(bf16), before, preferred_element_type=f32) + seen
                out.append(jnp.sum(hot * prior, axis=0, keepdims=True).astype(jnp.int32))
                seen = seen + jnp.sum(hot, axis=1, keepdims=True)
            return out, seen

        ids = [ids_ref[c:c + 1, :] for c in range(2)]
        pos, _ = ranks(ids, [i >= 0 for i in ids], experts)
        over = [p >= mean for p in pos]
        dest = [i // per_dev for i in ids]
        local = [i - d * per_dev for i, d in zip(ids, dest)]
        spot, seen = ranks([d // 2 for d in dest], over, 8)
        flag_ref[...] = jnp.broadcast_to(jnp.max(seen, axis=0, keepdims=True), flag_ref.shape)
        rows, full, codes = [], [], []
        for p, v, d, l, q in zip(pos, over, dest, local, spot):
            pair = l // 2 * ndev + d
            rows.append(jnp.where(v, base + d // 2 * crow + q, pair * crow + l % 2 * mean + p))
            full.append(pair * 2 * cap + l % 2 * cap + p)
            codes.append(jnp.where(v, 1 + (d % 2 * per_dev + l) * mean + p - mean, 0))
        for n, row in enumerate(rows + full):
            lane_ref[n:n + 1, :] = row
        tall[...] = jnp.zeros_like(tall)
        for n, row in enumerate(rows + full + [gates_ref[c:c + 1, :] for c in range(2)]):
            tall[n:n + 1, :] = row.astype(f32)
        col_ref[...] = tall[...].T
        lane = lax.broadcasted_iota(jnp.int32, (toks, ndev * crow), 1)
        for chip in range(chips):
            total = jnp.zeros(meta_ref.shape[1:], f32)
            for c in range(2):
                place = col_ref[:, c:c + 1].astype(jnp.int32) - (base + chip * crow) + me * crow
                hot = ((place == lane) & (lane // crow == me)).astype(f32).astype(bf16)
                code = jnp.broadcast_to(codes[c].astype(f32), (8, toks)).astype(bf16)
                total += jnp.dot(code, hot, preferred_element_type=f32)
            meta_ref[chip] = total

    def project(owner, half):
        r, t = owner // 4, owner % 4
        seg = r + half * (3 - 2 * r)
        x = xbuf[owner, pl.ds(pl.multiple_of(half * half_rows, half_rows), half_rows), :]
        out = jnp.dot(x, wqkv_ref[...], preferred_element_type=jnp.float32).astype(jnp.bfloat16)
        qkv[pl.ds(pl.multiple_of((seg * 4 + t) * half_rows, half_rows), half_rows), :] = out

    def near(s, _):
        @pl.when(s == 2)
        def _():
            arrive(CN, 0, half_rows, 0)

        @pl.when(s == 3)
        def _():
            arrive(CN, half_rows, half_rows, 2)

        project(idx(0, 0, s // 2), s % 2)
        return 0

    lax.fori_loop(0, 4, near, 0)
    tables()
    for j in range(1, ndev):
        flag_copy(j).start()

    w_x = [(1 + k, tp, cp * whalf + k * wpart, wpart, 1 + k, XN) for k in range(parts)]

    def gather(p):
        base = p * half_rows

        @pl.when(p == 0)
        def _():
            arrive(XN, 0, H, 0)
            arrive(YN, 0, H, 0)
            send(12, 10, 16, 17, 6, 8)

        def mid(u, _):
            @pl.when(u == 2)
            def _():
                arrive(XC, base, H, 2 * p)

            @pl.when(u == 3)
            def _():
                arrive(YC, base, H, 2 * p)

            project(idx(1 - u % 2, u % 2, u // 2), p)
            return 0

        lax.fori_loop(0, 4, mid, 0)

        @pl.when(p == 0)
        def _():
            arrive(XN, H, Q, 2)
            arrive(YN, H, Q, 2)
            send(11)

        arrive(DG, base, Q, 2 * p)
        arrive(DG, base + Q, Q, 2 * p + 1)

        @pl.when(p == 0)
        def _():
            send(14)

        @pl.when(p == 1)
        def _():
            send(15)

        def far(u, _):
            @pl.when(u == 1)
            def _():
                arrive(DC, base, H, 2 * p)

            project(idx(1, 1, u), p)
            return 0

        lax.fori_loop(0, 2, far, 0)

    def late():
        arrive(XN, H + Q, Q, 3)
        arrive(YN, H + Q, Q, 3)
        send(13, 7, 9)
        for spec in w_x:
            wcopy(*spec).start()

    coef = (head_dim ** -0.5) * math.log2(math.e)
    my_col = (4 * tp + 2 * cp) * head_dim

    def o_place(b):
        seg, t = b // 4, b % 4
        half = seg // 2
        return seg + half * (3 - 2 * seg), t, half

    def o_remote(b):
        r, t, half = o_place(b)
        return pltpu.make_async_remote_copy(
            src_ref=o_loc.at[pl.ds(pl.multiple_of(b * half_rows, half_rows), half_rows)],
            dst_ref=o_cat.at[pl.ds(pl.multiple_of(half * half_rows, half_rows), half_rows), pl.ds(pl.multiple_of(my_col, width), width)],
            send_sem=os_sem.at[b], recv_sem=or_sem.at[me, half], device_id={'cp': r, 'tp': t}, device_id_type=MESH)

    def o_local(b):
        _, _, half = o_place(b)
        return pltpu.make_async_copy(
            o_loc.at[pl.ds(pl.multiple_of(b * half_rows, half_rows), half_rows)],
            o_cat.at[pl.ds(pl.multiple_of(half * half_rows, half_rows), half_rows), pl.ds(pl.multiple_of(my_col, width), width)],
            os_sem.at[b])

    def o_send(i):
        for part in range(QB // half_rows):
            b = i * (QB // half_rows) + part
            r, t, _ = o_place(b)

            @pl.when(r * 4 + t != me)
            def _():
                o_remote(b).start()

            @pl.when(r * 4 + t == me)
            def _():
                o_local(b).start()

    peer_t = tp_of(1, 0)
    peer_c = tp_of(1, 1)

    def w_near(k, slot, shard, target):
        return wcopy(slot * parts + 1 + k, shard, cp * whalf + k * wpart, wpart, slot * parts + 1 + k, target)

    def w_far(k, slot, shard, target):
        return wcopy(slot * parts + 1 + k, shard, (1 - cp) * whalf + k * wpart, wpart, slot * parts + 1 + k, target)

    def w_pass(k):
        w_near(k, 0, peer_t, CN).wait_recv()
        w_near(k, 1, peer_t, YN).start()
        w_near(k, 2, peer_t, CN).start()

    def w_last(k):
        w_far(k, 1, peer_t, CN).wait_recv()
        w_far(k, 3, peer_t, CN).start()

    def at(i, step, *work):
        @pl.when(i == step)
        def _():
            for job, k in work:
                job(k)

    blocks = seq // QB

    def block_of(step):
        p, n = step // 4, step % 4
        y, x = (cp + 1 - n % 2) % 2, (xx + 1 - n // 2) % 2
        return 2 * (y + p * (3 - 2 * y)) + x

    def q_step(step, _):
        i = block_of(step)

        at(step, 4, (w_pass, 0))
        at(step, 5, (w_pass, 2))
        at(step, 7, (w_last, 1))

        q_rows = pl.ds(pl.multiple_of(i * QB, QB), QB)

        def cols(kind, h):
            return slice(kind * width + h * head_dim, kind * width + (h + 1) * head_dim)

        def scores(h, j):
            k = qkv[pl.ds(pl.multiple_of(j * QB, QB), QB), cols(1, h)]
            return lax.dot_general(qkv[q_rows, cols(0, h)], k, (((1,), (1,)), ((), ())), preferred_element_type=jnp.float32)

        def pass1(j, ms):
            out = []
            for h in range(heads):
                s = scores(h, j)
                s_ref[h, :, pl.ds(pl.multiple_of(j * QB, QB), QB)] = s
                out.append(jnp.maximum(ms[h], lane_fold(s, jnp.maximum)))
            return tuple(out)

        ms = lax.fori_loop(0, i, pass1, tuple(jnp.full((QB, 128), -jnp.inf, jnp.float32) for _ in range(heads)))
        keep = lax.broadcasted_iota(jnp.int32, (QB, QB), 1) <= lax.broadcasted_iota(jnp.int32, (QB, QB), 0)
        tops = []
        for h in range(heads):
            s = jnp.where(keep, scores(h, i), -jnp.inf)
            s_ref[h, :, pl.ds(pl.multiple_of(i * QB, QB), QB)] = s
            tops.append(jnp.max(jnp.maximum(ms[h], lane_fold(s, jnp.maximum)), axis=1, keepdims=True))
        acc_ref[...] = jnp.zeros_like(acc_ref)
        @pl.when(step == 2)
        def _():
            late()
            for early in range(2):
                o_send(block_of(early))

        at(step, 4, (w_pass, 1))
        at(step, 5, (w_pass, 3))
        at(step, 6, (w_last, 0))
        at(step, 7, (w_last, 2))


        def pass2(j, ls):
            out = []
            for h in range(heads):
                e = jnp.exp2((s_ref[h, :, pl.ds(pl.multiple_of(j * QB, QB), QB)] - tops[h]) * coef)
                v = qkv[pl.ds(pl.multiple_of(j * QB, QB), QB), cols(2, h)]
                acc_ref[h] += jnp.dot(e.astype(jnp.bfloat16), v, preferred_element_type=jnp.float32)
                out.append(ls[h] + lane_fold(e, jnp.add))
            return tuple(out)

        ls = lax.fori_loop(0, i + 1, pass2, tuple(jnp.zeros((QB, 128), jnp.float32) for _ in range(heads)))
        for h in range(heads):
            total = jnp.sum(ls[h], axis=1, keepdims=True)
            o_loc[q_rows, h * head_dim:(h + 1) * head_dim] = (acc_ref[h] / total).astype(jnp.bfloat16)

        @pl.when(step >= 2)
        def _():
            o_send(i)

        return 0

    def phase(p, _):
        gather(p)
        lax.fori_loop(p * (blocks // 2), (p + 1) * (blocks // 2), q_step, 0)
        return 0

    lax.fori_loop(0, 2, phase, 0)

    w_last(3)
    wcopy(0, tp_of(0, 1), 0, wrows, 0, CN).wait_recv()
    for k in range(parts):
        w_near(k, 2, peer_c, CN).wait_recv()
        w_far(k, 3, peer_c, CN).wait_recv()

    def o_arrived(half):
        for k in range(1, ndev):
            src = (me + k) % ndev
            col = (4 * (src % 4) + 2 * (src // 4)) * head_dim
            ref = o_cat.at[pl.ds(half * half_rows, half_rows), pl.ds(pl.multiple_of(col, width), width)]
            pltpu.make_async_remote_copy(src_ref=ref, dst_ref=ref, send_sem=os_sem.at[0], recv_sem=or_sem.at[src, half], device_id=dev(0, 0, 1), device_id_type=MESH).wait_recv()

    my_seg = [cp, 3 - cp]
    tile = 512
    for half in range(2):
        o_arrived(half)
        o_local(my_seg[half] * 4 + tp).wait()
        r = slice(half * half_rows, (half + 1) * half_rows)

        def out_step(n, _):
            c = pl.ds(pl.multiple_of(n * tile, tile), tile)
            a = jnp.dot(o_cat[r, :], wo_buf[:, c], preferred_element_type=jnp.float32)
            h_ref[r, c] = (xbuf[me, r, c].astype(jnp.float32) + a).astype(jnp.bfloat16)
            return 0

        lax.fori_loop(0, d_model // tile, out_step, 0)
        pltpu.make_async_copy(h_ref.at[r], h_hbm.at[r], h_sem.at[half]).start()

    def drain(b, _):
        r, t, _half = o_place(b)

        @pl.when(r * 4 + t != me)
        def _():
            o_remote(b).wait_send()

        return 0

    lax.fori_loop(0, seq // half_rows, drain, 0)

    most = flag_ref[...]
    for j in range(1, ndev):
        peer = (me + j) % ndev
        pltpu.make_async_remote_copy(src_ref=flag_ref, dst_ref=flags.at[peer], send_sem=fs.at[j], recv_sem=fr.at[peer], device_id=dev(0, 0, 1), device_id_type=MESH).wait_recv()
        most = jnp.maximum(most, flags[peer])
        flag_copy(j).wait_send()
    any_ref[0, 0] = jnp.max(most).astype(jnp.int32)

    for slot in range(len(sends)):
        xcopy(slot, *sends[slot]).wait_send()
    w_own.wait_send()
    for spec in w_x:
        wcopy(*spec).wait_send()
    for k in range(parts):
        w_near(k, 1, peer_t, YN).wait_send()
        w_near(k, 2, peer_t, CN).wait_send()
        w_far(k, 3, peer_t, CN).wait_send()
    for half in range(2):
        r = slice(half * half_rows, (half + 1) * half_rows)
        pltpu.make_async_copy(h_ref.at[r], h_hbm.at[r], h_sem.at[half]).wait()


def attention_block(x_blk, w_q, w_k, w_v, w_o, ids, gates, heads, head_dim, ndev, experts):
    rows, d_model = x_blk.shape
    seq = rows * ndev
    width = heads * head_dim
    vm = pl.BlockSpec(memory_space=pltpu.VMEM)
    hbm = pl.BlockSpec(memory_space=pl.ANY)
    bf16, f32 = jnp.bfloat16, jnp.float32
    dma = pltpu.SemaphoreType.DMA
    return pl.pallas_call(
        functools.partial(attn_block, heads=heads, head_dim=head_dim, experts=experts),
        name='attn_block',
        out_shape=(jax.ShapeDtypeStruct((rows, d_model), bf16), jax.ShapeDtypeStruct((1, 1), jnp.int32), jax.ShapeDtypeStruct((8, rows), jnp.int32), jax.ShapeDtypeStruct((rows, 128), f32), jax.ShapeDtypeStruct((ndev // 2, 8, rows * ndev * 4 // experts), f32)),
        in_specs=[hbm] * 5 + [vm] * 2,
        out_specs=(hbm, pl.BlockSpec(memory_space=pltpu.SMEM), vm, vm, vm),
        scratch_shapes=[
            pltpu.VMEM((ndev, rows, d_model), bf16), pltpu.VMEM((d_model, 3 * width), bf16), pltpu.VMEM((d_model, heads, head_dim), bf16), pltpu.VMEM((seq, 3 * width), bf16),
            pltpu.VMEM((heads, QB, seq), f32), pltpu.VMEM((heads, QB, head_dim), f32),
            pltpu.VMEM((seq, width), bf16), pltpu.VMEM((rows, ndev * width), bf16),
            pltpu.VMEM((ndev * width, d_model), bf16),
            pltpu.VMEM((8, 128), f32), pltpu.VMEM((ndev, 8, 128), f32), pltpu.VMEM((128, rows), f32), pltpu.VMEM((rows, d_model), bf16), dma((2,)),
            dma((3,)), dma((18,)), dma((ndev, 4)), dma((17,)), dma((17,)), dma((16,)), dma((ndev, 2)), dma((ndev,)), dma((ndev,)),
        ],
        compiler_params=pltpu.CompilerParams(collective_id=0, has_side_effects=True, vmem_limit_bytes=63 * MIB),
        cost_estimate=pl.CostEstimate(flops=2 * seq * d_model * width * 3 + 4 * seq * seq * width, bytes_accessed=16 * MIB, transcendentals=0),
    )(x_blk, w_q, w_k, w_v, w_o, ids, gates)


def moe_block(h_hbm, rl_ref, col_ref, meta_ref, wg_hbm, wu_hbm, wd_hbm, y_hbm, h_ref, y_ref, io_sem, send, recv, zbuf, ret,
              meta_in, sp_send, sp_recv, sp_z, sp_ret, pool_in, xs, zacc, acc, wg, wu, wd, ds, dr, rs, rr, ms, mr, sp_sem, sp_dr, pool_s, pool_r, sp_rs, sp_rr, wsem, *, main, spill):
    cp, tp = lax.axis_index('cp'), lax.axis_index('tp')
    xx, cc = tp // 2, tp % 2
    me = cp * 4 + tp
    chunks, ndev, crow, d_model = send.shape
    rows_all = ndev * crow
    toks = h_ref.shape[0]
    experts = wg_hbm.shape[0]
    slots, _, ff_half = wg.shape
    sp_rows = sp_send.shape[1]
    sp_base = chunks * rows_all
    c0 = 0 if spill else 2
    steps = 2 * experts
    tile = 512
    f32, bf16 = jnp.float32, jnp.bfloat16

    def weights(n):
        e, f, slot = n // 2, n % 2, n % slots
        fcols = pl.ds(pl.multiple_of(f * ff_half, ff_half), ff_half)
        return (pltpu.make_async_copy(wg_hbm.at[e, :, fcols], wg.at[slot], wsem.at[slot, 0]),
                pltpu.make_async_copy(wu_hbm.at[e, :, fcols], wu.at[slot], wsem.at[slot, 1]),
                pltpu.make_async_copy(wd_hbm.at[e, fcols, :], wd.at[slot], wsem.at[slot, 2]))

    def fetch(n):
        for copy in weights(n):
            copy.start()

    h_load = pltpu.make_async_copy(h_hbm, h_ref, io_sem.at[0])
    h_load.start()
    for n in range(slots - 1):
        fetch(n)

    def peer_of(j):
        return (me + j) % ndev

    def dev(p):
        return {'cp': p // 4, 'tp': p % 4}

    barrier = pltpu.get_barrier_semaphore()
    for j in range(1, ndev):
        pl.semaphore_signal(barrier, inc=1, device_id=dev(peer_of(j)), device_id_type=MESH)
    pl.semaphore_wait(barrier, ndev - 1)

    AWAY = [(1, 0), (0, 1), (1, 1)]

    def chip(dx, dy):
        return ((cp + dy) % 2) * 2 + (xx + dx) % 2

    def idx(dx, dy, dc):
        return chip(dx, dy) * 2 + (cc + dc) % 2

    def sp_copy(src, dst, ssem, rsem, target):
        return pltpu.make_async_remote_copy(src_ref=src, dst_ref=dst, send_sem=ssem, recv_sem=rsem, device_id=dev(idx(*target)), device_id_type=MESH)

    def sp_out(n):
        if n < 3:
            return sp_copy(sp_send.at[chip(*AWAY[n])], sp_recv.at[me], sp_sem.at[n], sp_dr.at[me], AWAY[n] + (0,))
        return sp_copy(sp_send.at[chip(0, 0)], sp_recv.at[me], sp_sem.at[3], sp_dr.at[me], (0, 0, 1))

    def sp_pass(n):
        ref = sp_recv.at[idx(*AWAY[n], 0)]
        return sp_copy(ref, ref, sp_sem.at[4 + n], sp_dr.at[idx(*AWAY[n], 0)], (0, 0, 1))

    def sp_arrived(source):
        ref = sp_recv.at[idx(*source)]
        sp_copy(ref, ref, sp_sem.at[0], sp_dr.at[idx(*source)], (0, 0, 1)).wait_recv()

    def sp_pool(n):
        side = ([(0, 0)] + AWAY)[n]
        return sp_copy(sp_z.at[idx(*side, 1)], pool_in.at[n], pool_s.at[n], pool_r.at[n], (0, 0, 1))

    def sp_back(n):
        side = AWAY[n]
        return sp_copy(sp_z.at[idx(*side, 0)], sp_ret.at[chip(0, 0)], sp_rs.at[n], sp_rr.at[chip(0, 0)], side + (0,))

    def meta_copy(j):
        return pltpu.make_async_remote_copy(src_ref=meta_ref.at[peer_of(j) // 2], dst_ref=meta_in.at[me], send_sem=ms.at[j], recv_sem=mr.at[me], device_id=dev(peer_of(j)), device_id_type=MESH)

    if spill:
        for j in range(1, ndev):
            meta_copy(j).start()

    def exchange(src, dst, ssem, rsem, k):
        def copy(j):
            return pltpu.make_async_remote_copy(src_ref=src.at[k, peer_of(j)], dst_ref=dst.at[k, me], send_sem=ssem.at[k, j], recv_sem=rsem.at[k, me], device_id=dev(peer_of(j)), device_id_type=MESH)

        local = pltpu.make_async_copy(src.at[k, me], dst.at[k, me], ssem.at[k, 0])
        return copy, local

    def begin(src, dst, ssem, rsem, k):
        copy, local = exchange(src, dst, ssem, rsem, k)
        local.start()
        for j in range(1, ndev):
            copy(j).start()

    def arrived(src, dst, ssem, rsem, k):
        for j in range(1, ndev):
            pltpu.make_async_remote_copy(src_ref=src.at[k, peer_of(j)], dst_ref=dst.at[k, peer_of(j)], send_sem=ssem.at[k, j], recv_sem=rsem.at[k, peer_of(j)], device_id=dev(peer_of(j)), device_id_type=MESH).wait_recv()
        exchange(src, dst, ssem, rsem, k)[1].wait()

    def left(src, dst, ssem, rsem, k):
        copy, _ = exchange(src, dst, ssem, rsem, k)
        for j in range(1, ndev):
            copy(j).wait_send()

    out_way = (send, recv, ds, dr)
    back_way = (zbuf, ret, rs, rr)

    def sp_own():
        return pltpu.make_async_copy(sp_send.at[chip(0, 0)], sp_recv.at[me], sp_sem.at[7])

    h_load.wait()
    if spill:
        ids = lax.broadcasted_iota(jnp.int32, (4 * sp_rows, toks), 0) + sp_base
        pick = ((ids == rl_ref[c0:c0 + 1, :]) | (ids == rl_ref[c0 + 1:c0 + 2, :])).astype(f32).astype(bf16)

        def sp_cols(n, _):
            c = pl.ds(pl.multiple_of(n * tile, tile), tile)
            sp_send[:, :, c] = jnp.dot(pick, h_ref[:, c], preferred_element_type=f32).astype(bf16).reshape(4, sp_rows, tile)
            return 0

        lax.fori_loop(0, d_model // tile, sp_cols, 0)
        for n in range(4):
            sp_out(n).start()
        sp_own().start()

    def pack(k, _):
        ids = lax.broadcasted_iota(jnp.int32, (rows_all, toks), 0) + k * rows_all
        pick = ((ids == rl_ref[c0:c0 + 1, :]) | (ids == rl_ref[c0 + 1:c0 + 2, :])).astype(f32).astype(bf16)

        def cols(n, _):
            c = pl.ds(pl.multiple_of(n * tile, tile), tile)
            rows = jnp.dot(pick, h_ref[:, c], preferred_element_type=f32).astype(bf16)
            send[k, :, :, c] = rows.reshape(ndev, crow, tile)
            return 0

        lax.fori_loop(0, d_model // tile, cols, 0)

        @pl.when(k > 0)
        def _():
            begin(*out_way, k - 1)

        return 0

    lax.fori_loop(0, chunks, pack, 0)
    begin(*out_way, chunks - 1)

    if spill:
        for j in range(1, ndev):
            p = peer_of(j)
            pltpu.make_async_remote_copy(src_ref=meta_in.at[p], dst_ref=meta_in.at[p], send_sem=ms.at[j], recv_sem=mr.at[p], device_id=dev(p), device_id_type=MESH).wait_recv()
        for n in range(3):
            sp_arrived(AWAY[n] + (0,))
            sp_pass(n).start()
        sp_own().wait()
        sp_arrived((0, 0, 1))
        for n in range(3):
            sp_arrived(AWAY[n] + (1,))
        total = meta_ref[me // 2]
        for j in range(1, ndev):
            total = total + meta_in[peer_of(j)]
        code = total[0:1, :].astype(jnp.int32) - 1 - cc * (experts * main)
        lane = lax.broadcasted_iota(jnp.int32, code.shape, 1)
        place = (lane // sp_rows) * main + (code & (main - 1))
        owner = code // main
        sp_z[...] = jnp.zeros_like(sp_z)
    body = ndev * main

    def expert(e, _):
        k = e // 2
        part = pl.ds(pl.multiple_of((e % 2) * main, main), main)

        @pl.when(e % 2 == 0)
        def _():
            arrived(*out_way, k)

        xs[0:body, :] = recv[k, :, part, :].reshape(body, d_model)
        if spill:
            slot_id = lax.broadcasted_iota(jnp.int32, (body, ndev * sp_rows), 0)
            pick = ((slot_id == place) & (owner == e)).astype(f32).astype(bf16)

            def gather(n, _):
                c = pl.ds(pl.multiple_of(n * tile, tile), tile)
                xs[body:2 * body, c] = jnp.dot(pick, sp_recv[:, :, c].reshape(ndev * sp_rows, tile), preferred_element_type=f32).astype(bf16)
                return 0

            lax.fori_loop(0, d_model // tile, gather, 0)

        for f in range(2):
            n = 2 * e + f
            slot = n % slots
            for copy in weights(n):
                copy.wait()

            @pl.when(n + slots - 1 < steps)
            def _():
                fetch(n + slots - 1)

            x = xs[...]
            gate = jnp.dot(x, wg[slot], preferred_element_type=f32)
            up = jnp.dot(x, wu[slot], preferred_element_type=f32)
            u = (gate * jax.nn.sigmoid(gate) * up).astype(bf16)

            def down(n, _):
                c = pl.ds(pl.multiple_of(n * tile, tile), tile)
                z = jnp.dot(u, wd[slot, :, c], preferred_element_type=f32)
                if f == 0:
                    zacc[:, c] = z
                else:
                    z = (zacc[:, c] + z).astype(bf16)
                    zbuf[k, :, part, c] = z[0:body].reshape(ndev, main, tile)
                    if spill:
                        spread = lax.dot_general(pick, z[body:], (((0,), (0,)), ((), ())), preferred_element_type=f32)
                        sp_z[:, :, c] = sp_z[:, :, c] + spread.astype(bf16).reshape(ndev, sp_rows, tile)
                return 0

            lax.fori_loop(0, d_model // tile, down, 0)
            if f == 0:
                @pl.when((e % 2 == 0) & (e > 0))
                def _():
                    begin(*back_way, k - 1)

        return 0

    lax.fori_loop(0, experts, expert, 0)
    if spill:
        for n in range(4):
            sp_pool(n).start()
    begin(*back_way, chunks - 1)
    acc[...] = jnp.zeros_like(acc)

    def sp_home():
        return pltpu.make_async_copy(sp_z.at[me], sp_ret.at[chip(0, 0)], sp_rs.at[3])

    if spill:
        for n in range(4):
            sp_pool(n).wait_recv()
            at = idx(*([(0, 0)] + AWAY)[n], 0)
            sp_z[at] = sp_z[at] + pool_in[n]
        for n in range(3):
            sp_back(n).start()
        sp_home().start()

    row0, row1 = (col_ref[:, c:c + 1].astype(jnp.int32) for c in (c0, c0 + 1))

    def chosen(ids, z):
        z0 = jnp.dot((ids == row0).astype(f32).astype(bf16), z, preferred_element_type=f32)
        z1 = jnp.dot((ids == row1).astype(f32).astype(bf16), z, preferred_element_type=f32)
        return col_ref[:, 4:5] * z0 + col_ref[:, 5:6] * z1

    def combine(k, _):
        arrived(*back_way, k)
        ids = lax.broadcasted_iota(jnp.int32, (toks, rows_all), 1) + k * rows_all

        def cols(n, _):
            c = pl.ds(pl.multiple_of(n * tile, tile), tile)
            acc[:, c] += chosen(ids, ret[k, :, :, c].reshape(rows_all, tile))
            return 0

        lax.fori_loop(0, d_model // tile, cols, 0)
        return 0

    lax.fori_loop(0, chunks, combine, 0)
    if spill:
        sp_home().wait()
        for n in range(3):
            ref = sp_ret.at[chip(*AWAY[n])]
            sp_copy(ref, ref, sp_rs.at[n], sp_rr.at[chip(*AWAY[n])], (0, 0, 1)).wait_recv()

    def y_copy(n):
        c = pl.ds(pl.multiple_of(n * tile, tile), tile)
        return pltpu.make_async_copy(y_ref.at[:, c], y_hbm.at[:, c], io_sem.at[n])

    def finish(n, _):
        c = pl.ds(pl.multiple_of(n * tile, tile), tile)
        moe_out = acc[:, c]
        if spill:
            ids = lax.broadcasted_iota(jnp.int32, (toks, 4 * sp_rows), 1) + sp_base
            moe_out += chosen(ids, sp_ret[:, :, c].reshape(4 * sp_rows, tile))
        y_ref[:, c] = (h_ref[:, c].astype(f32) + moe_out).astype(bf16)
        y_copy(n).start()
        return 0

    lax.fori_loop(0, d_model // tile, finish, 0)

    def drain(k, _):
        left(*out_way, k)
        left(*back_way, k)
        return 0

    lax.fori_loop(0, chunks, drain, 0)
    for n in range(d_model // tile):
        y_copy(n).wait()
    if spill:
        for j in range(1, ndev):
            meta_copy(j).wait_send()
        for n in range(4):
            sp_out(n).wait_send()
            sp_pool(n).wait_send()
        for n in range(3):
            sp_pass(n).wait_send()
            sp_back(n).wait_send()


def moe(hidden, lane, col, meta, w_gate, w_up, w_down, ndev, main, spill):
    toks, d_model = hidden.shape
    experts, _, ff = w_gate.shape
    crow = 2 * main
    chunks = experts // 2
    sp_rows = 2 * main if spill else 16
    slots = 3 if spill else 2
    vm = pl.BlockSpec(memory_space=pltpu.VMEM)
    hbm = pl.BlockSpec(memory_space=pl.ANY)
    bf16, f32 = jnp.bfloat16, jnp.float32
    dma = pltpu.SemaphoreType.DMA
    buf = pltpu.VMEM((chunks, ndev, crow, d_model), bf16)
    tile_rows = 2 * ndev * main if spill else ndev * main
    return pl.pallas_call(
        functools.partial(moe_block, main=main, spill=spill),
        name='moe_spill' if spill else 'moe_full',
        out_shape=jax.ShapeDtypeStruct((toks, d_model), bf16),
        in_specs=[hbm] + [vm] * 3 + [hbm] * 3,
        out_specs=hbm,
        scratch_shapes=[
            pltpu.VMEM((toks, d_model), bf16), pltpu.VMEM((toks, d_model), bf16), dma((d_model // 512,)),
            buf, buf, buf, buf, pltpu.VMEM((ndev,) + meta.shape[1:], f32),
            pltpu.VMEM((4, sp_rows, d_model), bf16), pltpu.VMEM((ndev, sp_rows, d_model), bf16), pltpu.VMEM((ndev, sp_rows, d_model), bf16),
            pltpu.VMEM((4, sp_rows, d_model), bf16), pltpu.VMEM((4, sp_rows, d_model), bf16),
            pltpu.VMEM((tile_rows, d_model), bf16), pltpu.VMEM((tile_rows, d_model), f32), pltpu.VMEM((toks, d_model), f32),
            pltpu.VMEM((slots, d_model, ff // 2), bf16), pltpu.VMEM((slots, d_model, ff // 2), bf16), pltpu.VMEM((slots, ff // 2, d_model), bf16),
            dma((chunks, ndev)), dma((chunks, ndev)), dma((chunks, ndev)), dma((chunks, ndev)), dma((ndev,)), dma((ndev,)),
            dma((8,)), dma((ndev,)), dma((4,)), dma((4,)), dma((4,)), dma((4,)), dma((slots, 3)),
        ],
        compiler_params=pltpu.CompilerParams(collective_id=1 if spill else 2, has_side_effects=True, vmem_limit_bytes=63 * MIB),
        cost_estimate=pl.CostEstimate(flops=6 * tile_rows * experts * d_model * ff, bytes_accessed=6 * experts * d_model * ff, transcendentals=0),
    )(hidden, lane, col, meta, w_gate, w_up, w_down)


def solution(mesh):
    cp_size = mesh.shape['cp']
    tp_size = mesh.shape['tp']
    num_devs = cp_size * tp_size
    row_spec = P(('data', 'cp', 'tp'), None)
    head_spec = P(None, 'tp', None)
    wo_spec = P('tp', None, None)
    expert_spec = P(('cp', 'tp'), None, None)

    def device_fn(x_blk, w_q, w_k, w_v, w_o, idx_blk, gate_blk, w_gate, w_up, w_down):
        tok_dev, d_model = x_blk.shape
        heads_tp, head_dim = w_q.shape[1], w_q.shape[2]
        heads = heads_tp // cp_size
        exp_local = w_gate.shape[0]
        num_exp = exp_local * num_devs
        capacity = 4 * tok_dev // num_exp
        mean = capacity // 2
        crow = 2 * mean
        hidden, most, lane, col, meta = attention_block(x_blk, w_q, w_k, w_v, w_o.reshape(-1, d_model), idx_blk.T, gate_blk.T, heads, head_dim, num_devs, num_exp)

        def run(main, spill):
            return lambda h: moe(h, lane, col, meta, w_gate, w_up, w_down, num_devs, main, spill)

        return lax.cond(most[0, 0] <= crow, run(mean, True), run(capacity, False), hidden)

    return jax.shard_map(device_fn, mesh=mesh, in_specs=(row_spec, head_spec, head_spec, head_spec, wo_spec, row_spec, row_spec, expert_spec, expert_spec, expert_spec), out_specs=row_spec, check_vma=False)
```

```python
import functools
import math

import jax
import jax.numpy as jnp
from jax import lax
from jax.experimental import pallas as pl
from jax.experimental.pallas import tpu as pltpu
from jax.sharding import PartitionSpec as P

MESH = pl.DeviceIdType.MESH
MIB = 1024 * 1024
QB = 512


def lane_fold(s, op):
    out = s[:, :128]
    for g in range(1, s.shape[1] // 128):
        out = op(out, s[:, g * 128:(g + 1) * 128])
    return out


def attn_block(x_hbm, wq_hbm, wk_hbm, wv_hbm, wo_hbm, ids_ref, gates_ref, h_hbm, any_ref, lane_ref, col_ref, meta_ref, xbuf, wqkv_ref, w_pair, qkv, s_ref, acc_ref, o_loc, o_cat, wo_buf,
               flag_ref, flags, tall, h_ref, h_sem, loc_sem, xs, xr, ws, wr, os_sem, or_sem, fs, fr, *, heads, head_dim, experts):
    cp, tp = lax.axis_index('cp'), lax.axis_index('tp')
    xx, cc = tp // 2, tp % 2
    me = cp * 4 + tp
    ndev, rows, d_model = xbuf.shape
    half_rows = rows // 2
    quarter = half_rows // 2
    width = heads * head_dim
    seq = ndev * rows
    wrows = wo_hbm.shape[0]
    parts = 4
    whalf, wpart = wrows // 2, wrows // 2 // parts

    def tp_of(dx, dc):
        return ((xx + dx) % 2) * 2 + (cc + dc) % 2

    def idx(dx, dy, dc):
        return ((cp + dy) % 2) * 4 + tp_of(dx, dc)

    def dev(dx, dy, dc):
        return {'cp': (cp + dy) % 2, 'tp': tp_of(dx, dc)}

    x_load = pltpu.make_async_copy(x_hbm, xbuf.at[me], loc_sem.at[0])
    wo_load = pltpu.make_async_copy(wo_hbm, wo_buf.at[pl.ds(tp * wrows, wrows)], loc_sem.at[1])
    x_load.start()
    wo_load.start()
    w_loads = [pltpu.make_async_copy(w.at[:, pl.ds(heads * cp, heads), :], w_pair, loc_sem.at[2]) for w in (wq_hbm, wk_hbm, wv_hbm)]
    w_loads[0].start()

    barrier = pltpu.get_barrier_semaphore()
    for k in range(1, ndev):
        peer = (me + k) % ndev
        pl.semaphore_signal(barrier, inc=1, device_id={'cp': peer // 4, 'tp': peer % 4}, device_id_type=MESH)
    pl.semaphore_wait(barrier, ndev - 1)

    def xcopy(slot, owner, row0, count, part, target):
        ref = xbuf.at[idx(*owner), pl.ds(row0 if isinstance(row0, int) else pl.multiple_of(row0, quarter), count)]
        return pltpu.make_async_remote_copy(src_ref=ref, dst_ref=ref, send_sem=xs.at[slot], recv_sem=xr.at[idx(*owner), part], device_id=dev(*target), device_id_type=MESH)

    XN, YN, CN, DG, OWN = (1, 0, 0), (0, 1, 0), (0, 0, 1), (1, 1, 0), (0, 0, 0)
    XC, YC, DC = (1, 0, 1), (0, 1, 1), (1, 1, 1)
    H, Q = half_rows, quarter
    sends = [
        (OWN, 0, H, 0, XN), (OWN, H, Q, 2, XN), (OWN, 0, H, 0, YN), (OWN, H, Q, 2, YN), (OWN, 0, H, 0, CN), (OWN, H, H, 2, CN),
        (XN, 0, H, 0, CN), (XN, H, H, 2, CN), (YN, 0, H, 0, CN), (YN, H, H, 2, CN),
        (YN, 0, Q, 0, XN), (YN, H, Q, 2, XN), (XN, Q, Q, 1, YN), (XN, H + Q, Q, 3, YN),
        (DG, 0, H, 0, CN), (DG, H, H, 2, CN), (OWN, H + Q, Q, 3, XN), (OWN, H + Q, Q, 3, YN),
    ]

    def send(*slots):
        for slot in slots:
            xcopy(slot, *sends[slot]).start()

    def arrive(owner, row0, count, part):
        xcopy(0, owner, row0, count, part, CN).wait_recv()

    def wcopy(slot, shard, row0, count, sem, target):
        ref = wo_buf.at[pl.ds(shard * wrows + row0, count)]
        return pltpu.make_async_remote_copy(src_ref=ref, dst_ref=ref, send_sem=ws.at[slot], recv_sem=wr.at[sem], device_id=dev(*target), device_id_type=MESH)

    def flag_copy(j):
        peer = (me + j) % ndev
        return pltpu.make_async_remote_copy(src_ref=flag_ref, dst_ref=flags.at[me], send_sem=fs.at[j], recv_sem=fr.at[me], device_id={'cp': peer // 4, 'tp': peer % 4}, device_id_type=MESH)

    x_load.wait()
    send(0, 2, 4, 1, 3, 5)
    wo_load.wait()
    w_own = wcopy(0, tp, 0, wrows, 0, CN)
    w_own.start()

    for kind in range(3):
        w_loads[kind].wait()

        def relayout(n, _):
            r = pl.ds(pl.multiple_of(n * 256, 256), 256)
            for h in range(heads):
                c = kind * width + h * head_dim
                wqkv_ref[r, c:c + head_dim] = w_pair[r, h, :]
            return 0

        lax.fori_loop(0, d_model // 256, relayout, 0)
        if kind < 2:
            w_loads[kind + 1].start()

    def tables():
        toks = ids_ref.shape[1]
        f32, bf16 = jnp.float32, jnp.bfloat16
        cap = 4 * toks // experts
        mean = cap // 2
        per_dev = experts // ndev
        chips = ndev // 2
        crow = 2 * mean
        base = per_dev // 2 * ndev * crow
        before = (lax.broadcasted_iota(jnp.int32, (toks, toks), 0) < lax.broadcasted_iota(jnp.int32, (toks, toks), 1)).astype(f32).astype(bf16)

        def ranks(keys, keep, size):
            out, seen = [], jnp.zeros((size, 1), f32)
            for key, ok in zip(keys, keep):
                hot = jnp.where((lax.broadcasted_iota(jnp.int32, (size, toks), 0) == key) & ok, 1.0, 0.0)
                prior = jnp.dot(hot.astype(bf16), before, preferred_element_type=f32) + seen
                out.append(jnp.sum(hot * prior, axis=0, keepdims=True).astype(jnp.int32))
                seen = seen + jnp.sum(hot, axis=1, keepdims=True)
            return out, seen

        ids = [ids_ref[c:c + 1, :] for c in range(2)]
        pos, _ = ranks(ids, [i >= 0 for i in ids], experts)
        over = [p >= mean for p in pos]
        dest = [i // per_dev for i in ids]
        local = [i - d * per_dev for i, d in zip(ids, dest)]
        spot, seen = ranks([d // 2 for d in dest], over, 8)
        flag_ref[...] = jnp.broadcast_to(jnp.max(seen, axis=0, keepdims=True), flag_ref.shape)
        rows, full, codes = [], [], []
        for p, v, d, l, q in zip(pos, over, dest, local, spot):
            pair = l // 2 * ndev + d
            rows.append(jnp.where(v, base + d // 2 * crow + q, pair * crow + l % 2 * mean + p))
            full.append(pair * 2 * cap + l % 2 * cap + p)
            codes.append(jnp.where(v, 1 + (d % 2 * per_dev + l) * mean + p - mean, 0))
        for n, row in enumerate(rows + full):
            lane_ref[n:n + 1, :] = row
        tall[...] = jnp.zeros_like(tall)
        for n, row in enumerate(rows + full + [gates_ref[c:c + 1, :] for c in range(2)]):
            tall[n:n + 1, :] = row.astype(f32)
        col_ref[...] = tall[...].T
        lane = lax.broadcasted_iota(jnp.int32, (toks, ndev * crow), 1)
        for chip in range(chips):
            total = jnp.zeros(meta_ref.shape[1:], f32)
            for c in range(2):
                place = col_ref[:, c:c + 1].astype(jnp.int32) - (base + chip * crow) + me * crow
                hot = ((place == lane) & (lane // crow == me)).astype(f32).astype(bf16)
                code = jnp.broadcast_to(codes[c].astype(f32), (8, toks)).astype(bf16)
                total += jnp.dot(code, hot, preferred_element_type=f32)
            meta_ref[chip] = total

    def project(owner, half):
        r, t = owner // 4, owner % 4
        seg = r + half * (3 - 2 * r)
        x = xbuf[owner, pl.ds(pl.multiple_of(half * half_rows, half_rows), half_rows), :]
        out = jnp.dot(x, wqkv_ref[...], preferred_element_type=jnp.float32).astype(jnp.bfloat16)
        qkv[pl.ds(pl.multiple_of((seg * 4 + t) * half_rows, half_rows), half_rows), :] = out

    def near(s, _):
        @pl.when(s == 2)
        def _():
            arrive(CN, 0, half_rows, 0)

        @pl.when(s == 3)
        def _():
            arrive(CN, half_rows, half_rows, 2)

        project(idx(0, 0, s // 2), s % 2)
        return 0

    lax.fori_loop(0, 4, near, 0)
    tables()
    for j in range(1, ndev):
        flag_copy(j).start()

    w_x = [(1 + k, tp, cp * whalf + k * wpart, wpart, 1 + k, XN) for k in range(parts)]

    def gather(p):
        base = p * half_rows

        @pl.when(p == 0)
        def _():
            arrive(XN, 0, H, 0)
            arrive(YN, 0, H, 0)
            send(12, 10, 16, 17, 6, 8)

        def mid(u, _):
            @pl.when(u == 2)
            def _():
                arrive(XC, base, H, 2 * p)

            @pl.when(u == 3)
            def _():
                arrive(YC, base, H, 2 * p)

            project(idx(1 - u % 2, u % 2, u // 2), p)
            return 0

        lax.fori_loop(0, 4, mid, 0)

        @pl.when(p == 0)
        def _():
            arrive(XN, H, Q, 2)
            arrive(YN, H, Q, 2)
            send(11)

        arrive(DG, base, Q, 2 * p)
        arrive(DG, base + Q, Q, 2 * p + 1)

        @pl.when(p == 0)
        def _():
            send(14)

        @pl.when(p == 1)
        def _():
            send(15)

        def far(u, _):
            @pl.when(u == 1)
            def _():
                arrive(DC, base, H, 2 * p)

            project(idx(1, 1, u), p)
            return 0

        lax.fori_loop(0, 2, far, 0)

    def late():
        arrive(XN, H + Q, Q, 3)
        arrive(YN, H + Q, Q, 3)
        send(13, 7, 9)
        for spec in w_x:
            wcopy(*spec).start()

    coef = (head_dim ** -0.5) * math.log2(math.e)
    my_col = (4 * tp + 2 * cp) * head_dim

    def o_place(b):
        seg, t = b // 4, b % 4
        half = seg // 2
        return seg + half * (3 - 2 * seg), t, half

    def o_remote(b):
        r, t, half = o_place(b)
        return pltpu.make_async_remote_copy(
            src_ref=o_loc.at[pl.ds(pl.multiple_of(b * half_rows, half_rows), half_rows)],
            dst_ref=o_cat.at[pl.ds(pl.multiple_of(half * half_rows, half_rows), half_rows), pl.ds(pl.multiple_of(my_col, width), width)],
            send_sem=os_sem.at[b], recv_sem=or_sem.at[me, half], device_id={'cp': r, 'tp': t}, device_id_type=MESH)

    def o_local(b):
        _, _, half = o_place(b)
        return pltpu.make_async_copy(
            o_loc.at[pl.ds(pl.multiple_of(b * half_rows, half_rows), half_rows)],
            o_cat.at[pl.ds(pl.multiple_of(half * half_rows, half_rows), half_rows), pl.ds(pl.multiple_of(my_col, width), width)],
            os_sem.at[b])

    def o_send(i):
        for part in range(QB // half_rows):
            b = i * (QB // half_rows) + part
            r, t, _ = o_place(b)

            @pl.when(r * 4 + t != me)
            def _():
                o_remote(b).start()

            @pl.when(r * 4 + t == me)
            def _():
                o_local(b).start()

    peer_t = tp_of(1, 0)
    peer_c = tp_of(1, 1)

    def w_near(k, slot, shard, target):
        return wcopy(slot * parts + 1 + k, shard, cp * whalf + k * wpart, wpart, slot * parts + 1 + k, target)

    def w_far(k, slot, shard, target):
        return wcopy(slot * parts + 1 + k, shard, (1 - cp) * whalf + k * wpart, wpart, slot * parts + 1 + k, target)

    def w_pass(k):
        w_near(k, 0, peer_t, CN).wait_recv()
        w_near(k, 1, peer_t, YN).start()
        w_near(k, 2, peer_t, CN).start()

    def w_last(k):
        w_far(k, 1, peer_t, CN).wait_recv()
        w_far(k, 3, peer_t, CN).start()

    def at(i, step, *work):
        @pl.when(i == step)
        def _():
            for job, k in work:
                job(k)

    blocks = seq // QB

    def block_of(step):
        p, n = step // 4, step % 4
        y, x = (cp + 1 - n % 2) % 2, (xx + 1 - n // 2) % 2
        return 2 * (y + p * (3 - 2 * y)) + x

    def q_step(step, _):
        i = block_of(step)

        at(step, 4, (w_pass, 0))
        at(step, 5, (w_pass, 2))
        at(step, 7, (w_last, 1))

        q_rows = pl.ds(pl.multiple_of(i * QB, QB), QB)

        def cols(kind, h):
            return slice(kind * width + h * head_dim, kind * width + (h + 1) * head_dim)

        def scores(h, j):
            k = qkv[pl.ds(pl.multiple_of(j * QB, QB), QB), cols(1, h)]
            return lax.dot_general(qkv[q_rows, cols(0, h)], k, (((1,), (1,)), ((), ())), preferred_element_type=jnp.float32)

        def pass1(j, ms):
            out = []
            for h in range(heads):
                s = scores(h, j)
                s_ref[h, :, pl.ds(pl.multiple_of(j * QB, QB), QB)] = s
                out.append(jnp.maximum(ms[h], lane_fold(s, jnp.maximum)))
            return tuple(out)

        ms = lax.fori_loop(0, i, pass1, tuple(jnp.full((QB, 128), -jnp.inf, jnp.float32) for _ in range(heads)))
        keep = lax.broadcasted_iota(jnp.int32, (QB, QB), 1) <= lax.broadcasted_iota(jnp.int32, (QB, QB), 0)
        tops = []
        for h in range(heads):
            s = jnp.where(keep, scores(h, i), -jnp.inf)
            s_ref[h, :, pl.ds(pl.multiple_of(i * QB, QB), QB)] = s
            tops.append(jnp.max(jnp.maximum(ms[h], lane_fold(s, jnp.maximum)), axis=1, keepdims=True))
        acc_ref[...] = jnp.zeros_like(acc_ref)
        @pl.when(step == 2)
        def _():
            late()
            for early in range(2):
                o_send(block_of(early))

        at(step, 4, (w_pass, 1))
        at(step, 5, (w_pass, 3))
        at(step, 6, (w_last, 0))
        at(step, 7, (w_last, 2))


        def pass2(j, ls):
            out = []
            for h in range(heads):
                e = jnp.exp2((s_ref[h, :, pl.ds(pl.multiple_of(j * QB, QB), QB)] - tops[h]) * coef)
                v = qkv[pl.ds(pl.multiple_of(j * QB, QB), QB), cols(2, h)]
                acc_ref[h] += jnp.dot(e.astype(jnp.bfloat16), v, preferred_element_type=jnp.float32)
                out.append(ls[h] + lane_fold(e, jnp.add))
            return tuple(out)

        ls = lax.fori_loop(0, i + 1, pass2, tuple(jnp.zeros((QB, 128), jnp.float32) for _ in range(heads)))
        for h in range(heads):
            total = jnp.sum(ls[h], axis=1, keepdims=True)
            o_loc[q_rows, h * head_dim:(h + 1) * head_dim] = (acc_ref[h] / total).astype(jnp.bfloat16)

        @pl.when(step >= 2)
        def _():
            o_send(i)

        return 0

    def phase(p, _):
        gather(p)
        lax.fori_loop(p * (blocks // 2), (p + 1) * (blocks // 2), q_step, 0)
        return 0

    lax.fori_loop(0, 2, phase, 0)

    w_last(3)
    wcopy(0, tp_of(0, 1), 0, wrows, 0, CN).wait_recv()
    for k in range(parts):
        w_near(k, 2, peer_c, CN).wait_recv()
        w_far(k, 3, peer_c, CN).wait_recv()

    def o_arrived(half):
        for k in range(1, ndev):
            src = (me + k) % ndev
            col = (4 * (src % 4) + 2 * (src // 4)) * head_dim
            ref = o_cat.at[pl.ds(half * half_rows, half_rows), pl.ds(pl.multiple_of(col, width), width)]
            pltpu.make_async_remote_copy(src_ref=ref, dst_ref=ref, send_sem=os_sem.at[0], recv_sem=or_sem.at[src, half], device_id=dev(0, 0, 1), device_id_type=MESH).wait_recv()

    my_seg = [cp, 3 - cp]
    tile = 512
    for half in range(2):
        o_arrived(half)
        o_local(my_seg[half] * 4 + tp).wait()
        r = slice(half * half_rows, (half + 1) * half_rows)

        def out_step(n, _):
            c = pl.ds(pl.multiple_of(n * tile, tile), tile)
            a = jnp.dot(o_cat[r, :], wo_buf[:, c], preferred_element_type=jnp.float32)
            h_ref[r, c] = (xbuf[me, r, c].astype(jnp.float32) + a).astype(jnp.bfloat16)
            return 0

        lax.fori_loop(0, d_model // tile, out_step, 0)
        pltpu.make_async_copy(h_ref.at[r], h_hbm.at[r], h_sem.at[half]).start()

    def drain(b, _):
        r, t, _half = o_place(b)

        @pl.when(r * 4 + t != me)
        def _():
            o_remote(b).wait_send()

        return 0

    lax.fori_loop(0, seq // half_rows, drain, 0)

    most = flag_ref[...]
    for j in range(1, ndev):
        peer = (me + j) % ndev
        pltpu.make_async_remote_copy(src_ref=flag_ref, dst_ref=flags.at[peer], send_sem=fs.at[j], recv_sem=fr.at[peer], device_id=dev(0, 0, 1), device_id_type=MESH).wait_recv()
        most = jnp.maximum(most, flags[peer])
        flag_copy(j).wait_send()
    any_ref[0, 0] = jnp.max(most).astype(jnp.int32)

    for slot in range(len(sends)):
        xcopy(slot, *sends[slot]).wait_send()
    w_own.wait_send()
    for spec in w_x:
        wcopy(*spec).wait_send()
    for k in range(parts):
        w_near(k, 1, peer_t, YN).wait_send()
        w_near(k, 2, peer_t, CN).wait_send()
        w_far(k, 3, peer_t, CN).wait_send()
    for half in range(2):
        r = slice(half * half_rows, (half + 1) * half_rows)
        pltpu.make_async_copy(h_ref.at[r], h_hbm.at[r], h_sem.at[half]).wait()


def attention_block(x_blk, w_q, w_k, w_v, w_o, ids, gates, heads, head_dim, ndev, experts):
    rows, d_model = x_blk.shape
    seq = rows * ndev
    width = heads * head_dim
    vm = pl.BlockSpec(memory_space=pltpu.VMEM)
    hbm = pl.BlockSpec(memory_space=pl.ANY)
    bf16, f32 = jnp.bfloat16, jnp.float32
    dma = pltpu.SemaphoreType.DMA
    return pl.pallas_call(
        functools.partial(attn_block, heads=heads, head_dim=head_dim, experts=experts),
        name='attn_block',
        out_shape=(jax.ShapeDtypeStruct((rows, d_model), bf16), jax.ShapeDtypeStruct((1, 1), jnp.int32), jax.ShapeDtypeStruct((8, rows), jnp.int32), jax.ShapeDtypeStruct((rows, 128), f32), jax.ShapeDtypeStruct((ndev // 2, 8, rows * ndev * 4 // experts), f32)),
        in_specs=[hbm] * 5 + [vm] * 2,
        out_specs=(hbm, pl.BlockSpec(memory_space=pltpu.SMEM), vm, vm, vm),
        scratch_shapes=[
            pltpu.VMEM((ndev, rows, d_model), bf16), pltpu.VMEM((d_model, 3 * width), bf16), pltpu.VMEM((d_model, heads, head_dim), bf16), pltpu.VMEM((seq, 3 * width), bf16),
            pltpu.VMEM((heads, QB, seq), f32), pltpu.VMEM((heads, QB, head_dim), f32),
            pltpu.VMEM((seq, width), bf16), pltpu.VMEM((rows, ndev * width), bf16),
            pltpu.VMEM((ndev * width, d_model), bf16),
            pltpu.VMEM((8, 128), f32), pltpu.VMEM((ndev, 8, 128), f32), pltpu.VMEM((128, rows), f32), pltpu.VMEM((rows, d_model), bf16), dma((2,)),
            dma((3,)), dma((18,)), dma((ndev, 4)), dma((17,)), dma((17,)), dma((16,)), dma((ndev, 2)), dma((ndev,)), dma((ndev,)),
        ],
        compiler_params=pltpu.CompilerParams(collective_id=0, has_side_effects=True, vmem_limit_bytes=63 * MIB),
        cost_estimate=pl.CostEstimate(flops=2 * seq * d_model * width * 3 + 4 * seq * seq * width, bytes_accessed=16 * MIB, transcendentals=0),
    )(x_blk, w_q, w_k, w_v, w_o, ids, gates)


def moe_block(h_hbm, rl_ref, col_ref, meta_ref, wg_hbm, wu_hbm, wd_hbm, y_hbm, h_ref, y_ref, io_sem, send, recv, zbuf, ret,
              meta_in, sp_send, sp_recv, sp_z, sp_ret, pool_in, xs, zacc, acc, wg, wu, wd, ds, dr, rs, rr, ms, mr, sp_sem, sp_dr, pool_s, pool_r, sp_rs, sp_rr, wsem, *, main, spill):
    cp, tp = lax.axis_index('cp'), lax.axis_index('tp')
    xx, cc = tp // 2, tp % 2
    me = cp * 4 + tp
    chunks, ndev, crow, d_model = send.shape
    rows_all = ndev * crow
    toks = h_ref.shape[0]
    experts = wg_hbm.shape[0]
    slots, _, ff_half = wg.shape
    sp_rows = sp_send.shape[1]
    sp_base = chunks * rows_all
    c0 = 0 if spill else 2
    steps = 2 * experts
    tile = 512
    f32, bf16 = jnp.float32, jnp.bfloat16

    def weights(n):
        e, f, slot = n // 2, n % 2, n % slots
        fcols = pl.ds(pl.multiple_of(f * ff_half, ff_half), ff_half)
        return (pltpu.make_async_copy(wg_hbm.at[e, :, fcols], wg.at[slot], wsem.at[slot, 0]),
                pltpu.make_async_copy(wu_hbm.at[e, :, fcols], wu.at[slot], wsem.at[slot, 1]),
                pltpu.make_async_copy(wd_hbm.at[e, fcols, :], wd.at[slot], wsem.at[slot, 2]))

    def fetch(n):
        for copy in weights(n):
            copy.start()

    h_load = pltpu.make_async_copy(h_hbm, h_ref, io_sem.at[0])
    h_load.start()
    for n in range(slots - 1):
        fetch(n)

    order = [(0, 0, 0), (1, 0, 0), (0, 1, 0), (1, 1, 0), (1, 0, 1), (0, 1, 1), (1, 1, 1), (0, 0, 1)]

    def peer_of(j):
        dx, dy, dc = order[j]
        return ((cp + dy) % 2) * 4 + ((xx + dx) % 2) * 2 + (cc + dc) % 2

    def dev(p):
        return {'cp': p // 4, 'tp': p % 4}

    barrier = pltpu.get_barrier_semaphore()
    for j in range(1, ndev):
        pl.semaphore_signal(barrier, inc=1, device_id=dev(peer_of(j)), device_id_type=MESH)
    pl.semaphore_wait(barrier, ndev - 1)

    AWAY = [(1, 0), (0, 1), (1, 1)]

    def chip(dx, dy):
        return ((cp + dy) % 2) * 2 + (xx + dx) % 2

    def idx(dx, dy, dc):
        return chip(dx, dy) * 2 + (cc + dc) % 2

    def sp_copy(src, dst, ssem, rsem, target):
        return pltpu.make_async_remote_copy(src_ref=src, dst_ref=dst, send_sem=ssem, recv_sem=rsem, device_id=dev(idx(*target)), device_id_type=MESH)

    def sp_out(n):
        if n < 3:
            return sp_copy(sp_send.at[chip(*AWAY[n])], sp_recv.at[me], sp_sem.at[n], sp_dr.at[me], AWAY[n] + (0,))
        return sp_copy(sp_send.at[chip(0, 0)], sp_recv.at[me], sp_sem.at[3], sp_dr.at[me], (0, 0, 1))

    def sp_pass(n):
        ref = sp_recv.at[idx(*AWAY[n], 0)]
        return sp_copy(ref, ref, sp_sem.at[4 + n], sp_dr.at[idx(*AWAY[n], 0)], (0, 0, 1))

    def sp_arrived(source):
        ref = sp_recv.at[idx(*source)]
        sp_copy(ref, ref, sp_sem.at[0], sp_dr.at[idx(*source)], (0, 0, 1)).wait_recv()

    def sp_pool(n):
        side = ([(0, 0)] + AWAY)[n]
        return sp_copy(sp_z.at[idx(*side, 1)], pool_in.at[n], pool_s.at[n], pool_r.at[n], (0, 0, 1))

    def sp_back(n):
        side = AWAY[n]
        return sp_copy(sp_z.at[idx(*side, 0)], sp_ret.at[chip(0, 0)], sp_rs.at[n], sp_rr.at[chip(0, 0)], side + (0,))

    def meta_copy(j):
        return pltpu.make_async_remote_copy(src_ref=meta_ref.at[peer_of(j) // 2], dst_ref=meta_in.at[me], send_sem=ms.at[j], recv_sem=mr.at[me], device_id=dev(peer_of(j)), device_id_type=MESH)

    if spill:
        for j in range(1, ndev):
            meta_copy(j).start()

    def exchange(src, dst, ssem, rsem, k):
        def copy(j):
            return pltpu.make_async_remote_copy(src_ref=src.at[k, peer_of(j)], dst_ref=dst.at[k, me], send_sem=ssem.at[k, j], recv_sem=rsem.at[k, me], device_id=dev(peer_of(j)), device_id_type=MESH)

        local = pltpu.make_async_copy(src.at[k, me], dst.at[k, me], ssem.at[k, 0])
        return copy, local

    def begin(src, dst, ssem, rsem, k):
        copy, local = exchange(src, dst, ssem, rsem, k)
        local.start()
        for j in range(1, ndev):
            copy(j).start()

    def arrived(src, dst, ssem, rsem, k):
        for j in range(1, ndev):
            pltpu.make_async_remote_copy(src_ref=src.at[k, peer_of(j)], dst_ref=dst.at[k, peer_of(j)], send_sem=ssem.at[k, j], recv_sem=rsem.at[k, peer_of(j)], device_id=dev(peer_of(j)), device_id_type=MESH).wait_recv()
        exchange(src, dst, ssem, rsem, k)[1].wait()

    def left(src, dst, ssem, rsem, k):
        copy, _ = exchange(src, dst, ssem, rsem, k)
        for j in range(1, ndev):
            copy(j).wait_send()

    out_way = (send, recv, ds, dr)
    back_way = (zbuf, ret, rs, rr)

    def sp_own():
        return pltpu.make_async_copy(sp_send.at[chip(0, 0)], sp_recv.at[me], sp_sem.at[7])

    h_load.wait()
    if spill:
        ids = lax.broadcasted_iota(jnp.int32, (4 * sp_rows, toks), 0) + sp_base
        pick = ((ids == rl_ref[c0:c0 + 1, :]) | (ids == rl_ref[c0 + 1:c0 + 2, :])).astype(f32).astype(bf16)

        def sp_cols(n, _):
            c = pl.ds(pl.multiple_of(n * tile, tile), tile)
            sp_send[:, :, c] = jnp.dot(pick, h_ref[:, c], preferred_element_type=f32).astype(bf16).reshape(4, sp_rows, tile)
            return 0

        lax.fori_loop(0, d_model // tile, sp_cols, 0)
        for n in range(4):
            sp_out(n).start()
        sp_own().start()

    def pack(k, _):
        ids = lax.broadcasted_iota(jnp.int32, (rows_all, toks), 0) + k * rows_all
        pick = ((ids == rl_ref[c0:c0 + 1, :]) | (ids == rl_ref[c0 + 1:c0 + 2, :])).astype(f32).astype(bf16)

        def cols(n, _):
            c = pl.ds(pl.multiple_of(n * tile, tile), tile)
            rows = jnp.dot(pick, h_ref[:, c], preferred_element_type=f32).astype(bf16)
            send[k, :, :, c] = rows.reshape(ndev, crow, tile)
            return 0

        lax.fori_loop(0, d_model // tile, cols, 0)

        @pl.when(k > 0)
        def _():
            begin(*out_way, k - 1)

        return 0

    lax.fori_loop(0, chunks, pack, 0)
    begin(*out_way, chunks - 1)

    if spill:
        for j in range(1, ndev):
            p = peer_of(j)
            pltpu.make_async_remote_copy(src_ref=meta_in.at[p], dst_ref=meta_in.at[p], send_sem=ms.at[j], recv_sem=mr.at[p], device_id=dev(p), device_id_type=MESH).wait_recv()
        for n in range(3):
            sp_arrived(AWAY[n] + (0,))
            sp_pass(n).start()
        sp_own().wait()
        sp_arrived((0, 0, 1))
        for n in range(3):
            sp_arrived(AWAY[n] + (1,))
        total = meta_ref[me // 2]
        for j in range(1, ndev):
            total = total + meta_in[peer_of(j)]
        code = total[0:1, :].astype(jnp.int32) - 1 - cc * (experts * main)
        lane = lax.broadcasted_iota(jnp.int32, code.shape, 1)
        place = (lane // sp_rows) * main + (code & (main - 1))
        owner = code // main
        sp_z[...] = jnp.zeros_like(sp_z)
    body = ndev * main

    def expert(e, _):
        k = e // 2
        part = pl.ds(pl.multiple_of((e % 2) * main, main), main)

        @pl.when(e % 2 == 0)
        def _():
            arrived(*out_way, k)

        xs[0:body, :] = recv[k, :, part, :].reshape(body, d_model)
        if spill:
            slot_id = lax.broadcasted_iota(jnp.int32, (body, ndev * sp_rows), 0)
            pick = ((slot_id == place) & (owner == e)).astype(f32).astype(bf16)

            def gather(n, _):
                c = pl.ds(pl.multiple_of(n * tile, tile), tile)
                xs[body:2 * body, c] = jnp.dot(pick, sp_recv[:, :, c].reshape(ndev * sp_rows, tile), preferred_element_type=f32).astype(bf16)
                return 0

            lax.fori_loop(0, d_model // tile, gather, 0)

        for f in range(2):
            n = 2 * e + f
            slot = n % slots
            for copy in weights(n):
                copy.wait()

            @pl.when(n + slots - 1 < steps)
            def _():
                fetch(n + slots - 1)

            x = xs[...]
            gate = jnp.dot(x, wg[slot], preferred_element_type=f32)
            up = jnp.dot(x, wu[slot], preferred_element_type=f32)
            u = (gate * jax.nn.sigmoid(gate) * up).astype(bf16)

            def down(n, _):
                c = pl.ds(pl.multiple_of(n * tile, tile), tile)
                z = jnp.dot(u, wd[slot, :, c], preferred_element_type=f32)
                if f == 0:
                    zacc[:, c] = z
                else:
                    z = (zacc[:, c] + z).astype(bf16)
                    zbuf[k, :, part, c] = z[0:body].reshape(ndev, main, tile)
                    if spill:
                        spread = lax.dot_general(pick, z[body:], (((0,), (0,)), ((), ())), preferred_element_type=f32)
                        sp_z[:, :, c] = sp_z[:, :, c] + spread.astype(bf16).reshape(ndev, sp_rows, tile)
                return 0

            lax.fori_loop(0, d_model // tile, down, 0)
            if f == 0:
                @pl.when((e % 2 == 0) & (e > 0))
                def _():
                    begin(*back_way, k - 1)

        return 0

    lax.fori_loop(0, experts, expert, 0)
    if spill:
        for n in range(4):
            sp_pool(n).start()
    begin(*back_way, chunks - 1)
    acc[...] = jnp.zeros_like(acc)

    def sp_home():
        return pltpu.make_async_copy(sp_z.at[me], sp_ret.at[chip(0, 0)], sp_rs.at[3])

    if spill:
        for n in range(4):
            sp_pool(n).wait_recv()
            at = idx(*([(0, 0)] + AWAY)[n], 0)
            sp_z[at] = sp_z[at] + pool_in[n]
        for n in range(3):
            sp_back(n).start()
        sp_home().start()

    row0, row1 = (col_ref[:, c:c + 1].astype(jnp.int32) for c in (c0, c0 + 1))

    def chosen(ids, z):
        z0 = jnp.dot((ids == row0).astype(f32).astype(bf16), z, preferred_element_type=f32)
        z1 = jnp.dot((ids == row1).astype(f32).astype(bf16), z, preferred_element_type=f32)
        return col_ref[:, 4:5] * z0 + col_ref[:, 5:6] * z1

    def combine(k, _):
        arrived(*back_way, k)
        ids = lax.broadcasted_iota(jnp.int32, (toks, rows_all), 1) + k * rows_all

        def cols(n, _):
            c = pl.ds(pl.multiple_of(n * tile, tile), tile)
            acc[:, c] += chosen(ids, ret[k, :, :, c].reshape(rows_all, tile))
            return 0

        lax.fori_loop(0, d_model // tile, cols, 0)
        return 0

    lax.fori_loop(0, chunks, combine, 0)
    if spill:
        sp_home().wait()
        for n in range(3):
            ref = sp_ret.at[chip(*AWAY[n])]
            sp_copy(ref, ref, sp_rs.at[n], sp_rr.at[chip(*AWAY[n])], (0, 0, 1)).wait_recv()

    def y_copy(n):
        c = pl.ds(pl.multiple_of(n * tile, tile), tile)
        return pltpu.make_async_copy(y_ref.at[:, c], y_hbm.at[:, c], io_sem.at[n])

    def finish(n, _):
        c = pl.ds(pl.multiple_of(n * tile, tile), tile)
        moe_out = acc[:, c]
        if spill:
            ids = lax.broadcasted_iota(jnp.int32, (toks, 4 * sp_rows), 1) + sp_base
            moe_out += chosen(ids, sp_ret[:, :, c].reshape(4 * sp_rows, tile))
        y_ref[:, c] = (h_ref[:, c].astype(f32) + moe_out).astype(bf16)
        y_copy(n).start()
        return 0

    lax.fori_loop(0, d_model // tile, finish, 0)

    def drain(k, _):
        left(*out_way, k)
        left(*back_way, k)
        return 0

    lax.fori_loop(0, chunks, drain, 0)
    for n in range(d_model // tile):
        y_copy(n).wait()
    if spill:
        for j in range(1, ndev):
            meta_copy(j).wait_send()
        for n in range(4):
            sp_out(n).wait_send()
            sp_pool(n).wait_send()
        for n in range(3):
            sp_pass(n).wait_send()
            sp_back(n).wait_send()


def moe(hidden, lane, col, meta, w_gate, w_up, w_down, ndev, main, spill):
    toks, d_model = hidden.shape
    experts, _, ff = w_gate.shape
    crow = 2 * main
    chunks = experts // 2
    sp_rows = 2 * main if spill else 16
    slots = 3 if spill else 2
    vm = pl.BlockSpec(memory_space=pltpu.VMEM)
    hbm = pl.BlockSpec(memory_space=pl.ANY)
    bf16, f32 = jnp.bfloat16, jnp.float32
    dma = pltpu.SemaphoreType.DMA
    buf = pltpu.VMEM((chunks, ndev, crow, d_model), bf16)
    tile_rows = 2 * ndev * main if spill else ndev * main
    return pl.pallas_call(
        functools.partial(moe_block, main=main, spill=spill),
        name='moe_spill' if spill else 'moe_full',
        out_shape=jax.ShapeDtypeStruct((toks, d_model), bf16),
        in_specs=[hbm] + [vm] * 3 + [hbm] * 3,
        out_specs=hbm,
        scratch_shapes=[
            pltpu.VMEM((toks, d_model), bf16), pltpu.VMEM((toks, d_model), bf16), dma((d_model // 512,)),
            buf, buf, buf, buf, pltpu.VMEM((ndev,) + meta.shape[1:], f32),
            pltpu.VMEM((4, sp_rows, d_model), bf16), pltpu.VMEM((ndev, sp_rows, d_model), bf16), pltpu.VMEM((ndev, sp_rows, d_model), bf16),
            pltpu.VMEM((4, sp_rows, d_model), bf16), pltpu.VMEM((4, sp_rows, d_model), bf16),
            pltpu.VMEM((tile_rows, d_model), bf16), pltpu.VMEM((tile_rows, d_model), f32), pltpu.VMEM((toks, d_model), f32),
            pltpu.VMEM((slots, d_model, ff // 2), bf16), pltpu.VMEM((slots, d_model, ff // 2), bf16), pltpu.VMEM((slots, ff // 2, d_model), bf16),
            dma((chunks, ndev)), dma((chunks, ndev)), dma((chunks, ndev)), dma((chunks, ndev)), dma((ndev,)), dma((ndev,)),
            dma((8,)), dma((ndev,)), dma((4,)), dma((4,)), dma((4,)), dma((4,)), dma((slots, 3)),
        ],
        compiler_params=pltpu.CompilerParams(collective_id=1 if spill else 2, has_side_effects=True, vmem_limit_bytes=63 * MIB),
        cost_estimate=pl.CostEstimate(flops=6 * tile_rows * experts * d_model * ff, bytes_accessed=6 * experts * d_model * ff, transcendentals=0),
    )(hidden, lane, col, meta, w_gate, w_up, w_down)


def solution(mesh):
    cp_size = mesh.shape['cp']
    tp_size = mesh.shape['tp']
    num_devs = cp_size * tp_size
    row_spec = P(('data', 'cp', 'tp'), None)
    head_spec = P(None, 'tp', None)
    wo_spec = P('tp', None, None)
    expert_spec = P(('cp', 'tp'), None, None)

    def device_fn(x_blk, w_q, w_k, w_v, w_o, idx_blk, gate_blk, w_gate, w_up, w_down):
        tok_dev, d_model = x_blk.shape
        heads_tp, head_dim = w_q.shape[1], w_q.shape[2]
        heads = heads_tp // cp_size
        exp_local = w_gate.shape[0]
        num_exp = exp_local * num_devs
        capacity = 4 * tok_dev // num_exp
        mean = capacity // 2
        crow = 2 * mean
        hidden, most, lane, col, meta = attention_block(x_blk, w_q, w_k, w_v, w_o.reshape(-1, d_model), idx_blk.T, gate_blk.T, heads, head_dim, num_devs, num_exp)

        def run(main, spill):
            return lambda h: moe(h, lane, col, meta, w_gate, w_up, w_down, num_devs, main, spill)

        return lax.cond(most[0, 0] <= crow, run(mean, True), run(capacity, False), hidden)

    return jax.shard_map(device_fn, mesh=mesh, in_specs=(row_spec, head_spec, head_spec, head_spec, wo_spec, row_spec, row_spec, expert_spec, expert_spec, expert_spec), out_specs=row_spec, check_vma=False)
```
